256 devices in a mesh: rows: 8 (over x_hi, y), cols: 32 (over z, x_lo, core).
Axes of the slice: x: 4 (x_hi: 2, x_lo: 2; x = x_hi * 2 + x_lo), y: 4, z: 8, core: 2. Of those that a mesh axis runs over, the one named last changes fastest.
Arguments:
- features: bfloat16 [4, 256, 64, 4096], P(None, None, 'rows', 'cols'), may hold values from -8 to 8
- cotangent: bfloat16 [4, 256, 64, 4096], P(None, None, 'rows', 'cols'), may hold values from -6 to 6
- reduce_weight: bfloat16 [256, 64], replicated, may hold values from -0.375 to 0.375
- spatial_weight: bfloat16 [9, 64, 64], replicated, may hold values from -0.25 to 0.25
- expand_weight: bfloat16 [64, 256], replicated, may hold values from -0.75 to 0.75
- reduce_factor: float32 [4, 256], replicated, may hold values from 0.25 to 1.75
- spatial_factor: float32 [4, 64], replicated, may hold values from 0.25 to 1.75
- expand_factor: float32 [4, 64], replicated, may hold values from 0.25 to 1.75
- output_factor: float32 [4, 256], replicated, may hold values from 0.25 to 1.75
- gain_first: float32 [64], replicated, may hold values from 0.25 to 1.75
- shift_first: float32 [64], replicated, may hold values from -3 to 3
- gain_second: float32 [64], replicated, may hold values from 0.25 to 1.75
- shift_second: float32 [64], replicated, may hold values from -3 to 3
Outputs:
- grad_features: bfloat16 [4, 256, 64, 4096], P(None, None, 'rows', 'cols')
- grad_reduce: float32 [256, 64], replicated
- grad_spatial: float32 [9, 64, 64], replicated
- grad_expand: float32 [64, 256], replicated
- grad_reduce_factor: float32 [4, 256], replicated
- grad_spatial_factor: float32 [4, 64], replicated
- grad_expand_factor: float32 [4, 64], replicated
- grad_output_factor: float32 [4, 256], replicated
- grad_gain_first: float32 [64], replicated
- grad_shift_first: float32 [64], replicated
- grad_gain_second: float32 [64], replicated
- grad_shift_second: float32 [64], replicated
The draws below stay inside these ranges and needn't reach their ends.
All inputs are finite; a program needn't handle non-finite values.
Results may differ from the reference program's by a relative error of at most 0.01.
Values may be sent and summed in bfloat16 or wider, within the bound.
A program may use at most 128 MiB of HBM per device.

```python
import jax
import jax.numpy as jnp
from jax import lax

C = 256
F = 64
M = 4
H = 64
W = 4096


def draw_features(key, part):
    first, second = jax.random.split(key, 2)
    trend = jnp.linspace(-0.5, 1.0, W, dtype=jnp.float32)
    base = jax.random.normal(first, (M, C, H, W), jnp.float32)
    scale = jnp.exp(jax.random.uniform(second, (1, C, 1, 1), jnp.float32, -0.5, 0.5))
    return jnp.clip(base * scale + trend[None, None, None, :], -8.0, 8.0).astype(jnp.bfloat16)


def level_of(stream_key, shape, cuts, smallest, high):
    loudness, own = 1.0, jax.random.fold_in(stream_key, 6)
    for dim, blocks in cuts:
        heights = jnp.exp(jax.random.uniform(jax.random.fold_in(own, dim), (blocks,), jnp.float32, smallest / len(cuts), high / len(cuts)))
        loudness = loudness * jnp.repeat(heights, shape[dim] // blocks).reshape([-1 if axis == dim else 1 for axis in range(len(shape))])
    return loudness


def noise(stream_key, extent, deviation, reach, cuts=(), kind=jnp.bfloat16):
    drawn = deviation * jax.random.normal(stream_key, extent, jnp.float32)
    if cuts:
        drawn = drawn * level_of(stream_key, extent, cuts, -0.22, 0.18)
    return jnp.clip(drawn, -reach, reach).astype(kind)


def setup_inputs(seed: int = 0) -> dict:
    seeds = jax.random.split(jax.random.key(seed), 14)
    return {
        "features": draw_features(jax.random.fold_in(seeds[13], 71), 0),
        "cotangent": noise(seeds[1], (M, C, H, W), 1.0, 6.0, ((2, 8), (3, 32))),
        "reduce_weight": noise(seeds[2], (C, F), C ** -0.5, 0.375),
        "spatial_weight": noise(seeds[3], (9, F, F), (9 * F) ** -0.5, 0.25),
        "expand_weight": noise(seeds[4], (F, C), F ** -0.5, 0.75),
        "reduce_factor": jnp.clip(1.0 + 0.15 * jax.random.normal(seeds[5], (M, C), jnp.float32), 0.25, 1.75),
        "spatial_factor": jnp.clip(1.0 + 0.15 * jax.random.normal(seeds[6], (M, F), jnp.float32), 0.25, 1.75),
        "expand_factor": jnp.clip(1.0 + 0.15 * jax.random.normal(seeds[7], (M, F), jnp.float32), 0.25, 1.75),
        "output_factor": jnp.clip(1.0 + 0.15 * jax.random.normal(seeds[8], (M, C), jnp.float32), 0.25, 1.75),
        "gain_first": jnp.clip(1.0 + 0.15 * jax.random.normal(seeds[9], (F,), jnp.float32), 0.25, 1.75),
        "shift_first": noise(seeds[10], (F,), 0.5, 3.0, (), jnp.float32),
        "gain_second": jnp.clip(1.0 + 0.15 * jax.random.normal(seeds[11], (F,), jnp.float32), 0.25, 1.75),
        "shift_second": noise(seeds[12], (F,), 0.5, 3.0, (), jnp.float32),
    }


EPSILON = 1e-05

def activate(value):
    return value * jax.nn.sigmoid(value)

def slope(value):
    sig = jax.nn.sigmoid(value)
    return sig * (1.0 + value * (1.0 - sig))

def norm_forward(acts, gain, shift):
    mean = lax.optimization_barrier(jnp.mean(acts, axis=1, keepdims=True))
    centred = acts - mean
    var = lax.optimization_barrier(jnp.mean(centred * centred, axis=1, keepdims=True))
    rstd = lax.rsqrt(var + EPSILON)
    normed = centred * rstd
    pre = gain[:, None] * normed + shift[:, None]
    return (activate(pre).astype(jnp.bfloat16), normed, pre, rstd)

def norm_backward(upstream, normed, pre, rstd, gain):
    count = upstream.shape[1]
    dpre = upstream * slope(pre)
    plain = lax.optimization_barrier(jnp.sum(dpre, axis=1, keepdims=True))
    weighted = lax.optimization_barrier(jnp.sum(dpre * normed, axis=1, keepdims=True))
    dact = gain[:, None] * rstd * (dpre - plain / count - normed * weighted / count)
    return (dact, weighted[:, 0], plain[:, 0])

def as_wide(value):
    return value.astype(jnp.float32)

def reference(features, cotangent, reduce_weight, spatial_weight, expand_weight, reduce_factor, spatial_factor, expand_factor, output_factor, gain_first, shift_first, gain_second, shift_second):
    narrow = reduce_weight.shape[1]
    cells = H * W
    rw = as_wide(reduce_weight)
    sw = as_wide(spatial_weight)
    ew = as_wide(expand_weight)
    member_reduce = (reduce_factor[:, :, None] * rw[None]).astype(jnp.bfloat16)
    member_spatial = (spatial_factor[:, None, :, None] * sw[None]).astype(jnp.bfloat16)
    member_expand = (expand_factor[:, :, None] * ew[None] * output_factor[:, None, :]).astype(jnp.bfloat16)

    def member_pass(inputs):
        image, upper, w_one, w_two, w_three = inputs
        flat = as_wide(image.reshape(C, cells))
        first = jnp.einsum('cf,cp->fp', as_wide(w_one), flat)
        hidden_one, normed_one, pre_one, rstd_one = norm_forward(first, gain_first, shift_first)
        padded_one = jnp.pad(as_wide(hidden_one).reshape(narrow, H, W), ((0, 0), (1, 1), (1, 1)))
        second = jnp.zeros((narrow, cells), jnp.float32)
        for tap in range(9):
            row_off, col_off = (tap // 3, tap % 3)
            window = padded_one[:, row_off:row_off + H, col_off:col_off + W].reshape(narrow, cells)
            second = second + jnp.einsum('fo,fp->op', as_wide(w_two[tap]), window)
        hidden_two, normed_two, pre_two, rstd_two = norm_forward(second, gain_second, shift_second)
        wide_two = as_wide(hidden_two)
        third = jnp.einsum('fc,fp->cp', as_wide(w_three), wide_two)
        summed = flat + third
        upstream = as_wide(upper.reshape(C, cells)) * slope(summed)
        upstream_low = as_wide(upstream.astype(jnp.bfloat16))
        back_two = jnp.einsum('fc,cp->fp', as_wide(w_three), upstream_low)
        part_expand = jnp.einsum('fp,cp->fc', wide_two, upstream_low)
        dact_two, gain_two_grad, shift_two_grad = norm_backward(back_two, normed_two, pre_two, rstd_two, gain_second)
        dact_two_low = as_wide(dact_two.astype(jnp.bfloat16))
        padded_back = jnp.pad(dact_two_low.reshape(narrow, H, W), ((0, 0), (1, 1), (1, 1)))
        back_one = jnp.zeros((narrow, cells), jnp.float32)
        pieces = []
        for tap in range(9):
            row_off, col_off = (tap // 3, tap % 3)
            flipped = padded_back[:, 2 - row_off:2 - row_off + H, 2 - col_off:2 - col_off + W].reshape(narrow, cells)
            back_one = back_one + jnp.einsum('fo,op->fp', as_wide(w_two[tap]), flipped)
            window = padded_one[:, row_off:row_off + H, col_off:col_off + W].reshape(narrow, cells)
            pieces.append(jnp.einsum('fp,op->fo', window, dact_two_low))
        part_spatial = jnp.stack(pieces, axis=0)
        dact_one, gain_one_grad, shift_one_grad = norm_backward(back_one, normed_one, pre_one, rstd_one, gain_first)
        dact_one_low = as_wide(dact_one.astype(jnp.bfloat16))
        grad_image = (upstream + jnp.einsum('cf,fp->cp', as_wide(w_one), dact_one_low)).astype(jnp.bfloat16)
        part_reduce = jnp.einsum('cp,fp->cf', flat, dact_one_low)
        return (grad_image.reshape(C, H, W), part_reduce, part_spatial, part_expand, gain_one_grad, shift_one_grad, gain_two_grad, shift_two_grad)
    outs = lax.map(member_pass, (features, cotangent, member_reduce, member_spatial, member_expand))
    grad_features, part_reduce, part_spatial, part_expand = (outs[0], outs[1], outs[2], outs[3])
    grad_reduce = lax.optimization_barrier(jnp.sum(part_reduce * reduce_factor[:, :, None], axis=0))
    grad_reduce_factor = lax.optimization_barrier(jnp.sum(part_reduce * rw[None], axis=2))
    grad_spatial = lax.optimization_barrier(jnp.sum(part_spatial * spatial_factor[:, None, :, None], axis=0))
    grad_spatial_factor = lax.optimization_barrier(jnp.sum(part_spatial * sw[None], axis=(1, 3)))
    grad_expand = lax.optimization_barrier(jnp.sum(part_expand * expand_factor[:, :, None] * output_factor[:, None, :], axis=0))
    grad_expand_factor = lax.optimization_barrier(jnp.sum(part_expand * ew[None] * output_factor[:, None, :], axis=2))
    grad_output_factor = lax.optimization_barrier(jnp.sum(part_expand * ew[None] * expand_factor[:, :, None], axis=1))
    return (grad_features, grad_reduce, grad_spatial, grad_expand, grad_reduce_factor, grad_spatial_factor, grad_expand_factor, grad_output_factor, lax.optimization_barrier(jnp.sum(outs[4], axis=0)), lax.optimization_barrier(jnp.sum(outs[5], axis=0)), lax.optimization_barrier(jnp.sum(outs[6], axis=0)), lax.optimization_barrier(jnp.sum(outs[7], axis=0)))
```

```python
import functools

import jax
import jax.numpy as jnp
from jax import lax
from jax.experimental import pallas as pl
from jax.experimental.pallas import tpu as pltpu
from jax.sharding import Mesh
from jax.sharding import PartitionSpec as P

ROWS = ("rows_0", "rows_1")
COLS = ("cols_0", "cols_1", "cols_2")
MESH = pl.DeviceIdType.MESH
EPSILON = 1e-05
F32 = jnp.float32
BF16 = jnp.bfloat16

CHUNK = 40
EXPAND, REDUCE, SPATIAL, REDUCE_F, OUTPUT_F, COLUMN_F = 0, 128, 256, 544, 552, 560


def dot(a, b, ca, cb):
    return lax.dot_general(a, b, (((ca,), (cb,)), ((), ())), preferred_element_type=F32)


def sigmoid(v):
    return 1.0 / (1.0 + jnp.exp(-v))


def silu(v):
    return v * sigmoid(v)


def slope(v):
    s = sigmoid(v)
    return s * (1.0 + v * (1.0 - s))


def lanes(shape):
    return lax.broadcasted_iota(jnp.int32, shape, len(shape) - 1)


def kernel(
    x_hbm, c_hbm, w1, w2, w2b, w3, rwt, sw, ew, rf, of, sfc, efc, gb,
    out_hbm, o_reduce, o_spatial, o_expand, o_rf, o_sf, o_ef, o_of, o_norm,
    x, c, u, hb, hq, dq, dpre1, nf, pk, pr, arb, ara, g, r1, r2, r3, cols,
    ld_sem, st_sem, s_sem, r_sem, hs_sem, hr_sem,
):
    count = float(64 * 4096)
    x_hi, y = lax.axis_index("rows_0"), lax.axis_index("rows_1")
    z, x_lo, core = lax.axis_index("cols_0"), lax.axis_index("cols_1"), lax.axis_index("cols_2")
    row = x_hi * 4 + y
    col = z * 4 + x_lo * 2 + core
    rank_a = x_hi * 8 + x_lo * 4 + y
    rank_b = z * 2 + core

    def peer_a(d):
        a = lax.rem(rank_a + d, 16)
        return (a // 8, lax.rem(a, 4), z, lax.rem(a // 4, 2), core)

    def peer_b(d):
        b = lax.rem(rank_b + d, 16)
        return (x_hi, y, b // 2, x_lo, lax.rem(b, 2))

    def at(dr, dc):
        rr, cc = lax.rem(row + dr + 8, 8), lax.rem(col + dc + 32, 32)
        return (rr // 4, lax.rem(rr, 4), cc // 4, lax.rem(cc // 2, 2), lax.rem(cc, 2))

    sides = ((0, 1), (0, -1), (1, 1), (1, -1), (-1, 1), (-1, -1))

    load_x = [pltpu.make_async_copy(x_hbm.at[m], x.at[m], ld_sem.at[m]) for m in range(4)]
    load_c = [pltpu.make_async_copy(c_hbm.at[m], c.at[m], ld_sem.at[4 + m]) for m in range(4)]
    for copy in load_x + load_c:
        copy.start()

    barrier = pltpu.get_barrier_semaphore()

    def greet(d, _):
        pl.semaphore_signal(barrier, inc=1, device_id=peer_a(d), device_id_type=MESH)
        pl.semaphore_signal(barrier, inc=1, device_id=peer_b(d), device_id_type=MESH)
        return 0

    lax.fori_loop(1, 16, greet, 0)
    for side in sides:
        pl.semaphore_signal(barrier, inc=1, device_id=at(*side), device_id_type=MESH)

    def exchange(stage, src, buf, rank, peer):
        def copy(d):
            return pltpu.make_async_remote_copy(
                src_ref=src(d), dst_ref=buf.at[rank], send_sem=s_sem.at[stage, d],
                recv_sem=r_sem.at[stage, d], device_id=peer(d), device_id_type=MESH,
            )

        def start(d, _):
            copy(d).start()
            return 0

        def wait(d, _):
            copy(d).wait()
            return 0

        return (lambda: lax.fori_loop(1, 16, start, 0)), (lambda: lax.fori_loop(1, 16, wait, 0))

    def total(buf):
        t = buf[0]
        for k in range(1, 16):
            t = t + buf[k]
        return t

    def reduce_start(k, tile):
        arb[k, rank_b] = tile
        start, wait = exchange(2 * k, lambda d: arb.at[k, rank_b], arb.at[k], rank_b, peer_b)
        start()
        return wait

    def reduce_end(k, wait):
        wait()
        ara[k, rank_a] = total(arb.at[k])
        start, wait = exchange(2 * k + 1, lambda d: ara.at[k, rank_a], ara.at[k], rank_a, peer_a)
        start()
        wait()
        return total(ara.at[k])

    def halo(k):
        copies = [
            pltpu.make_async_remote_copy(
                src_ref=hb.at[k, :, :, pl.ds(128, 128)], dst_ref=hb.at[k, :, :, pl.ds(1152, 128)],
                send_sem=hs_sem.at[k, 6], recv_sem=hr_sem.at[k, 6],
                device_id=at(-1, 0), device_id_type=MESH,
            ),
            pltpu.make_async_remote_copy(
                src_ref=hb.at[k, :, :, pl.ds(1024, 128)], dst_ref=hb.at[k, :, :, pl.ds(0, 128)],
                send_sem=hs_sem.at[k, 7], recv_sem=hr_sem.at[k, 7],
                device_id=at(1, 0), device_id_type=MESH,
            ),
        ]
        for n, side in enumerate(sides):
            copies.append(
                pltpu.make_async_remote_copy(
                    src_ref=pk.at[k], dst_ref=pr.at[k, n], send_sem=hs_sem.at[k, n],
                    recv_sem=hr_sem.at[k, n], device_id=at(*side), device_id_type=MESH,
                )
            )
        return copies

    lane = lanes((64, 128))

    def put(acc, n, value):
        return jnp.where(lane == n, value, acc)

    def rows_of_columns(acc):
        return jnp.transpose(jnp.concatenate([acc, jnp.zeros((64, 128), F32)], axis=0))[:8]

    def columns_of_rows(tile, k):
        t = jnp.transpose(jnp.concatenate([tile, jnp.zeros((120, 128), F32)], axis=0))
        for m in range(4):
            cols[k, m] = t[:64, m : m + 1]
            cols[k + 1, m] = t[:64, 4 + m : 5 + m]

    def sums(m, acc, a, b):
        acc = put(acc, m, jnp.sum(a, axis=1, keepdims=True))
        return put(acc, 4 + m, jnp.sum(b, axis=1, keepdims=True))

    def pack(k, m, acc):
        for i in range(8):
            t = hb[k, m, :, 128 + i * 128 : 256 + i * 128]
            acc = put(acc, m * 8 + i, t[:, 0:1])
            acc = put(acc, 32 + m * 8 + i, t[:, 127:128])
        return acc

    top = jnp.where(row > 0, 1.0, 0.0).astype(F32)
    bottom = jnp.where(row < 7, 1.0, 0.0).astype(F32)
    left = jnp.where(col > 0, 1.0, 0.0).astype(F32)
    right = jnp.where(col < 31, 1.0, 0.0).astype(F32)
    masks = (left, right, top * left, top * right, bottom * left, bottom * right)

    def spread(dst, m, tile, edge):
        edges = [edge(n) * masks[n] for n in range(6)]
        for i in range(10):
            t = tile(i)
            if i == 0:
                t, e0, e2, at_row = t * top, edges[2], edges[3], 7
            elif i == 9:
                t, e0, e2, at_row = t * bottom, edges[4], edges[5], 0
            else:
                e0, e2, at_row = edges[0], edges[1], i - 1
            where0 = 32 + m * 8 + at_row
            where2 = m * 8 + at_row
            before = jnp.where(
                lane == 0, pltpu.roll(e0, 128 - where0, axis=1), pltpu.roll(t, 1, axis=1)
            )
            after = jnp.where(
                lane == 127, pltpu.roll(e2, 127 - where2, axis=1), pltpu.roll(t, 127, axis=1)
            )
            span = slice(i * 128, i * 128 + 128)
            dst[m, 0:64, span] = before.astype(BF16)
            dst[m, 64:128, span] = t.astype(BF16)
            dst[m, 128:192, span] = after.astype(BF16)

    zero = jnp.zeros((64, 128), F32)

    def first_of(m, carry):
        acc, edge = carry
        a = dot(w1[m], x[m], 1, 0)
        hb[0, m, :, 128:1152] = a
        return sums(m, acc, a, a * a), pack(0, m, edge)

    for copy in load_x:
        copy.wait()
    acc, edge = lax.fori_loop(0, 4, first_of, (zero, zero))
    pk[0] = edge
    pl.semaphore_wait(barrier, 36)
    wait = reduce_start(0, rows_of_columns(acc))
    halos = halo(0)
    for copy in halos:
        copy.start()
    stats = reduce_end(0, wait)
    for copy in halos:
        copy.wait()

    def moments(k, tile):
        columns_of_rows(tile, k)
        for m in range(4):
            mean = cols[k, m] / count
            var = cols[k + 1, m] / count - mean * mean
            cols[k, m] = mean
            cols[k + 1, m] = lax.rsqrt(var + EPSILON)

    moments(0, stats)
    gain1, shift1, gain2, shift2 = (gb[n] for n in range(4))

    def second_of(m, carry):
        acc, edge = carry
        mean, rstd = cols[0, m], cols[1, m]

        def hidden(v):
            return silu(gain1 * ((v - mean) * rstd) + shift1)

        spread(
            hq, m, lambda i: hidden(hb[0, m, :, i * 128 : i * 128 + 128]),
            lambda n: hidden(pr[0, n]),
        )
        a = dot(w2[m, 0], hq[m, :, 0:1024], 0, 0)
        a = a + dot(w2[m, 1], hq[m, :, 128:1152], 0, 0)
        a = a + dot(w2[m, 2], hq[m, :, 256:1280], 0, 0)
        hb[1, m, :, 128:1152] = a
        return sums(m, acc, a, a * a), pack(1, m, edge)

    acc, edge = lax.fori_loop(0, 4, second_of, (zero, zero))
    pk[1] = edge
    wait = reduce_start(1, rows_of_columns(acc))
    halos = halo(1)
    for copy in halos:
        copy.start()
    stats = reduce_end(1, wait)
    for copy in halos:
        copy.wait()
    moments(2, stats)
    for copy in load_c:
        copy.wait()

    g[EXPAND : EXPAND + 128] = jnp.zeros((128, 128), F32)
    g[REDUCE : REDUCE + 128] = jnp.zeros((128, 128), F32)
    g[568:640] = jnp.zeros((72, 128), F32)

    def upstream_of(m, carry):
        acc, edge, fac = carry
        mean, rstd = cols[2, m], cols[3, m]

        def chunk(j, sums_):
            plain, weighted, part = sums_
            o = pl.multiple_of(j * 256, 256)
            normed = (hb[1, m, :, pl.ds(o + 128, 256)] - mean) * rstd
            pre = gain2 * normed + shift2
            s = sigmoid(pre)
            low = (pre * s).astype(BF16)
            third = dot(w3[m], low, 0, 0)
            up = c[m, :, pl.ds(o, 256)].astype(F32) * slope(x[m, :, pl.ds(o, 256)].astype(F32) + third)
            u[m, :, pl.ds(o, 256)] = up
            up = up.astype(BF16)
            back = dot(w3[m], up, 1, 0)
            hb[2, m, :, pl.ds(o + 128, 256)] = back
            dpre = back * (s * (1.0 + pre * (1.0 - s)))
            part = part + dot(low, up, 1, 1)
            plain = plain + jnp.sum(dpre, axis=1, keepdims=True)
            weighted = weighted + jnp.sum(dpre * normed, axis=1, keepdims=True)
            return plain, weighted, part

        one = jnp.zeros((64, 1), F32)
        plain, weighted, part = lax.fori_loop(0, 4, chunk, (one, one, jnp.zeros((64, 256), F32)))
        acc = put(put(acc, m, plain), 4 + m, weighted)
        ofm = of[m]
        ef = efc[m]
        scaled = part * ef * ofm
        g[EXPAND : EXPAND + 64] += scaled[:, :128]
        g[EXPAND + 64 : EXPAND + 128] += scaled[:, 128:]
        byw = part * ew[...]
        fac = put(fac, m, jnp.sum(byw * ofm, axis=1, keepdims=True))
        nf[1, m] = jnp.sum(byw * ef, axis=0, keepdims=True)
        return acc, pack(2, m, edge), fac

    acc, edge, fac = lax.fori_loop(0, 4, upstream_of, (zero, zero, zero))
    pk[2] = edge
    wait = reduce_start(2, rows_of_columns(acc))
    halos = halo(2)
    for copy in halos:
        copy.start()
    stats2 = reduce_end(2, wait)
    for copy in halos:
        copy.wait()
    columns_of_rows(stats2, 4)

    def back_of(m, carry):
        acc, fac = carry
        mean, rstd, plain, weighted = cols[2, m], cols[3, m], cols[4, m] / count, cols[5, m] / count

        def dact(second, back):
            normed = (second - mean) * rstd
            dpre = back * slope(gain2 * normed + shift2)
            return gain2 * rstd * (dpre - plain - normed * weighted)

        spread(
            dq, m,
            lambda i: dact(hb[1, m, :, i * 128 : i * 128 + 128], hb[2, m, :, i * 128 : i * 128 + 128]),
            lambda n: dact(pr[1, n], pr[2, n]),
        )
        a = dot(w2b[m, 0], dq[m, :, 0:1024], 1, 0)
        a = a + dot(w2b[m, 1], dq[m, :, 128:1152], 1, 0)
        a = a + dot(w2b[m, 2], dq[m, :, 256:1280], 1, 0)
        normed = (hb[0, m, :, 128:1152] - cols[0, m]) * cols[1, m]
        dpre = a * slope(gain1 * normed + shift1)
        dpre1[m] = dpre
        acc = sums(m, acc, dpre, dpre * normed)

        low = dq[m, 64:128, 128:1152]
        sf = sfc[m]
        byf = jnp.zeros((64, 1), F32)
        halves = []
        for p in range(3):
            part = dot(hq[m, :, p * 128 : p * 128 + 1024], low, 1, 1)
            byw = jnp.sum(part * sw[p * 192 : p * 192 + 192], axis=1, keepdims=True)
            byf = byf + byw[0:64] + byw[64:128] + byw[128:192]
            for q in range(3):
                halves.append(part[q * 64 : q * 64 + 64] * sf)
        whole = jnp.concatenate(halves, axis=0)
        whole = jnp.concatenate([whole[:288], whole[288:]], axis=1)

        @pl.when(m == 0)
        def _():
            g[SPATIAL : SPATIAL + 288] = whole

        @pl.when(m > 0)
        def _():
            g[SPATIAL : SPATIAL + 288] += whole

        return acc, put(fac, 4 + m, byf)

    acc, fac = lax.fori_loop(0, 4, back_of, (zero, fac))
    wait = reduce_start(3, rows_of_columns(acc))
    g[COLUMN_F : COLUMN_F + 8] = rows_of_columns(fac)
    stats1 = reduce_end(3, wait)
    columns_of_rows(stats1, 6)

    def low_of(m, _):
        mean, rstd, plain, weighted = cols[0, m], cols[1, m], cols[6, m] / count, cols[7, m] / count
        normed = (hb[0, m, :, 128:1152] - mean) * rstd
        d = (gain1 * rstd * (dpre1[m] - plain - normed * weighted)).astype(BF16)
        dq[m, 0:64, 0:1024] = d
        part = dot(d, x[m], 1, 1)
        scaled = part * rf[m]
        g[REDUCE : REDUCE + 64] += scaled[:, :128]
        g[REDUCE + 64 : REDUCE + 128] += scaled[:, 128:]
        nf[0, m] = jnp.sum(part * rwt[...], axis=0, keepdims=True)
        return 0

    lax.fori_loop(0, 4, low_of, 0)
    for k, at_row in ((0, REDUCE_F), (1, OUTPUT_F)):
        g[at_row : at_row + 8] = jnp.concatenate(
            [nf[k, m, :, h * 128 : h * 128 + 128] for h in range(2) for m in range(4)], axis=0
        )

    def chunk_of(d):
        return g.at[pl.ds(pl.multiple_of(lax.rem(rank_a + d, 16) * CHUNK, 8), CHUNK)]

    start, wait = exchange(8, chunk_of, r1, rank_a, peer_a)
    start()

    def grad_of(m, _):
        def chunk(j, _):
            o = pl.multiple_of(j * 256, 256)
            t = dot(w1[m], dq[m, 0:64, pl.ds(o, 256)], 0, 0)
            c[m, :, pl.ds(o, 256)] = (u[m, :, pl.ds(o, 256)] + t).astype(BF16)
            return 0

        lax.fori_loop(0, 4, chunk, 0)
        return 0

    lax.fori_loop(0, 4, grad_of, 0)
    stores = [pltpu.make_async_copy(c.at[m], out_hbm.at[m], st_sem.at[m]) for m in range(4)]
    for copy in stores:
        copy.start()

    wait()
    r1[rank_a] = g[pl.ds(pl.multiple_of(rank_a * CHUNK, 8), CHUNK)]
    r2[rank_b] = total(r1)
    start, wait = exchange(9, lambda d: r2.at[rank_b], r2, rank_b, peer_b)
    start()
    wait()
    r3[rank_a] = total(r2)
    start, wait = exchange(10, lambda d: r3.at[rank_a], r3, rank_a, peer_a)
    start()
    wait()

    def rows(at_row, n):
        return jnp.concatenate(
            [r3[r // CHUNK, r % CHUNK : r % CHUNK + 8] for r in range(at_row, at_row + n, 8)], axis=0
        )

    e = rows(EXPAND, 128)
    o_expand[...] = jnp.concatenate([e[:64], e[64:]], axis=1)
    e = rows(REDUCE, 128)
    o_reduce[...] = jnp.transpose(jnp.concatenate([e[:64], e[64:]], axis=1))
    e = rows(SPATIAL, 288)
    o_spatial[0:288] = e[:, :64]
    o_spatial[288:576] = e[:, 64:]
    e = rows(REDUCE_F, 8)
    o_rf[...] = jnp.concatenate([e[:4], e[4:]], axis=1)
    e = rows(OUTPUT_F, 8)
    o_of[...] = jnp.concatenate([e[:4], e[4:]], axis=1)
    e = rows(COLUMN_F, 8)
    o_ef[...] = e[:4, :64]
    o_sf[...] = e[4:, :64]
    o_norm[...] = jnp.concatenate(
        [
            jnp.sum(stats1[4:8], axis=0, keepdims=True),
            jnp.sum(stats1[0:4], axis=0, keepdims=True),
            jnp.sum(stats2[4:8], axis=0, keepdims=True),
            jnp.sum(stats2[0:4], axis=0, keepdims=True),
        ],
        axis=0,
    )[:, :64]
    for copy in stores:
        copy.wait()


def body(
    features, cotangent, reduce_weight, spatial_weight, expand_weight,
    reduce_factor, spatial_factor, expand_factor, output_factor,
    gain_first, shift_first, gain_second, shift_second,
):
    rw = reduce_weight.astype(F32)
    sw = spatial_weight.astype(F32)
    ew = expand_weight.astype(F32)
    rwt = rw.T
    w1 = (reduce_factor[:, None, :] * rwt[None]).astype(BF16)
    spatial = (spatial_factor[:, None, :, None] * sw[None]).astype(BF16)
    w2 = spatial.reshape(4, 3, 192, 64)
    w2b = spatial.reshape(4, 3, 3, 64, 64)[:, ::-1, ::-1].transpose(0, 1, 3, 2, 4).reshape(4, 3, 64, 192)
    w3 = (expand_factor[:, :, None] * ew[None] * output_factor[:, None, :]).astype(BF16)
    gb = jnp.stack([gain_first, shift_first, gain_second, shift_second])[:, :, None]
    vmem = pl.BlockSpec(memory_space=pltpu.VMEM)
    hbm = pl.BlockSpec(memory_space=pl.ANY)
    sds = jax.ShapeDtypeStruct
    outs = pl.pallas_call(
        kernel,
        out_shape=(
            sds((4, 256, 1024), BF16), sds((256, 64), F32), sds((576, 64), F32), sds((64, 256), F32),
            sds((4, 256), F32), sds((4, 64), F32), sds((4, 64), F32), sds((4, 256), F32), sds((4, 64), F32),
        ),
        in_specs=[hbm, hbm] + [vmem] * 12,
        out_specs=(hbm,) + (vmem,) * 8,
        scratch_shapes=[
            pltpu.VMEM((4, 256, 1024), BF16),
            pltpu.VMEM((4, 256, 1024), BF16),
            pltpu.VMEM((4, 256, 1024), F32),
            pltpu.VMEM((3, 4, 64, 1280), F32),
            pltpu.VMEM((4, 192, 1280), BF16),
            pltpu.VMEM((4, 192, 1280), BF16),
            pltpu.VMEM((4, 64, 1024), F32),
            pltpu.VMEM((2, 4, 1, 256), F32),
            pltpu.VMEM((3, 64, 128), F32),
            pltpu.VMEM((3, 6, 64, 128), F32),
            pltpu.VMEM((4, 16, 8, 128), F32),
            pltpu.VMEM((4, 16, 8, 128), F32),
            pltpu.VMEM((16 * CHUNK, 128), F32),
            pltpu.VMEM((16, CHUNK, 128), F32),
            pltpu.VMEM((16, CHUNK, 128), F32),
            pltpu.VMEM((16, CHUNK, 128), F32),
            pltpu.VMEM((8, 4, 64, 1), F32),
            pltpu.SemaphoreType.DMA((8,)),
            pltpu.SemaphoreType.DMA((4,)),
            pltpu.SemaphoreType.DMA((11, 16)),
            pltpu.SemaphoreType.DMA((11, 16)),
            pltpu.SemaphoreType.DMA((3, 8)),
            pltpu.SemaphoreType.DMA((3, 8)),
        ],
        compiler_params=pltpu.CompilerParams(
            collective_id=0, has_side_effects=True, vmem_limit_bytes=56 * 1024 * 1024
        ),
    )(
        features.reshape(4, 256, 1024), cotangent.reshape(4, 256, 1024), w1, w2, w2b, w3,
        rwt, sw.reshape(576, 64), ew, reduce_factor[:, None, :], output_factor[:, None, :],
        spatial_factor[:, :, None], expand_factor[:, :, None], gb,
    )
    grad, o_reduce, o_spatial, o_expand, o_rf, o_sf, o_ef, o_of, o_norm = outs
    return (
        grad.reshape(4, 256, 8, 128), o_reduce, o_spatial.reshape(9, 64, 64), o_expand,
        o_rf, o_sf, o_ef, o_of, o_norm[0], o_norm[1], o_norm[2], o_norm[3],
    )


def solution(mesh):
    split = Mesh(
        mesh.devices.reshape(2, 4, 8, 2, 2), ("rows_0", "rows_1", "cols_0", "cols_1", "cols_2")
    )
    image = P(None, None, ROWS, COLS)
    return jax.shard_map(
        body,
        mesh=split,
        in_specs=(image, image) + (P(),) * 11,
        out_specs=(image,) + (P(),) * 11,
        check_vma=False,
    )
```

```python
import functools

import jax
import jax.numpy as jnp
from jax import lax
from jax.experimental import pallas as pl
from jax.experimental.pallas import tpu as pltpu
from jax.sharding import Mesh
from jax.sharding import PartitionSpec as P

ROWS = ("rows_0", "rows_1")
COLS = ("cols_0", "cols_1", "cols_2")
MESH = pl.DeviceIdType.MESH
EPSILON = 1e-05
F32 = jnp.float32
BF16 = jnp.bfloat16

CHUNK = 40
EXPAND, REDUCE, SPATIAL, REDUCE_F, OUTPUT_F, COLUMN_F, NORMS = 0, 128, 256, 544, 552, 560, 568


def dot(a, b, ca, cb):
    return lax.dot_general(a, b, (((ca,), (cb,)), ((), ())), preferred_element_type=F32)


def sigmoid(v):
    return 1.0 / (1.0 + jnp.exp(-v))


def silu(v):
    return v * sigmoid(v)


def slope(v):
    s = sigmoid(v)
    return s * (1.0 + v * (1.0 - s))


def lanes(shape):
    return lax.broadcasted_iota(jnp.int32, shape, len(shape) - 1)


def kernel(
    x_hbm, c_hbm, rw_hbm, sw_hbm, ew_hbm, rf_hbm, sf_hbm, ef_hbm, of_hbm, g1_hbm, b1_hbm, g2_hbm, b2_hbm,
    y_hbm, packed,
    xraw, craw, wide, rw, sw, ew, rf, sf, ef, of, g1, b1, g2, b2,
    w1, w2, w2b, w3, rwt,
    x, c, u, hb, hq, dq, dpre1, nf, pk, pr, arb, ara, g, r1, r2, r3, cols,
    ld_sem, st_sem, s_sem, r_sem, hs_sem, hr_sem,
):
    count = float(64 * 4096)
    x_hi, y = lax.axis_index("rows_0"), lax.axis_index("rows_1")
    z, x_lo, core = lax.axis_index("cols_0"), lax.axis_index("cols_1"), lax.axis_index("cols_2")
    row = x_hi * 4 + y
    col = z * 4 + x_lo * 2 + core
    rank_a = x_hi * 8 + x_lo * 4 + y
    rank_b = z * 2 + core

    def peer_a(d):
        a = lax.rem(rank_a + d, 16)
        return (a // 8, lax.rem(a, 4), z, lax.rem(a // 4, 2), core)

    def peer_b(d):
        b = lax.rem(rank_b + d, 16)
        return (x_hi, y, b // 2, x_lo, lax.rem(b, 2))

    def at(dr, dc):
        rr, cc = lax.rem(row + dr + 8, 8), lax.rem(col + dc + 32, 32)
        return (rr // 4, lax.rem(rr, 4), cc // 4, lax.rem(cc // 2, 2), lax.rem(cc, 2))

    sides = ((0, 1), (0, -1), (1, 1), (1, -1), (-1, 1), (-1, -1))

    pairs = (
        (rw_hbm, rw), (rf_hbm, rf), (sw_hbm, sw), (ew_hbm, ew), (sf_hbm, sf), (ef_hbm, ef), (of_hbm, of),
        (g1_hbm, g1), (b1_hbm, b1), (g2_hbm, g2), (b2_hbm, b2),
    )
    load_w = [pltpu.make_async_copy(a, b, ld_sem.at[8 + n]) for n, (a, b) in enumerate(pairs)]
    load_x = [pltpu.make_async_copy(x_hbm.at[m], xraw.at[m], ld_sem.at[m]) for m in range(4)]
    load_c = [pltpu.make_async_copy(c_hbm.at[m], craw.at[m], ld_sem.at[4 + m]) for m in range(4)]
    for copy in load_w[:2] + load_x + load_w[2:] + load_c:
        copy.start()

    barrier = pltpu.get_barrier_semaphore()

    def greet(d, _):
        pl.semaphore_signal(barrier, inc=1, device_id=peer_a(d), device_id_type=MESH)
        pl.semaphore_signal(barrier, inc=1, device_id=peer_b(d), device_id_type=MESH)
        return 0

    lax.fori_loop(1, 16, greet, 0)
    for side in sides:
        pl.semaphore_signal(barrier, inc=1, device_id=at(*side), device_id_type=MESH)

    def exchange(stage, src, buf, rank, peer):
        def copy(d):
            return pltpu.make_async_remote_copy(
                src_ref=src(d), dst_ref=buf.at[rank], send_sem=s_sem.at[stage, d],
                recv_sem=r_sem.at[stage, d], device_id=peer(d), device_id_type=MESH,
            )

        def start(d, _):
            copy(d).start()
            return 0

        def wait(d, _):
            copy(d).wait()
            return 0

        return (lambda: lax.fori_loop(1, 16, start, 0)), (lambda: lax.fori_loop(1, 16, wait, 0))

    def total(buf):
        t = buf[0]
        for k in range(1, 16):
            t = t + buf[k]
        return t

    def reduce_start(k, tile):
        arb[k, rank_b] = tile
        start, wait = exchange(2 * k, lambda d: arb.at[k, rank_b], arb.at[k], rank_b, peer_b)
        start()
        return wait

    def reduce_end(k, wait):
        wait()
        ara[k, rank_a] = total(arb.at[k])
        start, wait = exchange(2 * k + 1, lambda d: ara.at[k, rank_a], ara.at[k], rank_a, peer_a)
        start()
        wait()
        return total(ara.at[k])

    def halo(k):
        copies = [
            pltpu.make_async_remote_copy(
                src_ref=hb.at[k, :, :, pl.ds(128, 128)], dst_ref=hb.at[k, :, :, pl.ds(1152, 128)],
                send_sem=hs_sem.at[k, 6], recv_sem=hr_sem.at[k, 6],
                device_id=at(-1, 0), device_id_type=MESH,
            ),
            pltpu.make_async_remote_copy(
                src_ref=hb.at[k, :, :, pl.ds(1024, 128)], dst_ref=hb.at[k, :, :, pl.ds(0, 128)],
                send_sem=hs_sem.at[k, 7], recv_sem=hr_sem.at[k, 7],
                device_id=at(1, 0), device_id_type=MESH,
            ),
        ]
        for n, side in enumerate(sides):
            copies.append(
                pltpu.make_async_remote_copy(
                    src_ref=pk.at[k], dst_ref=pr.at[k, n], send_sem=hs_sem.at[k, n],
                    recv_sem=hr_sem.at[k, n], device_id=at(*side), device_id_type=MESH,
                )
            )
        return copies

    lane = lanes((64, 128))

    def put(acc, n, value):
        return jnp.where(lane == n, value, acc)

    def rows_of_columns(acc):
        return jnp.transpose(jnp.concatenate([acc, jnp.zeros((64, 128), F32)], axis=0))[:8]

    def columns_of_rows(tile, k):
        t = jnp.transpose(jnp.concatenate([tile, jnp.zeros((120, 128), F32)], axis=0))
        for m in range(4):
            cols[k, m] = t[:64, m : m + 1]
            cols[k + 1, m] = t[:64, 4 + m : 5 + m]

    def sums(m, acc, a, b):
        acc = put(acc, m, jnp.sum(a, axis=1, keepdims=True))
        return put(acc, 4 + m, jnp.sum(b, axis=1, keepdims=True))

    def pack(k, m, acc):
        for i in range(8):
            t = hb[k, m, :, 128 + i * 128 : 256 + i * 128]
            acc = put(acc, m * 8 + i, t[:, 0:1])
            acc = put(acc, 32 + m * 8 + i, t[:, 127:128])
        return acc

    top = jnp.where(row > 0, 1.0, 0.0).astype(F32)
    bottom = jnp.where(row < 7, 1.0, 0.0).astype(F32)
    left = jnp.where(col > 0, 1.0, 0.0).astype(F32)
    right = jnp.where(col < 31, 1.0, 0.0).astype(F32)
    masks = (left, right, top * left, top * right, bottom * left, bottom * right)

    def spread(dst, m, tile, edge):
        edges = [edge(n) * masks[n] for n in range(6)]
        for i in range(10):
            t = tile(i)
            if i == 0:
                t, e0, e2, at_row = t * top, edges[2], edges[3], 7
            elif i == 9:
                t, e0, e2, at_row = t * bottom, edges[4], edges[5], 0
            else:
                e0, e2, at_row = edges[0], edges[1], i - 1
            where0 = 32 + m * 8 + at_row
            where2 = m * 8 + at_row
            before = jnp.where(
                lane == 0, pltpu.roll(e0, 128 - where0, axis=1), pltpu.roll(t, 1, axis=1)
            )
            after = jnp.where(
                lane == 127, pltpu.roll(e2, 127 - where2, axis=1), pltpu.roll(t, 127, axis=1)
            )
            span = slice(i * 128, i * 128 + 128)
            dst[m, 0:64, span] = before.astype(BF16)
            dst[m, 64:128, span] = t.astype(BF16)
            dst[m, 128:192, span] = after.astype(BF16)

    zero = jnp.zeros((64, 128), F32)

    def flatten(src, dst, m):
        wide[...] = src[m].astype(F32).reshape(2048, 128)
        for i in range(8):
            dst[m, :, i * 128 : i * 128 + 128] = wide[pl.ds(i, 256, stride=8), :].astype(BF16)

    def first_of(m, carry):
        acc, edge = carry
        flatten(xraw, x, m)
        a = dot(w1[m], x[m], 1, 0)
        hb[0, m, :, 128:1152] = a
        return sums(m, acc, a, a * a), pack(0, m, edge)

    for copy in load_w[:2]:
        copy.wait()
    rwt[...] = rw[...].astype(F32)
    for m in range(4):
        w1[m] = (rwt[...] * rf[m : m + 1]).astype(BF16)
    for copy in load_x:
        copy.wait()
    acc, edge = lax.fori_loop(0, 4, first_of, (zero, zero))
    pk[0] = edge
    pl.semaphore_wait(barrier, 36)
    wait = reduce_start(0, rows_of_columns(acc))
    halos = halo(0)
    for copy in halos:
        copy.start()
    for copy in load_w[2:]:
        copy.wait()
    lines = jnp.zeros((4, 64), F32)
    columns_of_rows(
        jnp.concatenate(
            [jnp.concatenate([sf[...], ef[...]], axis=0), jnp.zeros((8, 64), F32)], axis=1
        ), 8,
    )
    columns_of_rows(
        jnp.concatenate(
            [jnp.concatenate([g1[...], b1[...], g2[...], b2[...], lines], axis=0), jnp.zeros((8, 64), F32)], axis=1
        ), 10,
    )
    for m in range(4):
        sfm, efm = cols[8, m], cols[9, m]
        w3[m] = (efm * ew[...].astype(F32) * of[m : m + 1]).astype(BF16)
        for p in range(3):
            taps = [(sfm * sw[3 * p + q].astype(F32)).astype(BF16) for q in range(3)]
            for q in range(3):
                w2[m, p, q * 64 : q * 64 + 64] = taps[q]
            w2b[m, 2 - p] = jnp.concatenate(taps[::-1], axis=1)
    for copy in load_c:
        copy.wait()

    def flatten_c(m, _):
        flatten(craw, c, m)
        return 0

    lax.fori_loop(0, 4, flatten_c, 0)
    stats = reduce_end(0, wait)
    for copy in halos:
        copy.wait()

    def moments(k, tile):
        columns_of_rows(tile, k)
        for m in range(4):
            mean = cols[k, m] / count
            var = cols[k + 1, m] / count - mean * mean
            cols[k, m] = mean
            cols[k + 1, m] = lax.rsqrt(var + EPSILON)

    moments(0, stats)
    gain1, shift1, gain2, shift2 = (cols[10, n] for n in range(4))

    def second_of(m, carry):
        acc, edge = carry
        mean, rstd = cols[0, m], cols[1, m]

        def hidden(v):
            return silu(gain1 * ((v - mean) * rstd) + shift1)

        spread(
            hq, m, lambda i: hidden(hb[0, m, :, i * 128 : i * 128 + 128]),
            lambda n: hidden(pr[0, n]),
        )
        a = dot(w2[m, 0], hq[m, :, 0:1024], 0, 0)
        a = a + dot(w2[m, 1], hq[m, :, 128:1152], 0, 0)
        a = a + dot(w2[m, 2], hq[m, :, 256:1280], 0, 0)
        hb[1, m, :, 128:1152] = a
        return sums(m, acc, a, a * a), pack(1, m, edge)

    acc, edge = lax.fori_loop(0, 4, second_of, (zero, zero))
    pk[1] = edge
    wait = reduce_start(1, rows_of_columns(acc))
    halos = halo(1)
    for copy in halos:
        copy.start()
    stats = reduce_end(1, wait)
    for copy in halos:
        copy.wait()
    moments(2, stats)

    g[EXPAND : EXPAND + 128] = jnp.zeros((128, 128), F32)
    g[REDUCE : REDUCE + 128] = jnp.zeros((128, 128), F32)
    g[568:640] = jnp.zeros((72, 128), F32)

    def upstream_of(m, carry):
        acc, edge, fac = carry
        mean, rstd = cols[2, m], cols[3, m]

        def chunk(j, sums_):
            plain, weighted, part = sums_
            o = pl.multiple_of(j * 256, 256)
            normed = (hb[1, m, :, pl.ds(o + 128, 256)] - mean) * rstd
            pre = gain2 * normed + shift2
            s = sigmoid(pre)
            low = (pre * s).astype(BF16)
            third = dot(w3[m], low, 0, 0)
            up = c[m, :, pl.ds(o, 256)].astype(F32) * slope(x[m, :, pl.ds(o, 256)].astype(F32) + third)
            u[m, :, pl.ds(o, 256)] = up
            up = up.astype(BF16)
            back = dot(w3[m], up, 1, 0)
            hb[2, m, :, pl.ds(o + 128, 256)] = back
            dpre = back * (s * (1.0 + pre * (1.0 - s)))
            part = part + dot(low, up, 1, 1)
            plain = plain + jnp.sum(dpre, axis=1, keepdims=True)
            weighted = weighted + jnp.sum(dpre * normed, axis=1, keepdims=True)
            return plain, weighted, part

        one = jnp.zeros((64, 1), F32)
        plain, weighted, part = lax.fori_loop(0, 4, chunk, (one, one, jnp.zeros((64, 256), F32)))
        acc = put(put(acc, m, plain), 4 + m, weighted)
        ofm = of[pl.ds(m, 1), :]
        efm = cols[9, m]
        scaled = part * efm * ofm
        g[EXPAND : EXPAND + 64] += scaled[:, :128]
        g[EXPAND + 64 : EXPAND + 128] += scaled[:, 128:]
        byw = part * ew[...].astype(F32)
        fac = put(fac, m, jnp.sum(byw * ofm, axis=1, keepdims=True))
        nf[1, m] = jnp.sum(byw * efm, axis=0, keepdims=True)
        return acc, pack(2, m, edge), fac

    acc, edge, fac = lax.fori_loop(0, 4, upstream_of, (zero, zero, zero))
    pk[2] = edge
    wait = reduce_start(2, rows_of_columns(acc))
    halos = halo(2)
    for copy in halos:
        copy.start()
    stats2 = reduce_end(2, wait)
    for copy in halos:
        copy.wait()
    columns_of_rows(stats2, 4)

    def back_of(m, carry):
        acc, fac = carry
        mean, rstd, plain, weighted = cols[2, m], cols[3, m], cols[4, m] / count, cols[5, m] / count

        def dact(second, back):
            normed = (second - mean) * rstd
            dpre = back * slope(gain2 * normed + shift2)
            return gain2 * rstd * (dpre - plain - normed * weighted)

        spread(
            dq, m,
            lambda i: dact(hb[1, m, :, i * 128 : i * 128 + 128], hb[2, m, :, i * 128 : i * 128 + 128]),
            lambda n: dact(pr[1, n], pr[2, n]),
        )
        a = dot(w2b[m, 0], dq[m, :, 0:1024], 1, 0)
        a = a + dot(w2b[m, 1], dq[m, :, 128:1152], 1, 0)
        a = a + dot(w2b[m, 2], dq[m, :, 256:1280], 1, 0)
        normed = (hb[0, m, :, 128:1152] - cols[0, m]) * cols[1, m]
        dpre = a * slope(gain1 * normed + shift1)
        dpre1[m] = dpre
        acc = sums(m, acc, dpre, dpre * normed)

        low = dq[m, 64:128, 128:1152]
        sfm = cols[8, m]
        byf = jnp.zeros((64, 1), F32)
        halves = []
        for p in range(3):
            part = dot(hq[m, :, p * 128 : p * 128 + 1024], low, 1, 1)
            for q in range(3):
                tap = part[q * 64 : q * 64 + 64]
                byf = byf + jnp.sum(tap * sw[3 * p + q].astype(F32), axis=1, keepdims=True)
                halves.append(tap * sfm)
        whole = jnp.concatenate(halves, axis=0)
        whole = jnp.concatenate([whole[:288], whole[288:]], axis=1)

        @pl.when(m == 0)
        def _():
            g[SPATIAL : SPATIAL + 288] = whole

        @pl.when(m > 0)
        def _():
            g[SPATIAL : SPATIAL + 288] += whole

        return acc, put(fac, 4 + m, byf)

    acc, fac = lax.fori_loop(0, 4, back_of, (zero, fac))
    wait = reduce_start(3, rows_of_columns(acc))
    g[COLUMN_F : COLUMN_F + 8] = rows_of_columns(fac)
    stats1 = reduce_end(3, wait)
    columns_of_rows(stats1, 6)

    def low_of(m, _):
        mean, rstd, plain, weighted = cols[0, m], cols[1, m], cols[6, m] / count, cols[7, m] / count
        normed = (hb[0, m, :, 128:1152] - mean) * rstd
        d = (gain1 * rstd * (dpre1[m] - plain - normed * weighted)).astype(BF16)
        dq[m, 0:64, 0:1024] = d
        part = dot(d, x[m], 1, 1)
        scaled = part * rf[pl.ds(m, 1), :]
        g[REDUCE : REDUCE + 64] += scaled[:, :128]
        g[REDUCE + 64 : REDUCE + 128] += scaled[:, 128:]
        nf[0, m] = jnp.sum(part * rwt[...], axis=0, keepdims=True)
        return 0

    lax.fori_loop(0, 4, low_of, 0)
    for k, at_row in ((0, REDUCE_F), (1, OUTPUT_F)):
        g[at_row : at_row + 8] = jnp.concatenate(
            [nf[k, m, :, h * 128 : h * 128 + 128] for h in range(2) for m in range(4)], axis=0
        )

    def chunk_of(d):
        return g.at[pl.ds(pl.multiple_of(lax.rem(rank_a + d, 16) * CHUNK, 8), CHUNK)]

    start, wait = exchange(8, chunk_of, r1, rank_a, peer_a)
    start()

    def grad_of(m, _):
        for j in range(4):
            o = j * 256
            t = u[m, :, o : o + 256] + dot(w1[m], dq[m, 0:64, o : o + 256], 0, 0)
            wide[pl.ds(2 * j, 256, stride=8), :] = t[:, :128]
            wide[pl.ds(2 * j + 1, 256, stride=8), :] = t[:, 128:]
        craw[m] = wide[...].reshape(256, 8, 128).astype(BF16)
        return 0

    lax.fori_loop(0, 4, grad_of, 0)
    stores = [pltpu.make_async_copy(craw.at[m], y_hbm.at[m], st_sem.at[m]) for m in range(4)]
    for copy in stores:
        copy.start()

    wait()
    r1[rank_a] = g[pl.ds(pl.multiple_of(rank_a * CHUNK, 8), CHUNK)]
    r2[rank_b] = total(r1)
    start, wait = exchange(9, lambda d: r2.at[rank_b], r2, rank_b, peer_b)
    start()
    wait()
    r3[rank_a] = total(r2)
    start, wait = exchange(10, lambda d: r3.at[rank_a], r3, rank_a, peer_a)
    start()
    wait()

    for r in range(0, 640, 8):
        packed[r : r + 8] = r3[r // CHUNK, r % CHUNK : r % CHUNK + 8]
    packed[NORMS : NORMS + 8] = jnp.concatenate(
        [
            jnp.sum(stats1[4:8], axis=0, keepdims=True),
            jnp.sum(stats1[0:4], axis=0, keepdims=True),
            jnp.sum(stats2[4:8], axis=0, keepdims=True),
            jnp.sum(stats2[0:4], axis=0, keepdims=True),
            jnp.zeros((4, 128), F32),
        ],
        axis=0,
    )
    for copy in stores:
        copy.wait()


def unpack(
    y_hbm, packed_hbm,
    out_hbm, o_reduce, o_spatial, o_expand, o_rf, o_sf, o_ef, o_of, o_g1, o_b1, o_g2, o_b2,
    y, packed, sem,
):
    load = [pltpu.make_async_copy(packed_hbm, packed, sem.at[0])]
    load += [pltpu.make_async_copy(y_hbm.at[m], y.at[m], sem.at[1 + m]) for m in range(4)]
    store = [pltpu.make_async_copy(y.at[m], out_hbm.at[m], sem.at[5 + m]) for m in range(4)]
    for copy in load:
        copy.start()
    load[0].wait()
    o_expand[:, :128] = packed[EXPAND : EXPAND + 64]
    o_expand[:, 128:] = packed[EXPAND + 64 : EXPAND + 128]
    o_reduce[:, :128] = packed[REDUCE : REDUCE + 64]
    o_reduce[:, 128:] = packed[REDUCE + 64 : REDUCE + 128]
    for k in range(9):
        r = k * 64
        for t in range(r, r + 64, 32):
            at_row = SPATIAL + t % 288
            half = slice(0, 64) if t < 288 else slice(64, 128)
            o_spatial[k, t - r : t - r + 32] = packed[at_row : at_row + 32, half]
    for o, at_row in ((o_rf, REDUCE_F), (o_of, OUTPUT_F)):
        o[:, :128] = packed[at_row : at_row + 4]
        o[:, 128:] = packed[at_row + 4 : at_row + 8]
    o_ef[...] = packed[COLUMN_F : COLUMN_F + 4, :64]
    o_sf[...] = packed[COLUMN_F + 4 : COLUMN_F + 8, :64]
    for n, o in enumerate((o_g1, o_b1, o_g2, o_b2)):
        o[...] = packed[NORMS + n : NORMS + n + 1, :64]
    for m in range(4):
        load[1 + m].wait()
        store[m].start()
    for copy in store:
        copy.wait()


def body(
    features, cotangent, reduce_weight, spatial_weight, expand_weight,
    reduce_factor, spatial_factor, expand_factor, output_factor,
    gain_first, shift_first, gain_second, shift_second,
):
    vmem = pl.BlockSpec(memory_space=pltpu.VMEM)
    hbm = pl.BlockSpec(memory_space=pl.ANY)
    sds = jax.ShapeDtypeStruct
    y, packed = pl.pallas_call(
        kernel,
        out_shape=(sds((4, 256, 8, 128), BF16), sds((16 * CHUNK, 128), F32)),
        in_specs=[hbm] * 13,
        out_specs=(hbm, vmem),
        scratch_shapes=[
            pltpu.VMEM((4, 256, 8, 128), BF16),
            pltpu.VMEM((4, 256, 8, 128), BF16),
            pltpu.VMEM((2048, 128), F32),
            pltpu.VMEM((64, 256), BF16),
            pltpu.VMEM((9, 64, 64), BF16),
            pltpu.VMEM((64, 256), BF16),
            pltpu.VMEM((4, 256), F32),
            pltpu.VMEM((4, 64), F32),
            pltpu.VMEM((4, 64), F32),
            pltpu.VMEM((4, 256), F32),
            pltpu.VMEM((1, 64), F32),
            pltpu.VMEM((1, 64), F32),
            pltpu.VMEM((1, 64), F32),
            pltpu.VMEM((1, 64), F32),
            pltpu.VMEM((4, 64, 256), BF16),
            pltpu.VMEM((4, 3, 192, 64), BF16),
            pltpu.VMEM((4, 3, 64, 192), BF16),
            pltpu.VMEM((4, 64, 256), BF16),
            pltpu.VMEM((64, 256), F32),
            pltpu.VMEM((4, 256, 1024), BF16),
            pltpu.VMEM((4, 256, 1024), BF16),
            pltpu.VMEM((4, 256, 1024), F32),
            pltpu.VMEM((3, 4, 64, 1280), F32),
            pltpu.VMEM((4, 192, 1280), BF16),
            pltpu.VMEM((4, 192, 1280), BF16),
            pltpu.VMEM((4, 64, 1024), F32),
            pltpu.VMEM((2, 4, 1, 256), F32),
            pltpu.VMEM((3, 64, 128), F32),
            pltpu.VMEM((3, 6, 64, 128), F32),
            pltpu.VMEM((4, 16, 8, 128), F32),
            pltpu.VMEM((4, 16, 8, 128), F32),
            pltpu.VMEM((16 * CHUNK, 128), F32),
            pltpu.VMEM((16, CHUNK, 128), F32),
            pltpu.VMEM((16, CHUNK, 128), F32),
            pltpu.VMEM((16, CHUNK, 128), F32),
            pltpu.VMEM((12, 4, 64, 1), F32),
            pltpu.SemaphoreType.DMA((20,)),
            pltpu.SemaphoreType.DMA((4,)),
            pltpu.SemaphoreType.DMA((11, 16)),
            pltpu.SemaphoreType.DMA((11, 16)),
            pltpu.SemaphoreType.DMA((3, 8)),
            pltpu.SemaphoreType.DMA((3, 8)),
        ],
        compiler_params=pltpu.CompilerParams(
            collective_id=0, has_side_effects=True, vmem_limit_bytes=67043328
        ),
        name="step",
    )(
        features, cotangent, reduce_weight.T, spatial_weight, expand_weight,
        reduce_factor, spatial_factor, expand_factor, output_factor,
        gain_first.reshape(1, 64), shift_first.reshape(1, 64),
        gain_second.reshape(1, 64), shift_second.reshape(1, 64),
    )
    outs = pl.pallas_call(
        unpack,
        out_shape=(
            sds((4, 256, 8, 128), BF16), sds((64, 256), F32), sds((9, 64, 64), F32), sds((64, 256), F32),
            sds((4, 256), F32), sds((4, 64), F32), sds((4, 64), F32), sds((4, 256), F32),
        ) + (sds((1, 64), F32),) * 4,
        in_specs=[hbm, hbm],
        out_specs=(hbm,) + (vmem,) * 11,
        scratch_shapes=[
            pltpu.VMEM((4, 256, 8, 128), BF16),
            pltpu.VMEM((16 * CHUNK, 128), F32),
            pltpu.SemaphoreType.DMA((9,)),
        ],
        compiler_params=pltpu.CompilerParams(vmem_limit_bytes=67043328),
        name="unpack",
    )(y, packed)
    return (outs[0], outs[1].T) + outs[2:8] + tuple(o.reshape(64) for o in outs[8:])


def solution(mesh):
    split = Mesh(
        mesh.devices.reshape(2, 4, 8, 2, 2), ("rows_0", "rows_1", "cols_0", "cols_1", "cols_2")
    )
    image = P(None, None, ROWS, COLS)
    return jax.shard_map(
        body,
        mesh=split,
        in_specs=(image, image) + (P(),) * 11,
        out_specs=(image,) + (P(),) * 11,
        check_vma=False,
    )
```

```python
import functools

import jax
import jax.numpy as jnp
from jax import lax
from jax.experimental import pallas as pl
from jax.experimental.pallas import tpu as pltpu
from jax.sharding import Mesh
from jax.sharding import PartitionSpec as P

ROWS = ("rows_0", "rows_1")
COLS = ("cols_0", "cols_1", "cols_2")
MESH = pl.DeviceIdType.MESH
EPSILON = 1e-05
F32 = jnp.float32
BF16 = jnp.bfloat16

SHARE, WITH_PART = 40, 48
REDUCE_F, OUTPUT_F, COLUMN_F, TILES = 36, 37, 38, 48
NORMS = 16 * WITH_PART


def other(t):
    return t % 16, 16 + 8 * (t // 16)


def dot(a, b, ca, cb):
    return lax.dot_general(a, b, (((ca,), (cb,)), ((), ())), preferred_element_type=F32)


def sigmoid(v):
    return 0.5 + 0.5 * jnp.tanh(0.5 * v)


def silu(v):
    return v * sigmoid(v)


def slope(v):
    s = sigmoid(v)
    return s * (1.0 + v * (1.0 - s))


def total(buf):
    t = buf[0]
    for k in range(1, 16):
        t = t + buf[k]
    return t


def kernel(
    x_hbm, c_hbm, rw_hbm, sw_hbm, ew_hbm, rf_hbm, sf_hbm, ef_hbm, of_hbm, g1_hbm, b1_hbm, g2_hbm, b2_hbm,
    y_hbm, packed,
    xraw, craw, wide, rw, sw, ew, rf, sf, ef, of, g1, b1, g2, b2,
    w1, w2, w2b, w3, rwt,
    x, c, u, ulow, h2, hb, hq, dq, dpre1, nf, pk, pr, arb, ara,
    acce, accr, accs, sxs, bn, bn1, bn2, bnc, g, r1, r2, r3, cols,
    ld_sem, st_sem, s_sem, r_sem, hs_sem, hr_sem,
):
    count = float(64 * 4096)
    x_hi, y = lax.axis_index("rows_0"), lax.axis_index("rows_1")
    z, x_lo, core = lax.axis_index("cols_0"), lax.axis_index("cols_1"), lax.axis_index("cols_2")
    row = x_hi * 4 + y
    col = z * 4 + x_lo * 2 + core
    rank_a = x_hi * 8 + x_lo * 4 + y
    rank_b = z * 2 + core

    def peer_a(d):
        a = lax.rem(rank_a + d, 16)
        return (lax.div(a, 8), lax.rem(a, 4), z, lax.rem(lax.div(a, 4), 2), core)

    def peer_b(d):
        b = lax.rem(rank_b + d, 16)
        return (x_hi, y, lax.div(b, 2), x_lo, lax.rem(b, 2))

    def at(dr, dc):
        rr, cc = lax.rem(row + dr + 8, 8), lax.rem(col + dc + 32, 32)
        return (lax.div(rr, 4), lax.rem(rr, 4), lax.div(cc, 4), lax.rem(lax.div(cc, 2), 2), lax.rem(cc, 2))

    sides = ((0, 1), (0, -1), (1, 1), (1, -1), (-1, 1), (-1, -1))

    pairs = (
        (rw_hbm, rw), (rf_hbm, rf), (sw_hbm, sw), (ew_hbm, ew), (sf_hbm, sf), (ef_hbm, ef), (of_hbm, of),
        (g1_hbm, g1), (b1_hbm, b1), (g2_hbm, g2), (b2_hbm, b2),
    )
    load_w = [pltpu.make_async_copy(a, b, ld_sem.at[8 + n]) for n, (a, b) in enumerate(pairs)]
    load_x = [pltpu.make_async_copy(x_hbm.at[m], xraw.at[m], ld_sem.at[m]) for m in range(4)]
    load_c = [pltpu.make_async_copy(c_hbm.at[m], craw.at[m], ld_sem.at[4 + m]) for m in range(4)]
    for copy in load_w[:2] + load_x + load_w[2:] + load_c:
        copy.start()

    barrier = pltpu.get_barrier_semaphore()

    def greet(d, _):
        pl.semaphore_signal(barrier, inc=1, device_id=peer_a(d), device_id_type=MESH)
        pl.semaphore_signal(barrier, inc=1, device_id=peer_b(d), device_id_type=MESH)
        return 0

    lax.fori_loop(1, 16, greet, 0)
    for side in sides:
        pl.semaphore_signal(barrier, inc=1, device_id=at(*side), device_id_type=MESH)

    def exchange(stage, src, buf, rank, peer):
        def copy(d):
            return pltpu.make_async_remote_copy(
                src_ref=src(d), dst_ref=buf.at[rank], send_sem=s_sem.at[stage, d],
                recv_sem=r_sem.at[stage, d], device_id=peer(d), device_id_type=MESH,
            )

        def start(d, _):
            copy(d).start()
            return 0

        def wait(d, _):
            copy(d).wait()
            return 0

        lax.fori_loop(1, 16, start, 0)
        return lambda: lax.fori_loop(1, 16, wait, 0)

    def sum_start(k, n, tile):
        arb[2 * k + n, rank_b] = tile
        return exchange(
            4 * k + 2 * n, lambda d: arb.at[2 * k + n, rank_b], arb.at[2 * k + n], rank_b, peer_b
        )

    def sum_middle(k, n, wait):
        wait()
        ara[2 * k + n, rank_a] = total(arb.at[2 * k + n])
        return exchange(
            4 * k + 2 * n + 1, lambda d: ara.at[2 * k + n, rank_a], ara.at[2 * k + n], rank_a, peer_a
        )

    def sum_end(k, n, wait):
        wait()
        return total(ara.at[2 * k + n])

    def halo(k, n):
        members = pl.ds(2 * n, 2)
        copies = [
            pltpu.make_async_remote_copy(
                src_ref=hb.at[k, members, :, pl.ds(128, 128)],
                dst_ref=hb.at[k, members, :, pl.ds(1152, 128)],
                send_sem=hs_sem.at[2 * k + n, 6], recv_sem=hr_sem.at[2 * k + n, 6],
                device_id=at(-1, 0), device_id_type=MESH,
            ),
            pltpu.make_async_remote_copy(
                src_ref=hb.at[k, members, :, pl.ds(1024, 128)],
                dst_ref=hb.at[k, members, :, pl.ds(0, 128)],
                send_sem=hs_sem.at[2 * k + n, 7], recv_sem=hr_sem.at[2 * k + n, 7],
                device_id=at(1, 0), device_id_type=MESH,
            ),
        ]
        for e, side in enumerate(sides):
            copies.append(
                pltpu.make_async_remote_copy(
                    src_ref=pk.at[k, n], dst_ref=pr.at[k, n, e], send_sem=hs_sem.at[2 * k + n, e],
                    recv_sem=hr_sem.at[2 * k + n, e], device_id=at(*side), device_id_type=MESH,
                )
            )
        for copy in copies:
            copy.start()
        return copies

    lane = lax.broadcasted_iota(jnp.int32, (64, 128), 1)
    sub = lax.broadcasted_iota(jnp.int32, (8, 128), 0)
    zero = jnp.zeros((64, 128), F32)

    def put(acc, n, value):
        return jnp.where(lane == n, value, acc)

    def rows_of_columns(acc):
        return jnp.transpose(jnp.concatenate([acc, jnp.zeros((64, 128), F32)], axis=0))[:8]

    def columns_of_rows(tile, k, members):
        t = jnp.transpose(jnp.concatenate([tile, jnp.zeros((120, 128), F32)], axis=0))
        for m in members:
            cols[k, m] = t[:64, m : m + 1]
            cols[k + 1, m] = t[:64, 4 + m : 5 + m]

    def sums(m, acc, a, b):
        acc = put(acc, m, jnp.sum(a, axis=1, keepdims=True))
        return put(acc, 4 + m, jnp.sum(b, axis=1, keepdims=True))

    def pack(k, n):
        acc = zero
        for m in group(n):
            for i in range(8):
                t = hb[k, m, :, 128 + i * 128 : 256 + i * 128]
                acc = put(acc, m * 8 + i, t[:, 0:1])
                acc = put(acc, 32 + m * 8 + i, t[:, 127:128])
        pk[k, n] = acc

    def group(n):
        return (2 * n, 2 * n + 1)

    top = jnp.where(row > 0, 1.0, 0.0).astype(F32)
    bottom = jnp.where(row < 7, 1.0, 0.0).astype(F32)
    left = jnp.where(col > 0, 1.0, 0.0).astype(F32)
    right = jnp.where(col < 31, 1.0, 0.0).astype(F32)
    masks = (left, right, top * left, top * right, bottom * left, bottom * right)

    def spread(dst, m, tile, edge):
        edges = [edge(e) * masks[e] for e in range(6)]
        for i in range(10):
            t = tile(i)
            if i == 0:
                t, e0, e2, at_row = t * top, edges[2], edges[3], 7
            elif i == 9:
                t, e0, e2, at_row = t * bottom, edges[4], edges[5], 0
            else:
                e0, e2, at_row = edges[0], edges[1], i - 1
            where0 = 32 + m * 8 + at_row
            where2 = m * 8 + at_row
            before = jnp.where(
                lane == 0, pltpu.roll(e0, 128 - where0, axis=1), pltpu.roll(t, 1, axis=1)
            )
            after = jnp.where(
                lane == 127, pltpu.roll(e2, 127 - where2, axis=1), pltpu.roll(t, 127, axis=1)
            )
            span = slice(i * 128, i * 128 + 128)
            dst[m, 0:64, span] = before.astype(BF16)
            dst[m, 64:128, span] = t.astype(BF16)
            dst[m, 128:192, span] = after.astype(BF16)

    def flatten(src, dst, m):
        wide[m % 2] = src[m].astype(F32).reshape(2048, 128)
        for i in range(8):
            dst[m, :, i * 128 : i * 128 + 128] = wide[m % 2, pl.ds(i, 256, stride=8), :].astype(BF16)

    def moments(k, tile, members):
        columns_of_rows(tile, k, members)
        for m in members:
            mean = cols[k, m] / count
            var = cols[k + 1, m] / count - mean * mean
            cols[k, m] = mean
            cols[k + 1, m] = lax.rsqrt(var + EPSILON)

    for copy in load_w[:2]:
        copy.wait()
    rwt[...] = rw[...].astype(F32)
    for m in range(4):
        w1[m] = (rwt[...] * rf[m : m + 1]).astype(BF16)
    ones = jnp.ones((8, 1024), BF16)

    def free_rows(m):
        base = 2 if m < 2 else 0
        return (base + 4 * (m % 2), base + 4 * (m % 2) + 1)

    stats, halos = [None, None], [None, None]
    for n in range(2):
        acc = zero
        extra = []
        for m in group(n):
            load_x[m].wait()
            flatten(xraw, x, m)
            a = dot(w1[m], x[m], 1, 0)
            hb[0, m, :, 128:1152] = a
            acc = sums(m, acc, a, a * a)
            extra.append((m, dot(ones, x[m], 1, 1)))
        pack(0, n)
        tile = rows_of_columns(acc)
        for m, e in extra:
            for h, r in enumerate(free_rows(m)):
                tile = jnp.where(sub == r, e[:, h * 128 : h * 128 + 128], tile)
        if n == 0:
            pl.semaphore_wait(barrier, 36)
        stats[n] = sum_start(0, n, tile)
        halos[n] = halo(0, n)

    for copy in load_w[2:]:
        copy.wait()
    tail = jnp.zeros((8, 64), F32)
    columns_of_rows(
        jnp.concatenate([jnp.concatenate([sf[...], ef[...]], axis=0), tail], axis=1), 8, range(4)
    )
    columns_of_rows(
        jnp.concatenate(
            [jnp.concatenate([g1[...], b1[...], g2[...], b2[...], tail[:4]], axis=0), tail], axis=1
        ), 10, range(4),
    )
    for m in range(4):
        sfm, efm = cols[8, m], cols[9, m]
        w3[m] = (efm * ew[...].astype(F32) * of[m : m + 1]).astype(BF16)
        for p in range(3):
            taps = [(sfm * sw[3 * p + q].astype(F32)).astype(BF16) for q in range(3)]
            for q in range(3):
                w2[m, p, q * 64 : q * 64 + 64] = taps[q]
            w2b[m, 2 - p] = jnp.concatenate(taps[::-1], axis=1)
    gain1, shift1, gain2, shift2 = (cols[10, n] for n in range(4))
    for copy in load_c:
        copy.wait()
    for m in range(2):
        flatten(craw, c, m)
    stats[0] = sum_middle(0, 0, stats[0])
    for m in range(2, 4):
        flatten(craw, c, m)
    stats[1] = sum_middle(0, 1, stats[1])

    for n in range(2):
        tile = sum_end(0, n, stats[n])
        moments(0, tile, group(n))
        for m in group(n):
            for h, r in enumerate(free_rows(m)):
                sxs[m, h] = jnp.broadcast_to(tile[r : r + 1], (8, 128))
        for copy in halos[n]:
            copy.wait()
        acc = zero
        for m in group(n):
            mean, rstd = cols[0, m], cols[1, m]

            def hidden(v):
                return silu(gain1 * ((v - mean) * rstd) + shift1)

            spread(
                hq, m, lambda i: hidden(hb[0, m, :, i * 128 : i * 128 + 128]),
                lambda e: hidden(pr[0, n, e]),
            )
            a = dot(w2[m, 0], hq[m, :, 0:1024], 0, 0)
            a = a + dot(w2[m, 1], hq[m, :, 128:1152], 0, 0)
            a = a + dot(w2[m, 2], hq[m, :, 256:1280], 0, 0)
            hb[1, m, :, 128:1152] = a
            acc = sums(m, acc, a, a * a)
        pack(1, n)
        stats[n] = sum_start(1, n, rows_of_columns(acc))
        halos[n] = halo(1, n)

    def project(m):
        normed = ((hb[0, m, :, 128:1152] - cols[0, m]) * cols[1, m]).astype(BF16)
        part = dot(normed, x[m], 1, 1)
        for a in range(16):
            h, f = a // 8, a % 8
            bn[a, m * 8 : m * 8 + 8] = part[f * 8 : f * 8 + 8, h * 128 : h * 128 + 128]

    project(0)
    project(1)
    stats[0] = sum_middle(1, 0, stats[0])
    project(2)
    project(3)
    stats[1] = sum_middle(1, 1, stats[1])
    features = exchange(16, lambda d: bn.at[lax.rem(rank_a + d, 16)], bn1, rank_a, peer_a)

    sums2 = []
    for n in range(2):
        moments(2, sum_end(1, n, stats[n]), group(n))
        for copy in halos[n]:
            copy.wait()
        acc = zero
        for m in group(n):
            mean, rstd = cols[2, m], cols[3, m]
            for o in range(0, 1024, 256):
                span = slice(o, o + 256)
                pre = gain2 * ((hb[1, m, :, o + 128 : o + 384] - mean) * rstd) + shift2
                s = sigmoid(pre)
                h2[m, :, span] = (pre * s).astype(BF16)
                dpre1[m, :, span] = s * (1.0 + pre * (1.0 - s))
                third = dot(w3[m], h2[m, :, span], 0, 0)
                up = c[m, :, span].astype(F32) * slope(x[m, :, span].astype(F32) + third)
                u[m, :, span] = up
                ulow[m, :, span] = up.astype(BF16)
            back = dot(w3[m], ulow[m], 1, 0)
            hb[2, m, :, 128:1152] = back
            dpre = back * dpre1[m]
            acc = sums(m, acc, dpre, dpre * ((hb[1, m, :, 128:1152] - mean) * rstd))
        pack(2, n)
        stats[n] = sum_start(2, n, rows_of_columns(acc))
        halos[n] = halo(2, n)

    fac = zero

    def expand(m, fac):
        part = dot(h2[m], ulow[m], 1, 1)
        ofm, efm = of[m : m + 1], cols[9, m]
        scaled = part * efm * ofm
        acce[...] = scaled if m == 0 else acce[...] + scaled
        byw = part * ew[...].astype(F32)
        nf[1, m] = jnp.sum(byw * efm, axis=0, keepdims=True)
        return put(fac, m, jnp.sum(byw * ofm, axis=1, keepdims=True))

    fac = expand(1, expand(0, fac))
    stats[0] = sum_middle(2, 0, stats[0])
    fac = expand(3, expand(2, fac))
    stats[1] = sum_middle(2, 1, stats[1])
    features()
    bn1[rank_a] = bn[rank_a]
    bn2[rank_b] = total(bn1)
    features = exchange(17, lambda d: bn2.at[rank_b], bn2, rank_b, peer_b)

    for n in range(2):
        tile = sum_end(2, n, stats[n])
        sums2.append(tile)
        columns_of_rows(tile, 4, group(n))
        for copy in halos[n]:
            copy.wait()
        acc = zero
        for m in group(n):
            mean, rstd, plain, weighted = cols[2, m], cols[3, m], cols[4, m] / count, cols[5, m] / count

            def dact(second, back):
                normed = (second - mean) * rstd
                dpre = back * slope(gain2 * normed + shift2)
                return gain2 * rstd * (dpre - plain - normed * weighted)

            spread(
                dq, m,
                lambda i: dact(hb[1, m, :, i * 128 : i * 128 + 128], hb[2, m, :, i * 128 : i * 128 + 128]),
                lambda e: dact(pr[1, n, e], pr[2, n, e]),
            )
            a = dot(w2b[m, 0], dq[m, :, 0:1024], 1, 0)
            a = a + dot(w2b[m, 1], dq[m, :, 128:1152], 1, 0)
            a = a + dot(w2b[m, 2], dq[m, :, 256:1280], 1, 0)
            normed = (hb[0, m, :, 128:1152] - cols[0, m]) * cols[1, m]
            dpre = a * slope(gain1 * normed + shift1)
            dpre1[m] = dpre
            acc = sums(m, acc, dpre, dpre * normed)
        stats[n] = sum_start(3, n, rows_of_columns(acc))

    def gradients(m, fac):
        sfm = cols[8, m]
        byf = jnp.zeros((64, 1), F32)
        for p in range(3):
            part = dot(hq[m, :, p * 128 : p * 128 + 1024], dq[m, 64:128, 128:1152], 1, 1)
            for q in range(3):
                k = 3 * p + q
                tap = part[q * 64 : q * 64 + 64]
                byf = byf + jnp.sum(tap * sw[k].astype(F32), axis=1, keepdims=True)
                tap = tap * sfm
                accs[k] = tap if m == 0 else accs[k] + tap
        part = dot(dpre1[m].astype(BF16), x[m], 1, 1) * (gain1 * cols[1, m])
        scaled = part * rf[m : m + 1]
        accr[...] = scaled if m == 0 else accr[...] + scaled
        nf[0, m] = jnp.sum(part * rwt[...], axis=0, keepdims=True)
        return put(fac, 4 + m, byf)

    fac = gradients(1, gradients(0, fac))
    stats[0] = sum_middle(3, 0, stats[0])
    fac = gradients(3, gradients(2, fac))
    stats[1] = sum_middle(3, 1, stats[1])
    for a in range(16):
        h, f = a // 8, a % 8
        g[a, 0:8] = acce[f * 8 : f * 8 + 8, h * 128 : h * 128 + 128]
        g[a, 8:16] = accr[f * 8 : f * 8 + 8, h * 128 : h * 128 + 128]
    for t in range(36):
        low, high = t * 8, 288 + t * 8
        a, r = other(t)
        g[a, r : r + 8] = jnp.concatenate(
            [accs[low // 64, low % 64 : low % 64 + 8], accs[high // 64, high % 64 : high % 64 + 8]], axis=1
        )
    for k, t in ((0, REDUCE_F), (1, OUTPUT_F)):
        a, r = other(t)
        g[a, r : r + 8] = jnp.concatenate(
            [nf[k, m, :, h * 128 : h * 128 + 128] for h in range(2) for m in range(4)], axis=0
        )
    a, r = other(COLUMN_F)
    g[a, r : r + 8] = rows_of_columns(fac)
    for t in range(COLUMN_F + 1, TILES):
        a, r = other(t)
        g[a, r : r + 8] = jnp.zeros((8, 128), F32)
    shares = exchange(18, lambda d: g.at[lax.rem(rank_a + d, 16)], r1, rank_a, peer_a)
    features()
    bnc[...] = total(bn2)

    def finish(m):
        mean, rstd, plain, weighted = cols[0, m], cols[1, m], cols[6, m] / count, cols[7, m] / count
        normed = (hb[0, m, :, 128:1152] - mean) * rstd
        dq[m, 0:64, 0:1024] = (gain1 * rstd * (dpre1[m] - plain - normed * weighted)).astype(BF16)
        for j in range(4):
            o = j * 256
            t = u[m, :, o : o + 256] + dot(w1[m], dq[m, 0:64, o : o + 256], 0, 0)
            wide[m % 2, pl.ds(2 * j, 256, stride=8), :] = t[:, :128]
            wide[m % 2, pl.ds(2 * j + 1, 256, stride=8), :] = t[:, 128:]
        craw[m] = wide[m % 2].reshape(256, 8, 128).astype(BF16)
        store = pltpu.make_async_copy(craw.at[m], y_hbm.at[m], st_sem.at[m])
        store.start()
        return store

    tile = sum_end(3, 0, stats[0])
    sums1 = [tile]
    columns_of_rows(tile, 6, group(0))
    stores = [finish(0), finish(1)]
    shares()
    r1[rank_a] = g[rank_a]
    r2[rank_b] = total(r1)
    shares = exchange(19, lambda d: r2.at[rank_b], r2, rank_b, peer_b)
    tile = sum_end(3, 1, stats[1])
    sums1.append(tile)
    columns_of_rows(tile, 6, group(1))
    stores += [finish(2), finish(3)]

    half, block = lax.div(rank_a, 8), pl.ds(pl.multiple_of(lax.rem(rank_a, 8) * 8, 8), 8)
    span = pl.ds(pl.multiple_of(half * 128, 128), 128)
    fix = jnp.zeros((8, 128), F32)
    part = jnp.zeros((8, 128), F32)
    for m in range(4):
        plain, weighted = cols[6, m, block] / count, cols[7, m, block] / count
        e = cols[10, 0, block] * cols[1, m, block] * (
            plain * sxs[m, half] + weighted * bnc[m * 8 : m * 8 + 8]
        )
        fix = fix + e * rf[m : m + 1, span]
        part = jnp.where(
            sub == half * 4 + m, jnp.sum(e * rwt[block, span], axis=0, keepdims=True), part
        )
    shares()
    share = total(r2)
    r3[rank_a, 0:8] = share[0:8]
    r3[rank_a, 8:16] = share[8:16] - fix
    r3[rank_a, 16:40] = share[16:40]
    r3[rank_a, 40:48] = part
    shares = exchange(20, lambda d: r3.at[rank_a], r3, rank_a, peer_a)
    first, second = sums1[0] + sums1[1], sums2[0] + sums2[1]
    packed[NORMS : NORMS + 8] = jnp.concatenate(
        [
            jnp.sum(first[4:8], axis=0, keepdims=True),
            jnp.sum(first[0:4], axis=0, keepdims=True),
            jnp.sum(second[4:8], axis=0, keepdims=True),
            jnp.sum(second[0:4], axis=0, keepdims=True),
            jnp.zeros((4, 128), F32),
        ],
        axis=0,
    )
    shares()
    for a in range(16):
        packed[a * WITH_PART : a * WITH_PART + WITH_PART] = r3[a]
    for copy in stores:
        copy.wait()


def unpack(
    y_hbm, packed_hbm,
    out_hbm, o_reduce, o_spatial, o_expand, o_rf, o_sf, o_ef, o_of, o_g1, o_b1, o_g2, o_b2,
    y, packed, sem,
):
    load = [pltpu.make_async_copy(packed_hbm, packed, sem.at[0])]
    load += [pltpu.make_async_copy(y_hbm.at[m], y.at[m], sem.at[1 + m]) for m in range(4)]
    store = [pltpu.make_async_copy(y.at[m], out_hbm.at[m], sem.at[5 + m]) for m in range(4)]
    for copy in load:
        copy.start()
    for m in range(4):
        load[1 + m].wait()
        store[m].start()
    load[0].wait()

    def tile(a, r):
        return packed[a * WITH_PART + r : a * WITH_PART + r + 8]

    fix = jnp.zeros((8, 128), F32)
    for a in range(16):
        h, f = a // 8, a % 8
        o_expand[f * 8 : f * 8 + 8, h * 128 : h * 128 + 128] = tile(a, 0)
        o_reduce[f * 8 : f * 8 + 8, h * 128 : h * 128 + 128] = tile(a, 8)
        fix = fix + tile(a, 40)
    for t in range(36):
        both = tile(*other(t))
        for n in range(2):
            r = n * 288 + t * 8
            o_spatial[r // 64, r % 64 : r % 64 + 8] = both[:, n * 64 : n * 64 + 64]
    for o, e in ((o_rf, tile(*other(REDUCE_F)) - fix), (o_of, tile(*other(OUTPUT_F)))):
        o[:, :128] = e[:4]
        o[:, 128:] = e[4:]
    e = tile(*other(COLUMN_F))
    o_ef[...] = e[:4, :64]
    o_sf[...] = e[4:, :64]
    for n, o in enumerate((o_g1, o_b1, o_g2, o_b2)):
        o[...] = packed[NORMS + n : NORMS + n + 1, :64]
    for copy in store:
        copy.wait()


def body(
    features, cotangent, reduce_weight, spatial_weight, expand_weight,
    reduce_factor, spatial_factor, expand_factor, output_factor,
    gain_first, shift_first, gain_second, shift_second,
):
    vmem = pl.BlockSpec(memory_space=pltpu.VMEM)
    hbm = pl.BlockSpec(memory_space=pl.ANY)
    sds = jax.ShapeDtypeStruct
    y, packed = pl.pallas_call(
        kernel,
        out_shape=(sds((4, 256, 8, 128), BF16), sds((NORMS + 8, 128), F32)),
        in_specs=[hbm] * 13,
        out_specs=(hbm, vmem),
        scratch_shapes=[
            pltpu.VMEM((4, 256, 8, 128), BF16),
            pltpu.VMEM((4, 256, 8, 128), BF16),
            pltpu.VMEM((2, 2048, 128), F32),
            pltpu.VMEM((64, 256), BF16),
            pltpu.VMEM((9, 64, 64), BF16),
            pltpu.VMEM((64, 256), BF16),
            pltpu.VMEM((4, 256), F32),
            pltpu.VMEM((4, 64), F32),
            pltpu.VMEM((4, 64), F32),
            pltpu.VMEM((4, 256), F32),
            pltpu.VMEM((1, 64), F32),
            pltpu.VMEM((1, 64), F32),
            pltpu.VMEM((1, 64), F32),
            pltpu.VMEM((1, 64), F32),
            pltpu.VMEM((4, 64, 256), BF16),
            pltpu.VMEM((4, 3, 192, 64), BF16),
            pltpu.VMEM((4, 3, 64, 192), BF16),
            pltpu.VMEM((4, 64, 256), BF16),
            pltpu.VMEM((64, 256), F32),
            pltpu.VMEM((4, 256, 1024), BF16),
            pltpu.VMEM((4, 256, 1024), BF16),
            pltpu.VMEM((4, 256, 1024), F32),
            pltpu.VMEM((4, 256, 1024), BF16),
            pltpu.VMEM((4, 64, 1024), BF16),
            pltpu.VMEM((3, 4, 64, 1280), F32),
            pltpu.VMEM((4, 192, 1280), BF16),
            pltpu.VMEM((4, 192, 1280), BF16),
            pltpu.VMEM((4, 64, 1024), F32),
            pltpu.VMEM((2, 4, 1, 256), F32),
            pltpu.VMEM((3, 2, 64, 128), F32),
            pltpu.VMEM((3, 2, 6, 64, 128), F32),
            pltpu.VMEM((8, 16, 8, 128), F32),
            pltpu.VMEM((8, 16, 8, 128), F32),
            pltpu.VMEM((64, 256), F32),
            pltpu.VMEM((64, 256), F32),
            pltpu.VMEM((9, 64, 64), F32),
            pltpu.VMEM((4, 2, 8, 128), F32),
            pltpu.VMEM((16, 32, 128), F32),
            pltpu.VMEM((16, 32, 128), F32),
            pltpu.VMEM((16, 32, 128), F32),
            pltpu.VMEM((32, 128), F32),
            pltpu.VMEM((16, SHARE, 128), F32),
            pltpu.VMEM((16, SHARE, 128), F32),
            pltpu.VMEM((16, SHARE, 128), F32),
            pltpu.VMEM((16, WITH_PART, 128), F32),
            pltpu.VMEM((12, 4, 64, 1), F32),
            pltpu.SemaphoreType.DMA((20,)),
            pltpu.SemaphoreType.DMA((4,)),
            pltpu.SemaphoreType.DMA((21, 16)),
            pltpu.SemaphoreType.DMA((21, 16)),
            pltpu.SemaphoreType.DMA((6, 8)),
            pltpu.SemaphoreType.DMA((6, 8)),
        ],
        compiler_params=pltpu.CompilerParams(
            collective_id=0, has_side_effects=True, vmem_limit_bytes=67043328
        ),
        name="step",
    )(
        features, cotangent, reduce_weight.T, spatial_weight, expand_weight,
        reduce_factor, spatial_factor, expand_factor, output_factor,
        gain_first.reshape(1, 64), shift_first.reshape(1, 64),
        gain_second.reshape(1, 64), shift_second.reshape(1, 64),
    )
    outs = pl.pallas_call(
        unpack,
        out_shape=(
            sds((4, 256, 8, 128), BF16), sds((64, 256), F32), sds((9, 64, 64), F32), sds((64, 256), F32),
            sds((4, 256), F32), sds((4, 64), F32), sds((4, 64), F32), sds((4, 256), F32),
        ) + (sds((1, 64), F32),) * 4,
        in_specs=[hbm, hbm],
        out_specs=(hbm,) + (vmem,) * 11,
        scratch_shapes=[
            pltpu.VMEM((4, 256, 8, 128), BF16),
            pltpu.VMEM((NORMS + 8, 128), F32),
            pltpu.SemaphoreType.DMA((9,)),
        ],
        compiler_params=pltpu.CompilerParams(vmem_limit_bytes=67043328),
        name="unpack",
    )(y, packed)
    return (outs[0], outs[1].T) + outs[2:8] + tuple(o.reshape(64) for o in outs[8:])


def solution(mesh):
    split = Mesh(
        mesh.devices.reshape(2, 4, 8, 2, 2), ("rows_0", "rows_1", "cols_0", "cols_1", "cols_2")
    )
    image = P(None, None, ROWS, COLS)
    return jax.shard_map(
        body,
        mesh=split,
        in_specs=(image, image) + (P(),) * 11,
        out_specs=(image,) + (P(),) * 11,
        check_vma=False,
    )
```

```python
import functools

import jax
import jax.numpy as jnp
from jax import lax
from jax.experimental import pallas as pl
from jax.experimental.pallas import tpu as pltpu
from jax.sharding import Mesh
from jax.sharding import PartitionSpec as P

ROWS = ("rows_0", "rows_1")
COLS = ("cols_0", "cols_1", "cols_2")
MESH = pl.DeviceIdType.MESH
EPSILON = 1e-05
F32 = jnp.float32
BF16 = jnp.bfloat16

EARLY, LATE, WHOLE = 8, 16, 32
OUTPUT_F, EXPAND_F, EARLY_TILES = 16, 17, 32
SPATIAL, REDUCE_F, SPATIAL_F, LATE_TILES = 16, 52, 53, 64


def dot(a, b, ca, cb):
    return lax.dot_general(a, b, (((ca,), (cb,)), ((), ())), preferred_element_type=F32)


def sigmoid(v):
    return 0.5 + 0.5 * jnp.tanh(0.5 * v)


def silu(v):
    return v * sigmoid(v)


def slope(v):
    s = sigmoid(v)
    return s * (1.0 + v * (1.0 - s))


def total(buf, n=16):
    t = buf[0]
    for k in range(1, n):
        t = t + buf[k]
    return t


def kernel(
    x_hbm, c_hbm, rw_hbm, sw_hbm, ew_hbm, rf_hbm, sf_hbm, ef_hbm, of_hbm, g1_hbm, b1_hbm, g2_hbm, b2_hbm,
    y_hbm, late_hbm, early_hbm, norms_hbm,
    xraw, craw, wide, rw, sw, ew, rf, sf, ef, of, g1, b1, g2, b2,
    w1, w2, w2b, w3, rwt,
    x, c, u, ulow, h2, hb, hq, dq, dpre1, nf, pk, pr, arb, ara,
    acce, accr, accs, sxs, bn, bn0, bn1, bn2, bnc, e, e0, e1, e2, e3, g, g0, g1_, g2_, g3, norms, cols,
    ld_sem, st_sem, s_sem, r_sem, hs_sem, hr_sem, cs_sem, cr_sem,
):
    count = float(64 * 4096)
    x_hi, y = lax.axis_index("rows_0"), lax.axis_index("rows_1")
    z, x_lo, core = lax.axis_index("cols_0"), lax.axis_index("cols_1"), lax.axis_index("cols_2")
    row = x_hi * 4 + y
    col = z * 4 + x_lo * 2 + core
    rank_a = x_hi * 8 + x_lo * 4 + y
    rank_b = z * 2 + core

    def peer_a(d):
        a = lax.rem(rank_a + d, 16)
        return (lax.div(a, 8), lax.rem(a, 4), z, lax.rem(lax.div(a, 4), 2), core)

    def peer_b(d):
        b = lax.rem(rank_b + d, 16)
        return (x_hi, y, lax.div(b, 2), x_lo, lax.rem(b, 2))

    def peer_z(d):
        return (x_hi, y, lax.rem(z + d, 8), x_lo, core)

    def at(dr, dc):
        rr, cc = lax.rem(row + dr + 8, 8), lax.rem(col + dc + 32, 32)
        return (lax.div(rr, 4), lax.rem(rr, 4), lax.div(cc, 4), lax.rem(lax.div(cc, 2), 2), lax.rem(cc, 2))

    sides = ((0, 1), (0, -1), (1, 1), (1, -1), (-1, 1), (-1, -1))

    pairs = (
        (rw_hbm, rw), (rf_hbm, rf), (sw_hbm, sw), (ew_hbm, ew), (sf_hbm, sf), (ef_hbm, ef), (of_hbm, of),
        (g1_hbm, g1), (b1_hbm, b1), (g2_hbm, g2), (b2_hbm, b2),
    )
    load_w = [pltpu.make_async_copy(a, b, ld_sem.at[8 + n]) for n, (a, b) in enumerate(pairs)]
    load_x = [pltpu.make_async_copy(x_hbm.at[m], xraw.at[m], ld_sem.at[m]) for m in range(4)]
    load_c = [pltpu.make_async_copy(c_hbm.at[m], craw.at[m], ld_sem.at[4 + m]) for m in range(4)]
    for copy in load_w[:2] + load_x + load_w[2:] + load_c:
        copy.start()

    barrier = pltpu.get_barrier_semaphore()

    def greet(d, _):
        pl.semaphore_signal(barrier, inc=1, device_id=peer_a(d), device_id_type=MESH)
        pl.semaphore_signal(barrier, inc=1, device_id=peer_b(d), device_id_type=MESH)
        return 0

    lax.fori_loop(1, 16, greet, 0)
    for side in sides:
        pl.semaphore_signal(barrier, inc=1, device_id=at(*side), device_id_type=MESH)

    def exchange(stage, src, buf, rank, peer, n=16):
        def start(d, _):
            pltpu.make_async_remote_copy(
                src_ref=src(d), dst_ref=buf.at[rank], send_sem=s_sem.at[stage],
                recv_sem=r_sem.at[stage], device_id=peer(d), device_id_type=MESH,
            ).start()
            return 0

        lax.fori_loop(1, n, start, 0)
        return together(buf.at[pl.ds(0, n - 1)], s_sem.at[stage], r_sem.at[stage]).wait

    def together(ref, send, recv):
        return pltpu.make_async_remote_copy(
            src_ref=ref, dst_ref=ref, send_sem=send, recv_sem=recv,
            device_id=(x_hi, y, z, x_lo, 1 - core), device_id_type=MESH,
        )

    def swap(stage, src, dst):
        copy = pltpu.make_async_remote_copy(
            src_ref=src, dst_ref=dst, send_sem=cs_sem.at[stage], recv_sem=cr_sem.at[stage],
            device_id=(x_hi, y, z, x_lo, 1 - core), device_id_type=MESH,
        )
        copy.start()
        return copy.wait

    def share_cores(stage, tiles, partner):
        return swap(stage, tiles.at[1 - core], partner)

    def share_plane(stage, wait, tiles, partner, buf):
        wait()
        for a in range(16):
            partner[a] = partner[a] + tiles[core, a]
        return exchange(stage, lambda d: partner.at[lax.rem(rank_a + d, 16)], buf, rank_a, peer_a)

    def share_depth(stage, wait, partner, buf, slots):
        wait()
        buf[rank_a] = partner[rank_a]
        slots[z] = total(buf)
        return exchange(stage, lambda d: slots.at[z], slots, z, peer_z, 8)

    def gather_plane(stage, whole):
        return exchange(stage, lambda d: whole.at[core, rank_a], whole.at[core], rank_a, peer_a)

    def gather_cores(stage, wait, whole):
        wait()
        return swap(stage, whole.at[core], whole.at[core])

    def sum_start(k, n, tile):
        arb[2 * k + n, rank_b] = tile
        return exchange(
            4 * k + 2 * n, lambda d: arb.at[2 * k + n, rank_b], arb.at[2 * k + n], rank_b, peer_b
        )

    def sum_middle(k, n, wait):
        wait()
        ara[2 * k + n, rank_a] = total(arb.at[2 * k + n])
        return exchange(
            4 * k + 2 * n + 1, lambda d: ara.at[2 * k + n, rank_a], ara.at[2 * k + n], rank_a, peer_a
        )

    def sum_end(k, n, wait):
        wait()
        return total(ara.at[2 * k + n])

    def halo(k, n):
        members = pl.ds(2 * n, 2)
        t = 2 * k + n
        copies = [
            pltpu.make_async_remote_copy(
                src_ref=hb.at[k, members, :, pl.ds(128, 128)],
                dst_ref=hb.at[k, members, :, pl.ds(1152, 128)],
                send_sem=hs_sem.at[t, 0], recv_sem=hr_sem.at[t, 0],
                device_id=at(-1, 0), device_id_type=MESH,
            ),
            pltpu.make_async_remote_copy(
                src_ref=hb.at[k, members, :, pl.ds(1024, 128)],
                dst_ref=hb.at[k, members, :, pl.ds(0, 128)],
                send_sem=hs_sem.at[t, 0], recv_sem=hr_sem.at[t, 0],
                device_id=at(1, 0), device_id_type=MESH,
            ),
        ]
        for edge, side in enumerate(sides):
            copies.append(
                pltpu.make_async_remote_copy(
                    src_ref=pk.at[k, n], dst_ref=pr.at[k, n, edge], send_sem=hs_sem.at[t, 1],
                    recv_sem=hr_sem.at[t, 1], device_id=at(*side), device_id_type=MESH,
                )
            )
        for copy in copies:
            copy.start()
        return [
            together(hb.at[k, :, :, pl.ds(0, 128)], hs_sem.at[t, 0], hr_sem.at[t, 0]),
            together(pr.at[k, n], hs_sem.at[t, 1], hr_sem.at[t, 1]),
        ]

    lane = lax.broadcasted_iota(jnp.int32, (64, 128), 1)
    sub = lax.broadcasted_iota(jnp.int32, (8, 128), 0)
    zero = jnp.zeros((64, 128), F32)

    def put(acc, n, value):
        return jnp.where(lane == n, value, acc)

    def rows_of_columns(acc):
        return jnp.transpose(jnp.concatenate([acc, jnp.zeros((64, 128), F32)], axis=0))[:8]

    def columns_of_rows(tile, k, members):
        t = jnp.transpose(jnp.concatenate([tile, jnp.zeros((120, 128), F32)], axis=0))
        for m in members:
            cols[k, m] = t[:64, m : m + 1]
            cols[k + 1, m] = t[:64, 4 + m : 5 + m]

    def sums(m, acc, a, b):
        acc = put(acc, m, jnp.sum(a, axis=1, keepdims=True))
        return put(acc, 4 + m, jnp.sum(b, axis=1, keepdims=True))

    def pack(k, n):
        acc = zero
        for m in group(n):
            for i in range(8):
                t = hb[k, m, :, 128 + i * 128 : 256 + i * 128]
                acc = put(acc, m * 8 + i, t[:, 0:1])
                acc = put(acc, 32 + m * 8 + i, t[:, 127:128])
        pk[k, n] = acc

    def group(n):
        return (2 * n, 2 * n + 1)

    top = jnp.where(row > 0, 1.0, 0.0).astype(F32)
    bottom = jnp.where(row < 7, 1.0, 0.0).astype(F32)
    left = jnp.where(col > 0, 1.0, 0.0).astype(F32)
    right = jnp.where(col < 31, 1.0, 0.0).astype(F32)
    masks = (left, right, top * left, top * right, bottom * left, bottom * right)

    def spread(dst, m, tile, edge):
        edges = [edge(e) * masks[e] for e in range(6)]
        for i in range(10):
            t = tile(i)
            if i == 0:
                t, e0, e2, at_row = t * top, edges[2], edges[3], 7
            elif i == 9:
                t, e0, e2, at_row = t * bottom, edges[4], edges[5], 0
            else:
                e0, e2, at_row = edges[0], edges[1], i - 1
            where0 = 32 + m * 8 + at_row
            where2 = m * 8 + at_row
            before = jnp.where(
                lane == 0, pltpu.roll(e0, 128 - where0, axis=1), pltpu.roll(t, 1, axis=1)
            )
            after = jnp.where(
                lane == 127, pltpu.roll(e2, 127 - where2, axis=1), pltpu.roll(t, 127, axis=1)
            )
            span = slice(i * 128, i * 128 + 128)
            dst[m, 0:64, span] = before.astype(BF16)
            dst[m, 64:128, span] = t.astype(BF16)
            dst[m, 128:192, span] = after.astype(BF16)

    def flatten(src, dst, m):
        wide[m % 2] = src[m].astype(F32).reshape(2048, 128)
        for i in range(8):
            dst[m, :, i * 128 : i * 128 + 128] = wide[m % 2, pl.ds(i, 256, stride=8), :].astype(BF16)

    def moments(k, tile, members):
        columns_of_rows(tile, k, members)
        for m in members:
            mean = cols[k, m] / count
            var = cols[k + 1, m] / count - mean * mean
            cols[k, m] = mean
            cols[k + 1, m] = lax.rsqrt(var + EPSILON)

    for copy in load_w[:2]:
        copy.wait()
    rwt[...] = rw[...].astype(F32)
    for m in range(4):
        w1[m] = (rwt[...] * rf[m : m + 1]).astype(BF16)
    ones = jnp.ones((8, 1024), BF16)

    def free_rows(m):
        base = 2 if m < 2 else 0
        return (base + 4 * (m % 2), base + 4 * (m % 2) + 1)

    stats, halos, tiles = [None, None], [None, None], [None, None]
    for n in range(2):
        acc = zero
        extra = []
        for m in group(n):
            load_x[m].wait()
            flatten(xraw, x, m)
            a = dot(w1[m], x[m], 1, 0)
            hb[0, m, :, 128:1152] = a
            acc = sums(m, acc, a, a * a)
            extra.append((m, dot(ones, x[m], 1, 1)))
        tile = rows_of_columns(acc)
        for m, line in extra:
            for h, r in enumerate(free_rows(m)):
                tile = jnp.where(sub == r, line[:, h * 128 : h * 128 + 128], tile)
        tiles[n] = tile
        pack(0, n)
    pl.semaphore_wait(barrier, 36)
    for n in range(2):
        stats[n] = sum_start(0, n, tiles[n])
        halos[n] = halo(0, n)

    for copy in load_w[2:]:
        copy.wait()
    tail = jnp.zeros((8, 64), F32)
    columns_of_rows(
        jnp.concatenate([jnp.concatenate([sf[...], ef[...]], axis=0), tail], axis=1), 8, range(4)
    )
    columns_of_rows(
        jnp.concatenate(
            [jnp.concatenate([g1[...], b1[...], g2[...], b2[...], tail[:4]], axis=0), tail], axis=1
        ), 10, range(4),
    )
    for m in range(4):
        sfm, efm = cols[8, m], cols[9, m]
        w3[m] = (efm * ew[...].astype(F32) * of[m : m + 1]).astype(BF16)
        for p in range(3):
            taps = [(sfm * sw[3 * p + q].astype(F32)).astype(BF16) for q in range(3)]
            for q in range(3):
                w2[m, p, q * 64 : q * 64 + 64] = taps[q]
            w2b[m, 2 - p] = jnp.concatenate(taps[::-1], axis=1)
    gain1, shift1, gain2, shift2 = (cols[10, n] for n in range(4))
    for copy in load_c:
        copy.wait()
    for m in range(4):
        flatten(craw, c, m)
    stats[0] = sum_middle(0, 0, stats[0])
    stats[1] = sum_middle(0, 1, stats[1])

    for n in range(2):
        tile = sum_end(0, n, stats[n])
        moments(0, tile, group(n))
        for m in group(n):
            for h, r in enumerate(free_rows(m)):
                sxs[m, h] = jnp.broadcast_to(tile[r : r + 1], (8, 128))
        for copy in halos[n]:
            copy.wait()
        acc = zero
        for m in group(n):
            mean, rstd = cols[0, m], cols[1, m]

            def hidden(v):
                return silu(gain1 * ((v - mean) * rstd) + shift1)

            spread(
                hq, m, lambda i: hidden(hb[0, m, :, i * 128 : i * 128 + 128]),
                lambda e: hidden(pr[0, n, e]),
            )
            a = dot(w2[m, 0], hq[m, :, 0:1024], 0, 0)
            a = a + dot(w2[m, 1], hq[m, :, 128:1152], 0, 0)
            a = a + dot(w2[m, 2], hq[m, :, 256:1280], 0, 0)
            hb[1, m, :, 128:1152] = a
            acc = sums(m, acc, a, a * a)
        stats[n] = sum_start(1, n, rows_of_columns(acc))
        pack(1, n)
        halos[n] = halo(1, n)

    def project(m):
        normed = ((hb[0, m, :, 128:1152] - cols[0, m]) * cols[1, m]).astype(BF16)
        part = dot(normed, x[m], 1, 1)
        for a in range(16):
            h, f = a // 8, a % 8
            bn[m // 2, a, m % 2 * 8 : m % 2 * 8 + 8] = part[f * 8 : f * 8 + 8, h * 128 : h * 128 + 128]

    for m in range(4):
        project(m)
    corrections = share_cores(0, bn, bn0)
    stats[0] = sum_middle(1, 0, stats[0])
    stats[1] = sum_middle(1, 1, stats[1])
    corrections = share_plane(16, corrections, bn, bn0, bn1)

    sums2 = []
    for n in range(2):
        moments(2, sum_end(1, n, stats[n]), group(n))
        for copy in halos[n]:
            copy.wait()
        acc = zero
        for m in group(n):
            mean, rstd = cols[2, m], cols[3, m]
            for o in range(0, 1024, 256):
                span = slice(o, o + 256)
                pre = gain2 * ((hb[1, m, :, o + 128 : o + 384] - mean) * rstd) + shift2
                s = sigmoid(pre)
                h2[m, :, span] = (pre * s).astype(BF16)
                dpre1[m, :, span] = s * (1.0 + pre * (1.0 - s))
                third = dot(w3[m], h2[m, :, span], 0, 0)
                up = c[m, :, span].astype(F32) * slope(x[m, :, span].astype(F32) + third)
                u[m, :, span] = up
                ulow[m, :, span] = up.astype(BF16)
            back = dot(w3[m], ulow[m], 1, 0)
            hb[2, m, :, 128:1152] = back
            dpre = back * dpre1[m]
            acc = sums(m, acc, dpre, dpre * ((hb[1, m, :, 128:1152] - mean) * rstd))
        stats[n] = sum_start(2, n, rows_of_columns(acc))
        pack(2, n)
        halos[n] = halo(2, n)

    fac = zero

    def expand(m, fac):
        part = dot(h2[m], ulow[m], 1, 1)
        ofm, efm = of[m : m + 1], cols[9, m]
        scaled = part * efm * ofm
        acce[...] = scaled if m == 0 else acce[...] + scaled
        byw = part * ew[...].astype(F32)
        nf[1, m] = jnp.sum(byw * efm, axis=0, keepdims=True)
        return put(fac, m, jnp.sum(byw * ofm, axis=1, keepdims=True))

    for m in range(4):
        fac = expand(m, fac)

    def place(buf, t, value):
        r = t // 32 * 8
        buf[t // 16 % 2, t % 16, r : r + 8] = value

    def lines(k):
        return jnp.concatenate(
            [nf[k, m, :, h * 128 : h * 128 + 128] for h in range(2) for m in range(4)], axis=0
        )

    for a in range(16):
        h, f = a // 8, a % 8
        place(e, a, acce[f * 8 : f * 8 + 8, h * 128 : h * 128 + 128])
    place(e, OUTPUT_F, lines(1))
    place(e, EXPAND_F, rows_of_columns(fac))
    for t in range(EXPAND_F + 1, EARLY_TILES):
        place(e, t, jnp.zeros((8, 128), F32))
    early = share_cores(1, e, e0)
    stats[0] = sum_middle(2, 0, stats[0])
    stats[1] = sum_middle(2, 1, stats[1])
    early = share_plane(18, early, e, e0, e1)
    corrections = share_depth(17, corrections, bn0, bn1, bn2)

    for n in range(2):
        tile = sum_end(2, n, stats[n])
        sums2.append(tile)
        columns_of_rows(tile, 4, group(n))
        for copy in halos[n]:
            copy.wait()
        acc = zero
        for m in group(n):
            mean, rstd, plain, weighted = cols[2, m], cols[3, m], cols[4, m] / count, cols[5, m] / count

            def dact(second, back):
                normed = (second - mean) * rstd
                dpre = back * slope(gain2 * normed + shift2)
                return gain2 * rstd * (dpre - plain - normed * weighted)

            spread(
                dq, m,
                lambda i: dact(hb[1, m, :, i * 128 : i * 128 + 128], hb[2, m, :, i * 128 : i * 128 + 128]),
                lambda e: dact(pr[1, n, e], pr[2, n, e]),
            )
            a = dot(w2b[m, 0], dq[m, :, 0:1024], 1, 0)
            a = a + dot(w2b[m, 1], dq[m, :, 128:1152], 1, 0)
            a = a + dot(w2b[m, 2], dq[m, :, 256:1280], 1, 0)
            normed = (hb[0, m, :, 128:1152] - cols[0, m]) * cols[1, m]
            dpre = a * slope(gain1 * normed + shift1)
            dpre1[m] = dpre
            acc = sums(m, acc, dpre, dpre * normed)
        stats[n] = sum_start(3, n, rows_of_columns(acc))

    def gradients(m, fac):
        sfm = cols[8, m]
        byf = jnp.zeros((64, 1), F32)
        for p in range(3):
            part = dot(hq[m, :, p * 128 : p * 128 + 1024], dq[m, 64:128, 128:1152], 1, 1)
            for q in range(3):
                k = 3 * p + q
                tap = part[q * 64 : q * 64 + 64]
                byf = byf + jnp.sum(tap * sw[k].astype(F32), axis=1, keepdims=True)
                tap = tap * sfm
                accs[k] = tap if m == 0 else accs[k] + tap
        part = dot(dpre1[m].astype(BF16), x[m], 1, 1) * (gain1 * cols[1, m])
        scaled = part * rf[m : m + 1]
        accr[...] = scaled if m == 0 else accr[...] + scaled
        nf[0, m] = jnp.sum(part * rwt[...], axis=0, keepdims=True)
        return put(fac, m, byf)

    fac = zero
    for m in range(4):
        fac = gradients(m, fac)
    for a in range(16):
        h, f = a // 8, a % 8
        place(g, a, accr[f * 8 : f * 8 + 8, h * 128 : h * 128 + 128])
    for t in range(36):
        low, high = t * 8, 288 + t * 8
        place(g, SPATIAL + t, jnp.concatenate(
            [accs[low // 64, low % 64 : low % 64 + 8], accs[high // 64, high % 64 : high % 64 + 8]], axis=1
        ))
    place(g, REDUCE_F, lines(0))
    place(g, SPATIAL_F, rows_of_columns(fac))
    for t in range(SPATIAL_F + 1, LATE_TILES):
        place(g, t, jnp.zeros((8, 128), F32))
    late = share_cores(2, g, g0)
    early = share_depth(19, early, e0, e1, e2)
    late = share_plane(21, late, g, g0, g1_)
    stats[0] = sum_middle(3, 0, stats[0])
    stats[1] = sum_middle(3, 1, stats[1])
    corrections()
    bnc[...] = total(bn2, 8)
    early()
    e3[core, rank_a] = total(e2, 8)
    early = gather_plane(20, e3)

    def finish(m):
        mean, rstd, plain, weighted = cols[0, m], cols[1, m], cols[6, m] / count, cols[7, m] / count
        normed = (hb[0, m, :, 128:1152] - mean) * rstd
        dq[m, 0:64, 0:1024] = (gain1 * rstd * (dpre1[m] - plain - normed * weighted)).astype(BF16)
        for j in range(4):
            o = j * 256
            t = u[m, :, o : o + 256] + dot(w1[m], dq[m, 0:64, o : o + 256], 0, 0)
            wide[m % 2, pl.ds(2 * j, 256, stride=8), :] = t[:, :128]
            wide[m % 2, pl.ds(2 * j + 1, 256, stride=8), :] = t[:, 128:]
        craw[m] = wide[m % 2].reshape(256, 8, 128).astype(BF16)
        store = pltpu.make_async_copy(craw.at[m], y_hbm.at[m], st_sem.at[m])
        store.start()
        return store

    tile = sum_end(3, 0, stats[0])
    sums1 = [tile]
    columns_of_rows(tile, 6, group(0))
    late = share_depth(22, late, g0, g1_, g2_)
    stores = [finish(0), finish(1)]
    tile = sum_end(3, 1, stats[1])
    sums1.append(tile)
    columns_of_rows(tile, 6, group(1))

    half, block = lax.div(rank_a, 8), pl.ds(pl.multiple_of(lax.rem(rank_a, 8) * 8, 8), 8)
    span = pl.ds(pl.multiple_of(half * 128, 128), 128)
    fix = jnp.zeros((8, 128), F32)
    part = jnp.zeros((8, 128), F32)
    for k in range(2):
        m = 2 * core + k
        plain, weighted = cols[6, m, block] / count, cols[7, m, block] / count
        v = cols[10, 0, block] * cols[1, m, block] * (
            plain * sxs[m, half] + weighted * bnc[k * 8 : k * 8 + 8]
        )
        fix = fix + v * jnp.where(core == 0, rf[k : k + 1, span], rf[k + 2 : k + 3, span])
        part = jnp.where(
            sub == half * 4 + m, jnp.sum(v * rwt[block, span], axis=0, keepdims=True), part
        )
    g3[core, rank_a, LATE : LATE + 8] = fix
    g3[core, rank_a, LATE + 8 : WHOLE] = part
    late()
    g3[core, rank_a, 0:LATE] = total(g2_, 8)
    late = gather_plane(23, g3)
    early = gather_cores(3, early, e3)
    stores += [finish(2), finish(3)]
    first, second = sums1[0] + sums1[1], sums2[0] + sums2[1]
    norms[...] = jnp.concatenate(
        [
            jnp.sum(first[4:8], axis=0, keepdims=True),
            jnp.sum(first[0:4], axis=0, keepdims=True),
            jnp.sum(second[4:8], axis=0, keepdims=True),
            jnp.sum(second[0:4], axis=0, keepdims=True),
            jnp.zeros((4, 128), F32),
        ],
        axis=0,
    )
    stores.append(pltpu.make_async_copy(norms, norms_hbm, st_sem.at[4]))
    stores[-1].start()
    late = gather_cores(4, late, g3)
    early()
    stores.append(pltpu.make_async_copy(e3, early_hbm, st_sem.at[5]))
    stores[-1].start()
    late()
    stores.append(pltpu.make_async_copy(g3, late_hbm, st_sem.at[6]))
    stores[-1].start()
    for copy in stores:
        copy.wait()


def unpack(
    y_hbm, late_hbm, early_hbm, norms_hbm,
    out_hbm, o_reduce, o_spatial, o_expand, o_rf, o_sf, o_ef, o_of, o_g1, o_b1, o_g2, o_b2,
    y, whole, expand, norms, sem,
):
    load = [pltpu.make_async_copy(y_hbm.at[m], y.at[m], sem.at[m]) for m in range(4)]
    store = [pltpu.make_async_copy(y.at[m], out_hbm.at[m], sem.at[4 + m]) for m in range(4)]
    small = [
        pltpu.make_async_copy(src, dst, sem.at[8 + n])
        for n, (src, dst) in enumerate(((late_hbm, whole), (early_hbm, expand), (norms_hbm, norms)))
    ]
    for copy in load + small:
        copy.start()
    for m in range(4):
        load[m].wait()
        store[m].start()
    for copy in small:
        copy.wait()

    def early(t):
        return expand[t // 16, t % 16]

    def late(t):
        return whole[t // 16 % 2, t % 16, t // 32 * 8 : t // 32 * 8 + 8]

    def fixes(a, k):
        r = LATE + k * 8
        return whole[0, a, r : r + 8] + whole[1, a, r : r + 8]

    fix = jnp.zeros((8, 128), F32)
    for a in range(16):
        h, f = a // 8, a % 8
        o_expand[f * 8 : f * 8 + 8, h * 128 : h * 128 + 128] = early(a)
        o_reduce[f * 8 : f * 8 + 8, h * 128 : h * 128 + 128] = late(a) - fixes(a, 0)
        fix = fix + fixes(a, 1)
    for t in range(36):
        both = late(SPATIAL + t)
        for n in range(2):
            r = n * 288 + t * 8
            o_spatial[r // 64, r % 64 : r % 64 + 8] = both[:, n * 64 : n * 64 + 64]
    for o, e in ((o_rf, late(REDUCE_F) - fix), (o_of, early(OUTPUT_F))):
        o[:, :128] = e[:4]
        o[:, 128:] = e[4:]
    o_ef[...] = early(EXPAND_F)[:4, :64]
    o_sf[...] = late(SPATIAL_F)[:4, :64]
    for n, o in enumerate((o_g1, o_b1, o_g2, o_b2)):
        o[...] = norms[n : n + 1, :64]
    for copy in store:
        copy.wait()


def body(
    features, cotangent, reduce_weight, spatial_weight, expand_weight,
    reduce_factor, spatial_factor, expand_factor, output_factor,
    gain_first, shift_first, gain_second, shift_second,
):
    vmem = pl.BlockSpec(memory_space=pltpu.VMEM)
    hbm = pl.BlockSpec(memory_space=pl.ANY)
    sds = jax.ShapeDtypeStruct
    bufs = pl.pallas_call(
        kernel,
        out_shape=(
            sds((4, 256, 8, 128), BF16), sds((2, 16, WHOLE, 128), F32), sds((2, 16, EARLY, 128), F32),
            sds((8, 128), F32),
        ),
        in_specs=[hbm] * 13,
        out_specs=(hbm,) * 4,
        scratch_shapes=[
            pltpu.VMEM((4, 256, 8, 128), BF16),
            pltpu.VMEM((4, 256, 8, 128), BF16),
            pltpu.VMEM((2, 2048, 128), F32),
            pltpu.VMEM((64, 256), BF16),
            pltpu.VMEM((9, 64, 64), BF16),
            pltpu.VMEM((64, 256), BF16),
            pltpu.VMEM((4, 256), F32),
            pltpu.VMEM((4, 64), F32),
            pltpu.VMEM((4, 64), F32),
            pltpu.VMEM((4, 256), F32),
            pltpu.VMEM((1, 64), F32),
            pltpu.VMEM((1, 64), F32),
            pltpu.VMEM((1, 64), F32),
            pltpu.VMEM((1, 64), F32),
            pltpu.VMEM((4, 64, 256), BF16),
            pltpu.VMEM((4, 3, 192, 64), BF16),
            pltpu.VMEM((4, 3, 64, 192), BF16),
            pltpu.VMEM((4, 64, 256), BF16),
            pltpu.VMEM((64, 256), F32),
            pltpu.VMEM((4, 256, 1024), BF16),
            pltpu.VMEM((4, 256, 1024), BF16),
            pltpu.VMEM((4, 256, 1024), F32),
            pltpu.VMEM((4, 256, 1024), BF16),
            pltpu.VMEM((4, 64, 1024), BF16),
            pltpu.VMEM((3, 4, 64, 1280), F32),
            pltpu.VMEM((4, 192, 1280), BF16),
            pltpu.VMEM((4, 192, 1280), BF16),
            pltpu.VMEM((4, 64, 1024), F32),
            pltpu.VMEM((2, 4, 1, 256), F32),
            pltpu.VMEM((3, 2, 64, 128), F32),
            pltpu.VMEM((3, 2, 6, 64, 128), F32),
            pltpu.VMEM((8, 16, 8, 128), F32),
            pltpu.VMEM((8, 16, 8, 128), F32),
            pltpu.VMEM((64, 256), F32),
            pltpu.VMEM((64, 256), F32),
            pltpu.VMEM((9, 64, 64), F32),
            pltpu.VMEM((4, 2, 8, 128), F32),
            pltpu.VMEM((2, 16, 16, 128), F32),
            pltpu.VMEM((16, 16, 128), F32),
            pltpu.VMEM((16, 16, 128), F32),
            pltpu.VMEM((8, 16, 128), F32),
            pltpu.VMEM((16, 128), F32),
            pltpu.VMEM((2, 16, EARLY, 128), F32),
            pltpu.VMEM((16, EARLY, 128), F32),
            pltpu.VMEM((16, EARLY, 128), F32),
            pltpu.VMEM((8, EARLY, 128), F32),
            pltpu.VMEM((2, 16, EARLY, 128), F32),
            pltpu.VMEM((2, 16, LATE, 128), F32),
            pltpu.VMEM((16, LATE, 128), F32),
            pltpu.VMEM((16, LATE, 128), F32),
            pltpu.VMEM((8, LATE, 128), F32),
            pltpu.VMEM((2, 16, WHOLE, 128), F32),
            pltpu.VMEM((8, 128), F32),
            pltpu.VMEM((12, 4, 64, 1), F32),
            pltpu.SemaphoreType.DMA((20,)),
            pltpu.SemaphoreType.DMA((7,)),
            pltpu.SemaphoreType.DMA((24,)),
            pltpu.SemaphoreType.DMA((24,)),
            pltpu.SemaphoreType.DMA((6, 2)),
            pltpu.SemaphoreType.DMA((6, 2)),
            pltpu.SemaphoreType.DMA((5,)),
            pltpu.SemaphoreType.DMA((5,)),
        ],
        compiler_params=pltpu.CompilerParams(
            collective_id=0, has_side_effects=True, vmem_limit_bytes=67043328
        ),
        name="step",
    )(
        features, cotangent, reduce_weight.T, spatial_weight, expand_weight,
        reduce_factor, spatial_factor, expand_factor, output_factor,
        gain_first.reshape(1, 64), shift_first.reshape(1, 64),
        gain_second.reshape(1, 64), shift_second.reshape(1, 64),
    )
    outs = pl.pallas_call(
        unpack,
        out_shape=(
            sds((4, 256, 8, 128), BF16), sds((64, 256), F32), sds((9, 64, 64), F32), sds((64, 256), F32),
            sds((4, 256), F32), sds((4, 64), F32), sds((4, 64), F32), sds((4, 256), F32),
        ) + (sds((1, 64), F32),) * 4,
        in_specs=[hbm] * 4,
        out_specs=(hbm,) + (vmem,) * 11,
        scratch_shapes=[
            pltpu.VMEM((4, 256, 8, 128), BF16),
            pltpu.VMEM((2, 16, WHOLE, 128), F32),
            pltpu.VMEM((2, 16, EARLY, 128), F32),
            pltpu.VMEM((8, 128), F32),
            pltpu.SemaphoreType.DMA((11,)),
        ],
        compiler_params=pltpu.CompilerParams(vmem_limit_bytes=67043328),
        name="unpack",
    )(*bufs)
    return (outs[0], outs[1].T) + outs[2:8] + tuple(o.reshape(64) for o in outs[8:])


def solution(mesh):
    split = Mesh(
        mesh.devices.reshape(2, 4, 8, 2, 2), ("rows_0", "rows_1", "cols_0", "cols_1", "cols_2")
    )
    image = P(None, None, ROWS, COLS)
    return jax.shard_map(
        body,
        mesh=split,
        in_specs=(image, image) + (P(),) * 11,
        out_specs=(image,) + (P(),) * 11,
        check_vma=False,
    )
```

```python
import functools

import jax
import jax.numpy as jnp
from jax import lax
from jax.experimental import pallas as pl
from jax.experimental.pallas import tpu as pltpu
from jax.sharding import Mesh
from jax.sharding import PartitionSpec as P

ROWS = ("rows_0", "rows_1")
COLS = ("cols_0", "cols_1", "cols_2")
MESH = pl.DeviceIdType.MESH
EPSILON = 1e-05
F32 = jnp.float32
BF16 = jnp.bfloat16

EARLY, LATE, WHOLE = 8, 16, 24
OUTPUT_F, EXPAND_F, EARLY_TILES = 16, 17, 32
SPATIAL, REDUCE_F, SPATIAL_F, LATE_TILES = 16, 52, 53, 64


def dot(a, b, ca, cb):
    return lax.dot_general(a, b, (((ca,), (cb,)), ((), ())), preferred_element_type=F32)


def sigmoid(v):
    return 0.5 + 0.5 * jnp.tanh(0.5 * v)


def silu(v):
    return v * sigmoid(v)


def slope(v):
    s = sigmoid(v)
    return s * (1.0 + v * (1.0 - s))


def total(buf, n=16):
    t = buf[0]
    for k in range(1, n):
        t = t + buf[k]
    return t


def kernel(
    x_hbm, c_hbm, rw_hbm, sw_hbm, ew_hbm, rf_hbm, sf_hbm, ef_hbm, of_hbm, g1_hbm, b1_hbm, g2_hbm, b2_hbm,
    y_hbm, late_out, early_out, norms,
    xraw, craw, wide, rw, sw, ew, rf, sf, ef, of, g1, b1, g2, b2,
    w1, w2, w2b, w3, rwt,
    x, c, u, ulow, h2, hb, hq, dq, dpre1, nf, pk, pr, arb, ara,
    acce, accr, accs, sxs, bn, bn0, bn1, bn2, bnc, e, e0, e1, e2, e3, g, g0, g1_, g2_, g3, both, slope1, ep, cols,
    ld_sem, st_sem, s_sem, r_sem, hs_sem, hr_sem, cs_sem, cr_sem,
):
    count = float(64 * 4096)
    x_hi, y = lax.axis_index("rows_0"), lax.axis_index("rows_1")
    z, x_lo, core = lax.axis_index("cols_0"), lax.axis_index("cols_1"), lax.axis_index("cols_2")
    row = x_hi * 4 + y
    col = z * 4 + x_lo * 2 + core
    rank_a = x_hi * 8 + x_lo * 4 + y
    rank_b = z * 2 + core

    def peer_a(d):
        a = lax.rem(rank_a + d, 16)
        return (lax.div(a, 8), lax.rem(a, 4), z, lax.rem(lax.div(a, 4), 2), core)

    def peer_b(d):
        b = lax.rem(rank_b + d, 16)
        return (x_hi, y, lax.div(b, 2), x_lo, lax.rem(b, 2))

    def peer_z(d):
        return (x_hi, y, lax.rem(z + d, 8), x_lo, core)

    def at(dr, dc):
        rr, cc = lax.rem(row + dr + 8, 8), lax.rem(col + dc + 32, 32)
        return (lax.div(rr, 4), lax.rem(rr, 4), lax.div(cc, 4), lax.rem(lax.div(cc, 2), 2), lax.rem(cc, 2))

    sides = ((0, 1), (0, -1), (1, 1), (1, -1), (-1, 1), (-1, -1))

    barrier = pltpu.get_barrier_semaphore()

    def greet(d, _):
        pl.semaphore_signal(barrier, inc=1, device_id=peer_a(d), device_id_type=MESH)
        pl.semaphore_signal(barrier, inc=1, device_id=peer_b(d), device_id_type=MESH)
        return 0

    lax.fori_loop(1, 16, greet, 0)
    for side in sides:
        pl.semaphore_signal(barrier, inc=1, device_id=at(*side), device_id_type=MESH)

    pairs = (
        (rw_hbm, rw), (rf_hbm, rf), (sw_hbm, sw), (ew_hbm, ew), (sf_hbm, sf), (ef_hbm, ef), (of_hbm, of),
        (g1_hbm, g1), (b1_hbm, b1), (g2_hbm, g2), (b2_hbm, b2),
    )
    load_w = [pltpu.make_async_copy(a, b, ld_sem.at[8 + n]) for n, (a, b) in enumerate(pairs)]
    load_x = [pltpu.make_async_copy(x_hbm.at[m], xraw.at[m], ld_sem.at[m]) for m in range(4)]
    load_c = [pltpu.make_async_copy(c_hbm.at[m], craw.at[m], ld_sem.at[4 + m]) for m in range(4)]
    for copy in load_w[:2] + load_x + load_w[2:] + load_c:
        copy.start()

    def exchange(stage, src, buf, rank, peer, n=16):
        def start(d, _):
            pltpu.make_async_remote_copy(
                src_ref=src(d), dst_ref=buf.at[rank], send_sem=s_sem.at[stage],
                recv_sem=r_sem.at[stage], device_id=peer(d), device_id_type=MESH,
            ).start()
            return 0

        lax.fori_loop(1, n, start, 0)
        return together(buf.at[pl.ds(0, n - 1)], s_sem.at[stage], r_sem.at[stage]).wait

    def together(ref, send, recv):
        return pltpu.make_async_remote_copy(
            src_ref=ref, dst_ref=ref, send_sem=send, recv_sem=recv,
            device_id=(x_hi, y, z, x_lo, 1 - core), device_id_type=MESH,
        )

    def swap(stage, src, dst):
        copy = pltpu.make_async_remote_copy(
            src_ref=src, dst_ref=dst, send_sem=cs_sem.at[stage], recv_sem=cr_sem.at[stage],
            device_id=(x_hi, y, z, x_lo, 1 - core), device_id_type=MESH,
        )
        copy.start()
        return copy.wait

    def share_cores(stage, tiles, partner):
        return swap(stage, tiles.at[1 - core], partner)

    def share_plane(stage, wait, tiles, partner, buf):
        wait()
        for a in range(16):
            partner[a] = partner[a] + tiles[core, a]
        return exchange(stage, lambda d: partner.at[lax.rem(rank_a + d, 16)], buf, rank_a, peer_a)

    def share_depth(stage, wait, partner, buf, slots):
        wait()
        buf[rank_a] = partner[rank_a]
        slots[z] = total(buf)
        return exchange(stage, lambda d: slots.at[z], slots, z, peer_z, 8)

    def gather_plane(stage, whole):
        return exchange(stage, lambda d: whole.at[core, rank_a], whole.at[core], rank_a, peer_a)

    def gather_cores(stage, wait, whole):
        wait()
        return swap(stage, whole.at[core], whole.at[core])

    def sum_start(k, n, tile):
        arb[2 * k + n, rank_b] = tile
        return exchange(
            4 * k + 2 * n, lambda d: arb.at[2 * k + n, rank_b], arb.at[2 * k + n], rank_b, peer_b
        )

    def sum_middle(k, n, wait):
        wait()
        ara[2 * k + n, rank_a] = total(arb.at[2 * k + n])
        return exchange(
            4 * k + 2 * n + 1, lambda d: ara.at[2 * k + n, rank_a], ara.at[2 * k + n], rank_a, peer_a
        )

    def sum_end(k, n, wait):
        wait()
        return total(ara.at[2 * k + n])

    def halo(k, n):
        members = pl.ds(2 * n, 2)
        t = 2 * k + n
        copies = [
            pltpu.make_async_remote_copy(
                src_ref=hb.at[k, members, :, pl.ds(128, 128)],
                dst_ref=hb.at[k, members, :, pl.ds(1152, 128)],
                send_sem=hs_sem.at[t, 0], recv_sem=hr_sem.at[t, 0],
                device_id=at(-1, 0), device_id_type=MESH,
            ),
            pltpu.make_async_remote_copy(
                src_ref=hb.at[k, members, :, pl.ds(1024, 128)],
                dst_ref=hb.at[k, members, :, pl.ds(0, 128)],
                send_sem=hs_sem.at[t, 0], recv_sem=hr_sem.at[t, 0],
                device_id=at(1, 0), device_id_type=MESH,
            ),
        ]
        for edge, side in enumerate(sides):
            copies.append(
                pltpu.make_async_remote_copy(
                    src_ref=pk.at[k, n], dst_ref=pr.at[k, n, edge], send_sem=hs_sem.at[t, 1],
                    recv_sem=hr_sem.at[t, 1], device_id=at(*side), device_id_type=MESH,
                )
            )
        for copy in copies:
            copy.start()
        return [
            together(hb.at[k, :, :, pl.ds(0, 128)], hs_sem.at[t, 0], hr_sem.at[t, 0]),
            together(pr.at[k, n], hs_sem.at[t, 1], hr_sem.at[t, 1]),
        ]

    lane = lax.broadcasted_iota(jnp.int32, (64, 128), 1)
    sub = lax.broadcasted_iota(jnp.int32, (8, 128), 0)
    zero = jnp.zeros((64, 128), F32)

    def put(acc, n, value):
        return jnp.where(lane == n, value, acc)

    def rows_of_columns(acc):
        return jnp.transpose(jnp.concatenate([acc, jnp.zeros((64, 128), F32)], axis=0))[:8]

    def columns_of_rows(tile, k, members):
        t = jnp.transpose(jnp.concatenate([tile, jnp.zeros((120, 128), F32)], axis=0))
        for m in members:
            cols[k, m] = t[:64, m : m + 1]
            cols[k + 1, m] = t[:64, 4 + m : 5 + m]

    def sums(m, acc, a, b):
        acc = put(acc, m, jnp.sum(a, axis=1, keepdims=True))
        return put(acc, 4 + m, jnp.sum(b, axis=1, keepdims=True))

    def pack(k, n):
        acc = zero
        for m in group(n):
            for i in range(8):
                t = hb[k, m, :, 128 + i * 128 : 256 + i * 128]
                acc = put(acc, m * 8 + i, t[:, 0:1])
                acc = put(acc, 32 + m * 8 + i, t[:, 127:128])
        pk[k, n] = acc

    def group(n):
        return (2 * n, 2 * n + 1)

    top = jnp.where(row > 0, 1.0, 0.0).astype(F32)
    bottom = jnp.where(row < 7, 1.0, 0.0).astype(F32)
    left = jnp.where(col > 0, 1.0, 0.0).astype(F32)
    right = jnp.where(col < 31, 1.0, 0.0).astype(F32)
    masks = (left, right, top * left, top * right, bottom * left, bottom * right)

    def spread(dst, m, tile, edge):
        edges = [edge(e) * masks[e] for e in range(6)]
        for i in range(10):
            t = tile(i)
            if i == 0:
                t, e0, e2, at_row = t * top, edges[2], edges[3], 7
            elif i == 9:
                t, e0, e2, at_row = t * bottom, edges[4], edges[5], 0
            else:
                e0, e2, at_row = edges[0], edges[1], i - 1
            where0 = 32 + m * 8 + at_row
            where2 = m * 8 + at_row
            before = jnp.where(
                lane == 0, pltpu.roll(e0, 128 - where0, axis=1), pltpu.roll(t, 1, axis=1)
            )
            after = jnp.where(
                lane == 127, pltpu.roll(e2, 127 - where2, axis=1), pltpu.roll(t, 127, axis=1)
            )
            span = slice(i * 128, i * 128 + 128)
            dst[m, 0:64, span] = before.astype(BF16)
            dst[m, 64:128, span] = t.astype(BF16)
            dst[m, 128:192, span] = after.astype(BF16)

    def flatten(src, dst, m):
        wide[m % 2] = src[m].astype(F32).reshape(2048, 128)
        for i in range(8):
            dst[m, :, i * 128 : i * 128 + 128] = wide[m % 2, pl.ds(i, 256, stride=8), :].astype(BF16)

    def moments(k, tile, members):
        columns_of_rows(tile, k, members)
        for m in members:
            mean = cols[k, m] / count
            var = cols[k + 1, m] / count - mean * mean
            cols[k, m] = mean
            cols[k + 1, m] = lax.rsqrt(var + EPSILON)

    for copy in load_w[:2]:
        copy.wait()
    rwt[...] = rw[...].astype(F32)
    for m in range(4):
        w1[m] = (rwt[...] * rf[m : m + 1]).astype(BF16)
    ones = jnp.ones((8, 1024), BF16)

    def free_rows(m):
        base = 2 if m < 2 else 0
        return (base + 4 * (m % 2), base + 4 * (m % 2) + 1)

    stats, halos = [None, None], [None, None]
    for n in range(2):
        acc = zero
        extra = []
        for m in group(n):
            load_x[m].wait()
            flatten(xraw, x, m)
            a = dot(w1[m], x[m], 1, 0)
            hb[0, m, :, 128:1152] = a
            acc = sums(m, acc, a, a * a)
            extra.append((m, dot(ones, x[m], 1, 1)))
        tile = rows_of_columns(acc)
        for m, line in extra:
            for h, r in enumerate(free_rows(m)):
                tile = jnp.where(sub == r, line[:, h * 128 : h * 128 + 128], tile)
        if n == 0:
            pl.semaphore_wait(barrier, 36)
        stats[n] = sum_start(0, n, tile)
        pack(0, n)
        halos[n] = halo(0, n)

    for copy in load_w[2:]:
        copy.wait()
    tail = jnp.zeros((8, 64), F32)
    columns_of_rows(
        jnp.concatenate([jnp.concatenate([sf[...], ef[...]], axis=0), tail], axis=1), 8, range(4)
    )
    columns_of_rows(
        jnp.concatenate(
            [jnp.concatenate([g1[...], b1[...], g2[...], b2[...], tail[:4]], axis=0), tail], axis=1
        ), 10, range(4),
    )
    for m in range(4):
        sfm, efm = cols[8, m], cols[9, m]
        w3[m] = (efm * ew[...].astype(F32) * of[m : m + 1]).astype(BF16)
        for p in range(3):
            taps = [(sfm * sw[3 * p + q].astype(F32)).astype(BF16) for q in range(3)]
            for q in range(3):
                w2[m, p, q * 64 : q * 64 + 64] = taps[q]
            w2b[m, 2 - p] = jnp.concatenate(taps[::-1], axis=1)
    gain1, shift1, gain2, shift2 = (cols[10, n] for n in range(4))
    for copy in load_c:
        copy.wait()
    for m in range(4):
        flatten(craw, c, m)
    stats[0] = sum_middle(0, 0, stats[0])
    stats[1] = sum_middle(0, 1, stats[1])

    for n in range(2):
        tile = sum_end(0, n, stats[n])
        moments(0, tile, group(n))
        for m in group(n):
            for h, r in enumerate(free_rows(m)):
                sxs[m, h] = jnp.broadcast_to(tile[r : r + 1], (8, 128))
        for copy in halos[n]:
            copy.wait()
        acc = zero
        for m in group(n):
            mean, rstd = cols[0, m], cols[1, m]

            def hidden(v):
                return silu(gain1 * ((v - mean) * rstd) + shift1)

            spread(
                hq, m, lambda i: hidden(hb[0, m, :, i * 128 : i * 128 + 128]),
                lambda e: hidden(pr[0, n, e]),
            )
            a = dot(w2[m, 0], hq[m, :, 0:1024], 0, 0)
            a = a + dot(w2[m, 1], hq[m, :, 128:1152], 0, 0)
            a = a + dot(w2[m, 2], hq[m, :, 256:1280], 0, 0)
            hb[1, m, :, 128:1152] = a
            acc = sums(m, acc, a, a * a)
        stats[n] = sum_start(1, n, rows_of_columns(acc))
        pack(1, n)
        halos[n] = halo(1, n)

    def project(m):
        normed = (hb[0, m, :, 128:1152] - cols[0, m]) * cols[1, m]
        slope1[m] = slope(gain1 * normed + shift1)
        part = dot(normed.astype(BF16), x[m], 1, 1)
        for a in range(16):
            h, f = a // 8, a % 8
            bn[m // 2, a, m % 2 * 8 : m % 2 * 8 + 8] = part[f * 8 : f * 8 + 8, h * 128 : h * 128 + 128]

    for m in range(4):
        project(m)
    corrections = share_cores(0, bn, bn0)
    stats[0] = sum_middle(1, 0, stats[0])
    stats[1] = sum_middle(1, 1, stats[1])
    corrections = share_plane(16, corrections, bn, bn0, bn1)

    sums2 = []
    for n in range(2):
        moments(2, sum_end(1, n, stats[n]), group(n))
        for copy in halos[n]:
            copy.wait()
        acc = zero
        for m in group(n):
            mean, rstd = cols[2, m], cols[3, m]
            for o in range(0, 1024, 256):
                span = slice(o, o + 256)
                pre = gain2 * ((hb[1, m, :, o + 128 : o + 384] - mean) * rstd) + shift2
                s = sigmoid(pre)
                h2[m, :, span] = (pre * s).astype(BF16)
                dpre1[m, :, span] = s * (1.0 + pre * (1.0 - s))
                third = dot(w3[m], h2[m, :, span], 0, 0)
                up = c[m, :, span].astype(F32) * slope(x[m, :, span].astype(F32) + third)
                u[m, :, span] = up
                ulow[m, :, span] = up.astype(BF16)
            back = dot(w3[m], ulow[m], 1, 0)
            hb[2, m, :, 128:1152] = back
            dpre = back * dpre1[m]
            acc = sums(m, acc, dpre, dpre * ((hb[1, m, :, 128:1152] - mean) * rstd))
        stats[n] = sum_start(2, n, rows_of_columns(acc))
        pack(2, n)
        halos[n] = halo(2, n)

    fac = zero

    def expand(m, fac):
        part = dot(h2[m], ulow[m], 1, 1)
        ofm, efm = of[m : m + 1], cols[9, m]
        scaled = part * efm * ofm
        acce[...] = scaled if m == 0 else acce[...] + scaled
        byw = part * ew[...].astype(F32)
        nf[1, m] = jnp.sum(byw * efm, axis=0, keepdims=True)
        return put(fac, m, jnp.sum(byw * ofm, axis=1, keepdims=True))

    for m in range(4):
        fac = expand(m, fac)

    def place(buf, t, value):
        r = t // 32 * 8
        buf[t // 16 % 2, t % 16, r : r + 8] = value

    def lines(k):
        return jnp.concatenate(
            [nf[k, m, :, h * 128 : h * 128 + 128] for h in range(2) for m in range(4)], axis=0
        )

    for a in range(16):
        h, f = a // 8, a % 8
        place(e, a, acce[f * 8 : f * 8 + 8, h * 128 : h * 128 + 128])
    place(e, OUTPUT_F, lines(1))
    place(e, EXPAND_F, rows_of_columns(fac))
    for t in range(EXPAND_F + 1, EARLY_TILES):
        place(e, t, jnp.zeros((8, 128), F32))
    early = share_cores(1, e, e0)

    def prepare(n):
        for copy in halos[n]:
            copy.wait()
        for m in group(n):
            mean, rstd = cols[2, m], cols[3, m]
            scale = gain2 * rstd

            def halves(second, back):
                normed = (second - mean) * rstd
                return scale * normed, scale * (back * slope(gain2 * normed + shift2))

            for i in range(10):
                span = slice(i * 128, i * 128 + 128)
                hb[1, m, :, span], hb[2, m, :, span] = halves(hb[1, m, :, span], hb[2, m, :, span])
            for edge in range(6):
                ep[0, m, edge], ep[1, m, edge] = halves(pr[1, n, edge], pr[2, n, edge])

    stats[0] = sum_middle(2, 0, stats[0])
    prepare(0)
    stats[1] = sum_middle(2, 1, stats[1])
    prepare(1)
    early = share_plane(18, early, e, e0, e1)
    corrections = share_depth(17, corrections, bn0, bn1, bn2)

    for n in range(2):
        tile = sum_end(2, n, stats[n])
        sums2.append(tile)
        columns_of_rows(tile, 4, group(n))
        acc = zero
        for m in group(n):
            plain, weighted = gain2 * cols[3, m] * cols[4, m] / count, cols[5, m] / count

            def dact(normed, part):
                return part - plain - normed * weighted

            spread(
                dq, m,
                lambda i: dact(hb[1, m, :, i * 128 : i * 128 + 128], hb[2, m, :, i * 128 : i * 128 + 128]),
                lambda edge: dact(ep[0, m, edge], ep[1, m, edge]),
            )
            a = dot(w2b[m, 0], dq[m, :, 0:1024], 1, 0)
            a = a + dot(w2b[m, 1], dq[m, :, 128:1152], 1, 0)
            a = a + dot(w2b[m, 2], dq[m, :, 256:1280], 1, 0)
            normed = (hb[0, m, :, 128:1152] - cols[0, m]) * cols[1, m]
            dpre = a * slope1[m]
            dpre1[m] = dpre
            acc = sums(m, acc, dpre, dpre * normed)
        stats[n] = sum_start(3, n, rows_of_columns(acc))

    def gradients(m, fac):
        sfm = cols[8, m]
        byf = jnp.zeros((64, 1), F32)
        for p in range(3):
            part = dot(hq[m, :, p * 128 : p * 128 + 1024], dq[m, 64:128, 128:1152], 1, 1)
            for q in range(3):
                k = 3 * p + q
                tap = part[q * 64 : q * 64 + 64]
                byf = byf + jnp.sum(tap * sw[k].astype(F32), axis=1, keepdims=True)
                tap = tap * sfm
                accs[k] = tap if m == 0 else accs[k] + tap
        part = dot(dpre1[m].astype(BF16), x[m], 1, 1) * (gain1 * cols[1, m])
        scaled = part * rf[m : m + 1]
        accr[...] = scaled if m == 0 else accr[...] + scaled
        nf[0, m] = jnp.sum(part * rwt[...], axis=0, keepdims=True)
        return put(fac, m, byf)

    fac = zero
    for m in range(4):
        fac = gradients(m, fac)
    for a in range(16):
        h, f = a // 8, a % 8
        place(g, a, accr[f * 8 : f * 8 + 8, h * 128 : h * 128 + 128])
    for t in range(36):
        low, high = t * 8, 288 + t * 8
        place(g, SPATIAL + t, jnp.concatenate(
            [accs[low // 64, low % 64 : low % 64 + 8], accs[high // 64, high % 64 : high % 64 + 8]], axis=1
        ))
    place(g, REDUCE_F, lines(0))
    place(g, SPATIAL_F, rows_of_columns(fac))
    for t in range(SPATIAL_F + 1, LATE_TILES):
        place(g, t, jnp.zeros((8, 128), F32))
    late = share_cores(2, g, g0)
    early = share_depth(19, early, e0, e1, e2)
    late = share_plane(21, late, g, g0, g1_)
    stats[0] = sum_middle(3, 0, stats[0])
    stats[1] = sum_middle(3, 1, stats[1])
    corrections()
    bnc[...] = total(bn2, 8)
    early()
    e3[core, rank_a] = total(e2, 8)
    early = gather_plane(20, e3)

    def finish(m):
        mean, rstd, plain, weighted = cols[0, m], cols[1, m], cols[6, m] / count, cols[7, m] / count
        normed = (hb[0, m, :, 128:1152] - mean) * rstd
        dq[m, 0:64, 0:1024] = (gain1 * rstd * (dpre1[m] - plain - normed * weighted)).astype(BF16)
        for j in range(4):
            o = j * 256
            t = u[m, :, o : o + 256] + dot(w1[m], dq[m, 0:64, o : o + 256], 0, 0)
            wide[m % 2, pl.ds(2 * j, 256, stride=8), :] = t[:, :128]
            wide[m % 2, pl.ds(2 * j + 1, 256, stride=8), :] = t[:, 128:]
        craw[m] = wide[m % 2].reshape(256, 8, 128).astype(BF16)
        store = pltpu.make_async_copy(craw.at[m], y_hbm.at[m], st_sem.at[m])
        store.start()
        return store

    tile = sum_end(3, 0, stats[0])
    sums1 = [tile]
    columns_of_rows(tile, 6, group(0))
    late = share_depth(22, late, g0, g1_, g2_)
    stores = [finish(0), finish(1)]
    tile = sum_end(3, 1, stats[1])
    sums1.append(tile)
    columns_of_rows(tile, 6, group(1))

    half, block = lax.div(rank_a, 8), pl.ds(pl.multiple_of(lax.rem(rank_a, 8) * 8, 8), 8)
    span = pl.ds(pl.multiple_of(half * 128, 128), 128)
    fix = jnp.zeros((8, 128), F32)
    part = jnp.zeros((8, 128), F32)
    for k in range(2):
        m = 2 * core + k
        plain, weighted = cols[6, m, block] / count, cols[7, m, block] / count
        v = cols[10, 0, block] * cols[1, m, block] * (
            plain * sxs[m, half] + weighted * bnc[k * 8 : k * 8 + 8]
        )
        fix = fix + v * jnp.where(core == 0, rf[k : k + 1, span], rf[k + 2 : k + 3, span])
        part = jnp.where(
            sub == half * 4 + m, jnp.sum(v * rwt[block, span], axis=0, keepdims=True), part
        )
    both[core, 0:8] = fix
    both[core, 8:16] = part
    swap(5, both.at[core], both.at[core])()
    fix = jnp.where(core == 0, both[0, 0:8] + both[1, 0:8], 0.0)
    late()
    share = total(g2_, 8)
    g3[core, rank_a, 0:8] = share[0:8] - fix
    g3[core, rank_a, 8:LATE] = share[8:LATE]
    g3[core, rank_a, LATE:WHOLE] = both[0, 8:16] + both[1, 8:16]
    late = gather_plane(23, g3)
    early = gather_cores(3, early, e3)
    stores += [finish(2), finish(3)]
    first, second = sums1[0] + sums1[1], sums2[0] + sums2[1]
    norms[...] = jnp.concatenate(
        [
            jnp.sum(first[4:8], axis=0, keepdims=True),
            jnp.sum(first[0:4], axis=0, keepdims=True),
            jnp.sum(second[4:8], axis=0, keepdims=True),
            jnp.sum(second[0:4], axis=0, keepdims=True),
            jnp.zeros((4, 128), F32),
        ],
        axis=0,
    )
    late = gather_cores(4, late, g3)
    early()
    early_out[...] = e3[...]
    late()
    late_out[...] = g3[...]
    for copy in stores:
        copy.wait()


def unpack(
    y_hbm, whole, expand, norms,
    out_hbm, o_reduce, o_spatial, o_expand, o_rf, o_sf, o_ef, o_of, o_g1, o_b1, o_g2, o_b2,
    sem,
):
    store = [pltpu.make_async_copy(y_hbm.at[m], out_hbm.at[m], sem.at[m]) for m in range(4)]
    for copy in store:
        copy.start()

    def early(t):
        return expand[t // 16, t % 16]

    def late(t):
        return whole[t // 16 % 2, t % 16, t // 32 * 8 : t // 32 * 8 + 8]

    fix = jnp.zeros((8, 128), F32)
    for a in range(16):
        h, f = a // 8, a % 8
        o_expand[f * 8 : f * 8 + 8, h * 128 : h * 128 + 128] = early(a)
        o_reduce[f * 8 : f * 8 + 8, h * 128 : h * 128 + 128] = late(a)
        fix = fix + whole[0, a, LATE:WHOLE]
    for t in range(36):
        both = late(SPATIAL + t)
        for n in range(2):
            r = n * 288 + t * 8
            o_spatial[r // 64, r % 64 : r % 64 + 8] = both[:, n * 64 : n * 64 + 64]
    for o, e in ((o_rf, late(REDUCE_F) - fix), (o_of, early(OUTPUT_F))):
        o[:, :128] = e[:4]
        o[:, 128:] = e[4:]
    o_ef[...] = early(EXPAND_F)[:4, :64]
    o_sf[...] = late(SPATIAL_F)[:4, :64]
    for n, o in enumerate((o_g1, o_b1, o_g2, o_b2)):
        o[...] = norms[n : n + 1, :64]
    for copy in store:
        copy.wait()


def body(
    features, cotangent, reduce_weight, spatial_weight, expand_weight,
    reduce_factor, spatial_factor, expand_factor, output_factor,
    gain_first, shift_first, gain_second, shift_second,
):
    vmem = pl.BlockSpec(memory_space=pltpu.VMEM)
    hbm = pl.BlockSpec(memory_space=pl.ANY)
    sds = jax.ShapeDtypeStruct
    bufs = pl.pallas_call(
        kernel,
        out_shape=(
            sds((4, 256, 8, 128), BF16), sds((2, 16, WHOLE, 128), F32), sds((2, 16, EARLY, 128), F32),
            sds((8, 128), F32),
        ),
        in_specs=[pl.BlockSpec(memory_space=pltpu.HBM)] * 13,
        out_specs=(hbm, vmem, vmem, vmem),
        scratch_shapes=[
            pltpu.VMEM((4, 256, 8, 128), BF16),
            pltpu.VMEM((4, 256, 8, 128), BF16),
            pltpu.VMEM((2, 2048, 128), F32),
            pltpu.VMEM((64, 256), BF16),
            pltpu.VMEM((9, 64, 64), BF16),
            pltpu.VMEM((64, 256), BF16),
            pltpu.VMEM((4, 256), F32),
            pltpu.VMEM((4, 64), F32),
            pltpu.VMEM((4, 64), F32),
            pltpu.VMEM((4, 256), F32),
            pltpu.VMEM((1, 64), F32),
            pltpu.VMEM((1, 64), F32),
            pltpu.VMEM((1, 64), F32),
            pltpu.VMEM((1, 64), F32),
            pltpu.VMEM((4, 64, 256), BF16),
            pltpu.VMEM((4, 3, 192, 64), BF16),
            pltpu.VMEM((4, 3, 64, 192), BF16),
            pltpu.VMEM((4, 64, 256), BF16),
            pltpu.VMEM((64, 256), F32),
            pltpu.VMEM((4, 256, 1024), BF16),
            pltpu.VMEM((4, 256, 1024), BF16),
            pltpu.VMEM((4, 256, 1024), F32),
            pltpu.VMEM((4, 256, 1024), BF16),
            pltpu.VMEM((4, 64, 1024), BF16),
            pltpu.VMEM((3, 4, 64, 1280), F32),
            pltpu.VMEM((4, 192, 1280), BF16),
            pltpu.VMEM((4, 192, 1280), BF16),
            pltpu.VMEM((4, 64, 1024), F32),
            pltpu.VMEM((2, 4, 1, 256), F32),
            pltpu.VMEM((3, 2, 64, 128), F32),
            pltpu.VMEM((3, 2, 6, 64, 128), F32),
            pltpu.VMEM((8, 16, 8, 128), F32),
            pltpu.VMEM((8, 16, 8, 128), F32),
            pltpu.VMEM((64, 256), F32),
            pltpu.VMEM((64, 256), F32),
            pltpu.VMEM((9, 64, 64), F32),
            pltpu.VMEM((4, 2, 8, 128), F32),
            pltpu.VMEM((2, 16, 16, 128), F32),
            pltpu.VMEM((16, 16, 128), F32),
            pltpu.VMEM((16, 16, 128), F32),
            pltpu.VMEM((8, 16, 128), F32),
            pltpu.VMEM((16, 128), F32),
            pltpu.VMEM((2, 16, EARLY, 128), F32),
            pltpu.VMEM((16, EARLY, 128), F32),
            pltpu.VMEM((16, EARLY, 128), F32),
            pltpu.VMEM((8, EARLY, 128), F32),
            pltpu.VMEM((2, 16, EARLY, 128), F32),
            pltpu.VMEM((2, 16, LATE, 128), F32),
            pltpu.VMEM((16, LATE, 128), F32),
            pltpu.VMEM((16, LATE, 128), F32),
            pltpu.VMEM((8, LATE, 128), F32),
            pltpu.VMEM((2, 16, WHOLE, 128), F32),
            pltpu.VMEM((2, 16, 128), F32),
            pltpu.VMEM((4, 64, 1024), F32),
            pltpu.VMEM((2, 4, 6, 64, 128), F32),
            pltpu.VMEM((12, 4, 64, 1), F32),
            pltpu.SemaphoreType.DMA((20,)),
            pltpu.SemaphoreType.DMA((4,)),
            pltpu.SemaphoreType.DMA((24,)),
            pltpu.SemaphoreType.DMA((24,)),
            pltpu.SemaphoreType.DMA((6, 2)),
            pltpu.SemaphoreType.DMA((6, 2)),
            pltpu.SemaphoreType.DMA((6,)),
            pltpu.SemaphoreType.DMA((6,)),
        ],
        compiler_params=pltpu.CompilerParams(
            collective_id=0, has_side_effects=True, vmem_limit_bytes=44 * 1024 * 1024
        ),
        name="step",
    )(*[pltpu.with_memory_space_constraint(v, pltpu.HBM) for v in (
        features, cotangent, reduce_weight.T, spatial_weight, expand_weight,
        reduce_factor, spatial_factor, expand_factor, output_factor,
        gain_first.reshape(1, 64), shift_first.reshape(1, 64),
        gain_second.reshape(1, 64), shift_second.reshape(1, 64),
    )])
    outs = pl.pallas_call(
        unpack,
        out_shape=(
            sds((4, 256, 8, 128), BF16), sds((64, 256), F32), sds((9, 64, 64), F32), sds((64, 256), F32),
            sds((4, 256), F32), sds((4, 64), F32), sds((4, 64), F32), sds((4, 256), F32),
        ) + (sds((1, 64), F32),) * 4,
        in_specs=[hbm, vmem, vmem, vmem],
        out_specs=(hbm,) + (vmem,) * 11,
        scratch_shapes=[
            pltpu.SemaphoreType.DMA((4,)),
        ],
        compiler_params=pltpu.CompilerParams(vmem_limit_bytes=8 * 1024 * 1024),
        name="unpack",
    )(*bufs)
    return (outs[0], outs[1].T) + outs[2:8] + tuple(o.reshape(64) for o in outs[8:])


def solution(mesh):
    split = Mesh(
        mesh.devices.reshape(2, 4, 8, 2, 2), ("rows_0", "rows_1", "cols_0", "cols_1", "cols_2")
    )
    image = P(None, None, ROWS, COLS)
    return jax.shard_map(
        body,
        mesh=split,
        in_specs=(image, image) + (P(),) * 11,
        out_specs=(image,) + (P(),) * 11,
        check_vma=False,
    )
```

```python
import functools

import jax
import jax.numpy as jnp
from jax import lax
from jax.experimental import pallas as pl
from jax.experimental.pallas import tpu as pltpu
from jax.sharding import Mesh
from jax.sharding import PartitionSpec as P

ROWS = ("rows_0", "rows_1")
COLS = ("cols_0", "cols_1", "cols_2")
MESH = pl.DeviceIdType.MESH
EPSILON = 1e-05
F32 = jnp.float32
BF16 = jnp.bfloat16

EARLY, LATE, WHOLE = 8, 16, 24
OUTPUT_F, EXPAND_F, EARLY_TILES = 16, 17, 32
SPATIAL, REDUCE_F, SPATIAL_F, LATE_TILES = 16, 52, 53, 64


def dot(a, b, ca, cb):
    return lax.dot_general(a, b, (((ca,), (cb,)), ((), ())), preferred_element_type=F32)


def sigmoid(v):
    return 0.5 + 0.5 * jnp.tanh(0.5 * v)


def silu(v):
    return v * sigmoid(v)


def slope(v):
    s = sigmoid(v)
    return s * (1.0 + v * (1.0 - s))


def total(buf, n=16):
    t = buf[0]
    for k in range(1, n):
        t = t + buf[k]
    return t


def kernel(
    x_hbm, c_hbm, rw_hbm, sw_hbm, ew_hbm, rf_hbm, sf_hbm, ef_hbm, of_hbm, g1_hbm, b1_hbm, g2_hbm, b2_hbm,
    y_hbm, late_out, early_out, norms,
    xraw, craw, wide, rw, sw, ew, rf, sf, ef, of, g1, b1, g2, b2,
    w1, w2, w2b, w3, rwt,
    x, c, u, ulow, h2, hb, hq, dq, dpre1, nf, pk, pr, arb, ara,
    acce, accr, accs, sxs, bn, bn0, bn1, bn2, bnc, e, e0, e1, e2, e3, g, g0, g1_, g2_, g3, both, slope1, ep, cols,
    ld_sem, st_sem, s_sem, r_sem, hs_sem, hr_sem, cs_sem, cr_sem,
):
    count = float(64 * 4096)
    x_hi, y = lax.axis_index("rows_0"), lax.axis_index("rows_1")
    z, x_lo, core = lax.axis_index("cols_0"), lax.axis_index("cols_1"), lax.axis_index("cols_2")
    row = x_hi * 4 + y
    col = z * 4 + x_lo * 2 + core
    rank_a = x_hi * 8 + x_lo * 4 + y
    rank_b = z * 2 + core

    def peer_a(d):
        a = lax.rem(rank_a + d, 16)
        return (lax.div(a, 8), lax.rem(a, 4), z, lax.rem(lax.div(a, 4), 2), core)

    def peer_b(d):
        b = lax.rem(rank_b + d, 16)
        return (x_hi, y, lax.div(b, 2), x_lo, lax.rem(b, 2))

    def peer_z(d):
        return (x_hi, y, lax.rem(z + d, 8), x_lo, core)

    def at(dr, dc):
        rr, cc = lax.rem(row + dr + 8, 8), lax.rem(col + dc + 32, 32)
        return (lax.div(rr, 4), lax.rem(rr, 4), lax.div(cc, 4), lax.rem(lax.div(cc, 2), 2), lax.rem(cc, 2))

    sides = ((0, 1), (0, -1), (1, 1), (1, -1), (-1, 1), (-1, -1))

    pairs = (
        (rw_hbm, rw), (rf_hbm, rf), (sw_hbm, sw), (ew_hbm, ew), (sf_hbm, sf), (ef_hbm, ef), (of_hbm, of),
        (g1_hbm, g1), (b1_hbm, b1), (g2_hbm, g2), (b2_hbm, b2),
    )
    load_w = [pltpu.make_async_copy(a, b, ld_sem.at[8 + n]) for n, (a, b) in enumerate(pairs)]
    load_x = [pltpu.make_async_copy(x_hbm.at[m], xraw.at[m], ld_sem.at[m]) for m in range(4)]
    load_c = [pltpu.make_async_copy(c_hbm.at[m], craw.at[m], ld_sem.at[4 + m]) for m in range(4)]
    for copy in load_w[:2] + load_x:
        copy.start()

    barrier = pltpu.get_barrier_semaphore()

    def greet(d, _):
        pl.semaphore_signal(barrier, inc=1, device_id=peer_a(d), device_id_type=MESH)
        pl.semaphore_signal(barrier, inc=1, device_id=peer_b(d), device_id_type=MESH)
        return 0

    lax.fori_loop(1, 16, greet, 0)
    for side in sides:
        pl.semaphore_signal(barrier, inc=1, device_id=at(*side), device_id_type=MESH)
    for copy in load_w[2:] + load_c:
        copy.start()

    def exchange(stage, src, buf, rank, peer, n=16):
        def start(d, _):
            pltpu.make_async_remote_copy(
                src_ref=src(d), dst_ref=buf.at[rank], send_sem=s_sem.at[stage],
                recv_sem=r_sem.at[stage], device_id=peer(d), device_id_type=MESH,
            ).start()
            return 0

        lax.fori_loop(1, n, start, 0)
        return together(buf.at[pl.ds(0, n - 1)], s_sem.at[stage], r_sem.at[stage]).wait

    def together(ref, send, recv):
        return pltpu.make_async_remote_copy(
            src_ref=ref, dst_ref=ref, send_sem=send, recv_sem=recv,
            device_id=(x_hi, y, z, x_lo, 1 - core), device_id_type=MESH,
        )

    def swap(stage, src, dst):
        copy = pltpu.make_async_remote_copy(
            src_ref=src, dst_ref=dst, send_sem=cs_sem.at[stage], recv_sem=cr_sem.at[stage],
            device_id=(x_hi, y, z, x_lo, 1 - core), device_id_type=MESH,
        )
        copy.start()
        return copy.wait

    def share_cores(stage, tiles, partner):
        return swap(stage, tiles.at[1 - core], partner)

    def share_plane(stage, wait, tiles, partner, buf):
        wait()
        for a in range(16):
            partner[a] = partner[a] + tiles[core, a]
        return exchange(stage, lambda d: partner.at[lax.rem(rank_a + d, 16)], buf, rank_a, peer_a)

    def share_depth(stage, wait, partner, buf, slots):
        wait()
        buf[rank_a] = partner[rank_a]
        slots[z] = total(buf)
        return exchange(stage, lambda d: slots.at[z], slots, z, peer_z, 8)

    def gather_plane(stage, whole):
        return exchange(stage, lambda d: whole.at[core, rank_a], whole.at[core], rank_a, peer_a)

    def gather_cores(stage, wait, whole):
        wait()
        return swap(stage, whole.at[core], whole.at[core])

    def sum_start(k, n, tile):
        arb[2 * k + n, rank_b] = tile
        return exchange(
            4 * k + 2 * n, lambda d: arb.at[2 * k + n, rank_b], arb.at[2 * k + n], rank_b, peer_b
        )

    def sum_middle(k, n, wait):
        wait()
        ara[2 * k + n, rank_a] = total(arb.at[2 * k + n])
        return exchange(
            4 * k + 2 * n + 1, lambda d: ara.at[2 * k + n, rank_a], ara.at[2 * k + n], rank_a, peer_a
        )

    def sum_end(k, n, wait):
        wait()
        return total(ara.at[2 * k + n])

    def halo(k, n):
        members = pl.ds(2 * n, 2)
        t = 2 * k + n
        copies = [
            pltpu.make_async_remote_copy(
                src_ref=hb.at[k, members, :, pl.ds(128, 128)],
                dst_ref=hb.at[k, members, :, pl.ds(1152, 128)],
                send_sem=hs_sem.at[t, 0], recv_sem=hr_sem.at[t, 0],
                device_id=at(-1, 0), device_id_type=MESH,
            ),
            pltpu.make_async_remote_copy(
                src_ref=hb.at[k, members, :, pl.ds(1024, 128)],
                dst_ref=hb.at[k, members, :, pl.ds(0, 128)],
                send_sem=hs_sem.at[t, 0], recv_sem=hr_sem.at[t, 0],
                device_id=at(1, 0), device_id_type=MESH,
            ),
        ]
        for edge, side in enumerate(sides):
            copies.append(
                pltpu.make_async_remote_copy(
                    src_ref=pk.at[k, n, (side[1] + 1) // 2], dst_ref=pr.at[k, n, edge], send_sem=hs_sem.at[t, 1],
                    recv_sem=hr_sem.at[t, 1], device_id=at(*side), device_id_type=MESH,
                )
            )
        for copy in copies:
            copy.start()
        return [
            together(hb.at[k, :, :, pl.ds(0, 128)], hs_sem.at[t, 0], hr_sem.at[t, 0]),
            together(pr.at[k, n], hs_sem.at[t, 1], hr_sem.at[t, 1]),
        ]

    lane = lax.broadcasted_iota(jnp.int32, (64, 128), 1)
    sub = lax.broadcasted_iota(jnp.int32, (8, 128), 0)
    zero = jnp.zeros((64, 128), F32)

    def put(acc, n, value):
        return jnp.where(lane == n, value, acc)

    def rows_of_columns(acc):
        return jnp.transpose(jnp.concatenate([acc, jnp.zeros((64, 128), F32)], axis=0))[:8]

    def columns_of_rows(tile, k, members):
        t = jnp.transpose(jnp.concatenate([tile, jnp.zeros((120, 128), F32)], axis=0))
        for m in members:
            cols[k, m] = t[:64, m : m + 1]
            cols[k + 1, m] = t[:64, 4 + m : 5 + m]

    def sums(m, acc, a, b):
        acc = put(acc, m, jnp.sum(a, axis=1, keepdims=True))
        return put(acc, 4 + m, jnp.sum(b, axis=1, keepdims=True))

    def pack(k, n):
        acc = zero
        for m in group(n):
            for i in range(8):
                t = hb[k, m, :, 128 + i * 128 : 256 + i * 128]
                acc = put(acc, m % 2 * 8 + i, t[:, 0:1])
                acc = put(acc, 16 + m % 2 * 8 + i, t[:, 127:128])
        t = jnp.transpose(jnp.concatenate([acc, zero], axis=0))
        pk[k, n, 0] = t[0:16]
        pk[k, n, 1] = t[16:32]

    def received(k, n):
        t = jnp.concatenate([pr[k, n, e] for e in range(6)] + [jnp.zeros((32, 128), F32)], axis=0)
        return jnp.transpose(t)[:64]

    def group(n):
        return (2 * n, 2 * n + 1)

    top = jnp.where(row > 0, 1.0, 0.0).astype(F32)
    bottom = jnp.where(row < 7, 1.0, 0.0).astype(F32)
    left = jnp.where(col > 0, 1.0, 0.0).astype(F32)
    right = jnp.where(col < 31, 1.0, 0.0).astype(F32)
    inside = zero
    for edge, value in enumerate((left, right, top * left, top * right, bottom * left, bottom * right)):
        inside = jnp.where((lane >= edge * 16) & (lane < edge * 16 + 16), value, inside)

    def spread(dst, m, tile, edges):
        edges = edges * inside
        for i in range(10):
            t = tile(i)
            if i == 0:
                t, first, at_row = t * top, 2, 7
            elif i == 9:
                t, first, at_row = t * bottom, 4, 0
            else:
                first, at_row = 0, i - 1
            where0 = first * 16 + m % 2 * 8 + at_row
            where2 = where0 + 16
            e0 = edges if where0 == 0 else pltpu.roll(edges, 128 - where0, axis=1)
            before = jnp.where(lane == 0, e0, pltpu.roll(t, 1, axis=1))
            after = jnp.where(
                lane == 127, pltpu.roll(edges, 127 - where2, axis=1), pltpu.roll(t, 127, axis=1)
            )
            span = slice(i * 128, i * 128 + 128)
            dst[m, 0:64, span] = before.astype(BF16)
            dst[m, 64:128, span] = t.astype(BF16)
            dst[m, 128:192, span] = after.astype(BF16)

    def flatten(src, dst, m):
        wide[m % 2] = src[m].astype(F32).reshape(2048, 128)
        for i in range(8):
            dst[m, :, i * 128 : i * 128 + 128] = wide[m % 2, pl.ds(i, 256, stride=8), :].astype(BF16)

    def moments(k, tile, members):
        columns_of_rows(tile, k, members)
        for m in members:
            mean = cols[k, m] / count
            var = cols[k + 1, m] / count - mean * mean
            cols[k, m] = mean
            cols[k + 1, m] = lax.rsqrt(var + EPSILON)

    for copy in load_w[:2]:
        copy.wait()
    rwt[...] = rw[...].astype(F32)
    for m in range(4):
        w1[m] = (rwt[...] * rf[m : m + 1]).astype(BF16)
    ones = jnp.ones((8, 1024), BF16)

    def free_rows(m):
        base = 2 if m < 2 else 0
        return (base + 4 * (m % 2), base + 4 * (m % 2) + 1)

    stats, halos = [None, None], [None, None]
    for n in range(2):
        acc = zero
        extra = []
        for m in group(n):
            load_x[m].wait()
            flatten(xraw, x, m)
            a = dot(w1[m], x[m], 1, 0)
            hb[0, m, :, 128:1152] = a
            acc = sums(m, acc, a, a * a)
            extra.append((m, dot(ones, x[m], 1, 1)))
        tile = rows_of_columns(acc)
        for m, line in extra:
            for h, r in enumerate(free_rows(m)):
                tile = jnp.where(sub == r, line[:, h * 128 : h * 128 + 128], tile)
        if n == 0:
            pl.semaphore_wait(barrier, 36)
        stats[n] = sum_start(0, n, tile)
        pack(0, n)
        halos[n] = halo(0, n)

    for copy in load_w[2:]:
        copy.wait()
    tail = jnp.zeros((8, 64), F32)
    columns_of_rows(
        jnp.concatenate([jnp.concatenate([sf[...], ef[...]], axis=0), tail], axis=1), 8, range(4)
    )
    columns_of_rows(
        jnp.concatenate(
            [jnp.concatenate([g1[...], b1[...], g2[...], b2[...], tail[:4]], axis=0), tail], axis=1
        ), 10, range(4),
    )
    for m in range(4):
        sfm, efm = cols[8, m], cols[9, m]
        w3[m] = (efm * ew[...].astype(F32) * of[m : m + 1]).astype(BF16)
        for p in range(3):
            taps = [(sfm * sw[3 * p + q].astype(F32)).astype(BF16) for q in range(3)]
            for q in range(3):
                w2[m, p, q * 64 : q * 64 + 64] = taps[q]
            w2b[m, 2 - p] = jnp.concatenate(taps[::-1], axis=1)
    gain1, shift1, gain2, shift2 = (cols[10, n] for n in range(4))
    for copy in load_c:
        copy.wait()
    for m in range(4):
        flatten(craw, c, m)
    stats[0] = sum_middle(0, 0, stats[0])
    stats[1] = sum_middle(0, 1, stats[1])

    for n in range(2):
        tile = sum_end(0, n, stats[n])
        moments(0, tile, group(n))
        for m in group(n):
            for h, r in enumerate(free_rows(m)):
                sxs[m, h] = jnp.broadcast_to(tile[r : r + 1], (8, 128))
        for copy in halos[n]:
            copy.wait()
        edges = received(0, n)
        acc = zero
        for m in group(n):
            mean, rstd = cols[0, m], cols[1, m]

            def hidden(v):
                return silu(gain1 * ((v - mean) * rstd) + shift1)

            spread(
                hq, m, lambda i: hidden(hb[0, m, :, i * 128 : i * 128 + 128]),
                hidden(edges),
            )
            a = dot(w2[m, 0], hq[m, :, 0:1024], 0, 0)
            a = a + dot(w2[m, 1], hq[m, :, 128:1152], 0, 0)
            a = a + dot(w2[m, 2], hq[m, :, 256:1280], 0, 0)
            hb[1, m, :, 128:1152] = a
            acc = sums(m, acc, a, a * a)
        stats[n] = sum_start(1, n, rows_of_columns(acc))
        pack(1, n)
        halos[n] = halo(1, n)

    def project(m):
        normed = (hb[0, m, :, 128:1152] - cols[0, m]) * cols[1, m]
        slope1[m] = slope(gain1 * normed + shift1)
        part = dot(normed.astype(BF16), x[m], 1, 1)
        for a in range(16):
            h, f = a // 8, a % 8
            bn[m // 2, a, m % 2 * 8 : m % 2 * 8 + 8] = part[f * 8 : f * 8 + 8, h * 128 : h * 128 + 128]

    for m in range(4):
        project(m)
    corrections = share_cores(0, bn, bn0)
    stats[0] = sum_middle(1, 0, stats[0])
    stats[1] = sum_middle(1, 1, stats[1])
    corrections = share_plane(16, corrections, bn, bn0, bn1)

    sums2 = []
    for n in range(2):
        moments(2, sum_end(1, n, stats[n]), group(n))
        for copy in halos[n]:
            copy.wait()
        acc = zero
        for m in group(n):
            mean, rstd = cols[2, m], cols[3, m]
            for o in range(0, 1024, 256):
                span = slice(o, o + 256)
                pre = gain2 * ((hb[1, m, :, o + 128 : o + 384] - mean) * rstd) + shift2
                s = sigmoid(pre)
                h2[m, :, span] = (pre * s).astype(BF16)
                dpre1[m, :, span] = s * (1.0 + pre * (1.0 - s))
                third = dot(w3[m], h2[m, :, span], 0, 0)
                up = c[m, :, span].astype(F32) * slope(x[m, :, span].astype(F32) + third)
                u[m, :, span] = up
                ulow[m, :, span] = up.astype(BF16)
            back = dot(w3[m], ulow[m], 1, 0)
            hb[2, m, :, 128:1152] = back
            dpre = back * dpre1[m]
            acc = sums(m, acc, dpre, dpre * ((hb[1, m, :, 128:1152] - mean) * rstd))
        stats[n] = sum_start(2, n, rows_of_columns(acc))
        pack(2, n)
        halos[n] = halo(2, n)

    fac = zero

    def expand(m, fac):
        part = dot(h2[m], ulow[m], 1, 1)
        ofm, efm = of[m : m + 1], cols[9, m]
        scaled = part * efm * ofm
        acce[...] = scaled if m == 0 else acce[...] + scaled
        byw = part * ew[...].astype(F32)
        nf[1, m] = jnp.sum(byw * efm, axis=0, keepdims=True)
        return put(fac, m, jnp.sum(byw * ofm, axis=1, keepdims=True))

    for m in range(4):
        fac = expand(m, fac)

    def place(buf, t, value):
        r = t // 32 * 8
        buf[t // 16 % 2, t % 16, r : r + 8] = value

    def lines(k):
        return jnp.concatenate(
            [nf[k, m, :, h * 128 : h * 128 + 128] for h in range(2) for m in range(4)], axis=0
        )

    for a in range(16):
        h, f = a // 8, a % 8
        place(e, a, acce[f * 8 : f * 8 + 8, h * 128 : h * 128 + 128])
    place(e, OUTPUT_F, lines(1))
    place(e, EXPAND_F, rows_of_columns(fac))
    for t in range(EXPAND_F + 1, EARLY_TILES):
        place(e, t, jnp.zeros((8, 128), F32))
    early = share_cores(1, e, e0)

    def prepare(n):
        for copy in halos[n]:
            copy.wait()
        second_edges, back_edges = received(1, n), received(2, n)
        for m in group(n):
            mean, rstd = cols[2, m], cols[3, m]
            scale = gain2 * rstd

            def halves(second, back):
                normed = (second - mean) * rstd
                return scale * normed, scale * (back * slope(gain2 * normed + shift2))

            for i in range(10):
                span = slice(i * 128, i * 128 + 128)
                hb[1, m, :, span], hb[2, m, :, span] = halves(hb[1, m, :, span], hb[2, m, :, span])
            ep[0, m], ep[1, m] = halves(second_edges, back_edges)

    stats[0] = sum_middle(2, 0, stats[0])
    prepare(0)
    stats[1] = sum_middle(2, 1, stats[1])
    prepare(1)
    early = share_plane(18, early, e, e0, e1)
    corrections = share_depth(17, corrections, bn0, bn1, bn2)

    for n in range(2):
        tile = sum_end(2, n, stats[n])
        sums2.append(tile)
        columns_of_rows(tile, 4, group(n))
        acc = zero
        for m in group(n):
            plain, weighted = gain2 * cols[3, m] * cols[4, m] / count, cols[5, m] / count

            def dact(normed, part):
                return part - plain - normed * weighted

            spread(
                dq, m,
                lambda i: dact(hb[1, m, :, i * 128 : i * 128 + 128], hb[2, m, :, i * 128 : i * 128 + 128]),
                dact(ep[0, m], ep[1, m]),
            )
            a = dot(w2b[m, 0], dq[m, :, 0:1024], 1, 0)
            a = a + dot(w2b[m, 1], dq[m, :, 128:1152], 1, 0)
            a = a + dot(w2b[m, 2], dq[m, :, 256:1280], 1, 0)
            normed = (hb[0, m, :, 128:1152] - cols[0, m]) * cols[1, m]
            dpre = a * slope1[m]
            dpre1[m] = dpre
            acc = sums(m, acc, dpre, dpre * normed)
        stats[n] = sum_start(3, n, rows_of_columns(acc))

    def gradients(m, fac):
        sfm = cols[8, m]
        byf = jnp.zeros((64, 1), F32)
        for p in range(3):
            part = dot(hq[m, :, p * 128 : p * 128 + 1024], dq[m, 64:128, 128:1152], 1, 1)
            for q in range(3):
                k = 3 * p + q
                tap = part[q * 64 : q * 64 + 64]
                byf = byf + jnp.sum(tap * sw[k].astype(F32), axis=1, keepdims=True)
                tap = tap * sfm
                accs[k] = tap if m == 0 else accs[k] + tap
        part = dot(dpre1[m].astype(BF16), x[m], 1, 1) * (gain1 * cols[1, m])
        scaled = part * rf[m : m + 1]
        accr[...] = scaled if m == 0 else accr[...] + scaled
        nf[0, m] = jnp.sum(part * rwt[...], axis=0, keepdims=True)
        return put(fac, m, byf)

    fac = zero
    for m in range(4):
        fac = gradients(m, fac)
    for a in range(16):
        h, f = a // 8, a % 8
        place(g, a, accr[f * 8 : f * 8 + 8, h * 128 : h * 128 + 128])
    for t in range(36):
        low, high = t * 8, 288 + t * 8
        place(g, SPATIAL + t, jnp.concatenate(
            [accs[low // 64, low % 64 : low % 64 + 8], accs[high // 64, high % 64 : high % 64 + 8]], axis=1
        ))
    place(g, REDUCE_F, lines(0))
    place(g, SPATIAL_F, rows_of_columns(fac))
    for t in range(SPATIAL_F + 1, LATE_TILES):
        place(g, t, jnp.zeros((8, 128), F32))
    late = share_cores(2, g, g0)
    early = share_depth(19, early, e0, e1, e2)
    late = share_plane(21, late, g, g0, g1_)
    stats[0] = sum_middle(3, 0, stats[0])
    stats[1] = sum_middle(3, 1, stats[1])
    corrections()
    bnc[...] = total(bn2, 8)
    early()
    e3[core, rank_a] = total(e2, 8)
    early = gather_plane(20, e3)

    def finish(m):
        mean, rstd, plain, weighted = cols[0, m], cols[1, m], cols[6, m] / count, cols[7, m] / count
        normed = (hb[0, m, :, 128:1152] - mean) * rstd
        dq[m, 0:64, 0:1024] = (gain1 * rstd * (dpre1[m] - plain - normed * weighted)).astype(BF16)
        for j in range(4):
            o = j * 256
            t = u[m, :, o : o + 256] + dot(w1[m], dq[m, 0:64, o : o + 256], 0, 0)
            wide[m % 2, pl.ds(2 * j, 256, stride=8), :] = t[:, :128]
            wide[m % 2, pl.ds(2 * j + 1, 256, stride=8), :] = t[:, 128:]
        craw[m] = wide[m % 2].reshape(256, 8, 128).astype(BF16)
        store = pltpu.make_async_copy(craw.at[m], y_hbm.at[m], st_sem.at[m])
        store.start()
        return store

    tile = sum_end(3, 0, stats[0])
    sums1 = [tile]
    columns_of_rows(tile, 6, group(0))
    late = share_depth(22, late, g0, g1_, g2_)
    stores = [finish(0), finish(1)]
    tile = sum_end(3, 1, stats[1])
    sums1.append(tile)
    columns_of_rows(tile, 6, group(1))

    half, block = lax.div(rank_a, 8), pl.ds(pl.multiple_of(lax.rem(rank_a, 8) * 8, 8), 8)
    span = pl.ds(pl.multiple_of(half * 128, 128), 128)
    fix = jnp.zeros((8, 128), F32)
    part = jnp.zeros((8, 128), F32)
    for k in range(2):
        m = 2 * core + k
        plain, weighted = cols[6, m, block] / count, cols[7, m, block] / count
        v = cols[10, 0, block] * cols[1, m, block] * (
            plain * sxs[m, half] + weighted * bnc[k * 8 : k * 8 + 8]
        )
        fix = fix + v * jnp.where(core == 0, rf[k : k + 1, span], rf[k + 2 : k + 3, span])
        part = jnp.where(
            sub == half * 4 + m, jnp.sum(v * rwt[block, span], axis=0, keepdims=True), part
        )
    both[core, 0:8] = fix
    both[core, 8:16] = part
    swap(5, both.at[core], both.at[core])()
    fix = jnp.where(core == 0, both[0, 0:8] + both[1, 0:8], 0.0)
    late()
    share = total(g2_, 8)
    g3[core, rank_a, 0:8] = share[0:8] - fix
    g3[core, rank_a, 8:LATE] = share[8:LATE]
    g3[core, rank_a, LATE:WHOLE] = both[0, 8:16] + both[1, 8:16]
    late = gather_plane(23, g3)
    early = gather_cores(3, early, e3)
    stores += [finish(2), finish(3)]
    first, second = sums1[0] + sums1[1], sums2[0] + sums2[1]
    norms[...] = jnp.concatenate(
        [
            jnp.sum(first[4:8], axis=0, keepdims=True),
            jnp.sum(first[0:4], axis=0, keepdims=True),
            jnp.sum(second[4:8], axis=0, keepdims=True),
            jnp.sum(second[0:4], axis=0, keepdims=True),
            jnp.zeros((4, 128), F32),
        ],
        axis=0,
    )
    late = gather_cores(4, late, g3)
    early()
    early_out[...] = e3[...]
    late()
    late_out[...] = g3[...]
    for copy in stores:
        copy.wait()


def unpack(
    y_hbm, whole, expand, norms,
    out_hbm, o_reduce, o_spatial, o_expand, o_rf, o_sf, o_ef, o_of, o_g1, o_b1, o_g2, o_b2,
    sem,
):
    store = [pltpu.make_async_copy(y_hbm.at[m], out_hbm.at[m], sem.at[m]) for m in range(4)]
    for copy in store:
        copy.start()

    def early(t):
        return expand[t // 16, t % 16]

    def late(t):
        return whole[t // 16 % 2, t % 16, t // 32 * 8 : t // 32 * 8 + 8]

    fix = jnp.zeros((8, 128), F32)
    for a in range(16):
        h, f = a // 8, a % 8
        o_expand[f * 8 : f * 8 + 8, h * 128 : h * 128 + 128] = early(a)
        o_reduce[f * 8 : f * 8 + 8, h * 128 : h * 128 + 128] = late(a)
        fix = fix + whole[0, a, LATE:WHOLE]
    for t in range(36):
        both = late(SPATIAL + t)
        for n in range(2):
            r = n * 288 + t * 8
            o_spatial[r // 64, r % 64 : r % 64 + 8] = both[:, n * 64 : n * 64 + 64]
    for o, e in ((o_rf, late(REDUCE_F) - fix), (o_of, early(OUTPUT_F))):
        o[:, :128] = e[:4]
        o[:, 128:] = e[4:]
    o_ef[...] = early(EXPAND_F)[:4, :64]
    o_sf[...] = late(SPATIAL_F)[:4, :64]
    for n, o in enumerate((o_g1, o_b1, o_g2, o_b2)):
        o[...] = norms[n : n + 1, :64]
    for copy in store:
        copy.wait()


def body(
    features, cotangent, reduce_weight, spatial_weight, expand_weight,
    reduce_factor, spatial_factor, expand_factor, output_factor,
    gain_first, shift_first, gain_second, shift_second,
):
    vmem = pl.BlockSpec(memory_space=pltpu.VMEM)
    hbm = pl.BlockSpec(memory_space=pl.ANY)
    sds = jax.ShapeDtypeStruct
    bufs = pl.pallas_call(
        kernel,
        out_shape=(
            sds((4, 256, 8, 128), BF16), sds((2, 16, WHOLE, 128), F32), sds((2, 16, EARLY, 128), F32),
            sds((8, 128), F32),
        ),
        in_specs=[pl.BlockSpec(memory_space=pltpu.HBM)] * 13,
        out_specs=(hbm, vmem, vmem, vmem),
        scratch_shapes=[
            pltpu.VMEM((4, 256, 8, 128), BF16),
            pltpu.VMEM((4, 256, 8, 128), BF16),
            pltpu.VMEM((2, 2048, 128), F32),
            pltpu.VMEM((64, 256), BF16),
            pltpu.VMEM((9, 64, 64), BF16),
            pltpu.VMEM((64, 256), BF16),
            pltpu.VMEM((4, 256), F32),
            pltpu.VMEM((4, 64), F32),
            pltpu.VMEM((4, 64), F32),
            pltpu.VMEM((4, 256), F32),
            pltpu.VMEM((1, 64), F32),
            pltpu.VMEM((1, 64), F32),
            pltpu.VMEM((1, 64), F32),
            pltpu.VMEM((1, 64), F32),
            pltpu.VMEM((4, 64, 256), BF16),
            pltpu.VMEM((4, 3, 192, 64), BF16),
            pltpu.VMEM((4, 3, 64, 192), BF16),
            pltpu.VMEM((4, 64, 256), BF16),
            pltpu.VMEM((64, 256), F32),
            pltpu.VMEM((4, 256, 1024), BF16),
            pltpu.VMEM((4, 256, 1024), BF16),
            pltpu.VMEM((4, 256, 1024), F32),
            pltpu.VMEM((4, 256, 1024), BF16),
            pltpu.VMEM((4, 64, 1024), BF16),
            pltpu.VMEM((3, 4, 64, 1280), F32),
            pltpu.VMEM((4, 192, 1280), BF16),
            pltpu.VMEM((4, 192, 1280), BF16),
            pltpu.VMEM((4, 64, 1024), F32),
            pltpu.VMEM((2, 4, 1, 256), F32),
            pltpu.VMEM((3, 2, 2, 16, 128), F32),
            pltpu.VMEM((3, 2, 6, 16, 128), F32),
            pltpu.VMEM((8, 16, 8, 128), F32),
            pltpu.VMEM((8, 16, 8, 128), F32),
            pltpu.VMEM((64, 256), F32),
            pltpu.VMEM((64, 256), F32),
            pltpu.VMEM((9, 64, 64), F32),
            pltpu.VMEM((4, 2, 8, 128), F32),
            pltpu.VMEM((2, 16, 16, 128), F32),
            pltpu.VMEM((16, 16, 128), F32),
            pltpu.VMEM((16, 16, 128), F32),
            pltpu.VMEM((8, 16, 128), F32),
            pltpu.VMEM((16, 128), F32),
            pltpu.VMEM((2, 16, EARLY, 128), F32),
            pltpu.VMEM((16, EARLY, 128), F32),
            pltpu.VMEM((16, EARLY, 128), F32),
            pltpu.VMEM((8, EARLY, 128), F32),
            pltpu.VMEM((2, 16, EARLY, 128), F32),
            pltpu.VMEM((2, 16, LATE, 128), F32),
            pltpu.VMEM((16, LATE, 128), F32),
            pltpu.VMEM((16, LATE, 128), F32),
            pltpu.VMEM((8, LATE, 128), F32),
            pltpu.VMEM((2, 16, WHOLE, 128), F32),
            pltpu.VMEM((2, 16, 128), F32),
            pltpu.VMEM((4, 64, 1024), F32),
            pltpu.VMEM((2, 4, 64, 128), F32),
            pltpu.VMEM((12, 4, 64, 1), F32),
            pltpu.SemaphoreType.DMA((20,)),
            pltpu.SemaphoreType.DMA((4,)),
            pltpu.SemaphoreType.DMA((24,)),
            pltpu.SemaphoreType.DMA((24,)),
            pltpu.SemaphoreType.DMA((6, 2)),
            pltpu.SemaphoreType.DMA((6, 2)),
            pltpu.SemaphoreType.DMA((6,)),
            pltpu.SemaphoreType.DMA((6,)),
        ],
        compiler_params=pltpu.CompilerParams(
            collective_id=0, has_side_effects=True, vmem_limit_bytes=44 * 1024 * 1024
        ),
        name="step",
    )(*[pltpu.with_memory_space_constraint(v, pltpu.HBM) for v in (
        features, cotangent, reduce_weight.T, spatial_weight, expand_weight,
        reduce_factor, spatial_factor, expand_factor, output_factor,
        gain_first.reshape(1, 64), shift_first.reshape(1, 64),
        gain_second.reshape(1, 64), shift_second.reshape(1, 64),
    )])
    outs = pl.pallas_call(
        unpack,
        out_shape=(
            sds((4, 256, 8, 128), BF16), sds((64, 256), F32), sds((9, 64, 64), F32), sds((64, 256), F32),
            sds((4, 256), F32), sds((4, 64), F32), sds((4, 64), F32), sds((4, 256), F32),
        ) + (sds((1, 64), F32),) * 4,
        in_specs=[hbm, vmem, vmem, vmem],
        out_specs=(hbm,) + (vmem,) * 11,
        scratch_shapes=[
            pltpu.SemaphoreType.DMA((4,)),
        ],
        compiler_params=pltpu.CompilerParams(vmem_limit_bytes=8 * 1024 * 1024),
        name="unpack",
    )(*bufs)
    return (outs[0], outs[1].T) + outs[2:8] + tuple(o.reshape(64) for o in outs[8:])


def solution(mesh):
    split = Mesh(
        mesh.devices.reshape(2, 4, 8, 2, 2), ("rows_0", "rows_1", "cols_0", "cols_1", "cols_2")
    )
    image = P(None, None, ROWS, COLS)
    return jax.shard_map(
        body,
        mesh=split,
        in_specs=(image, image) + (P(),) * 11,
        out_specs=(image,) + (P(),) * 11,
        check_vma=False,
    )
```

```python
import functools

import jax
import jax.numpy as jnp
from jax import lax
from jax.experimental import pallas as pl
from jax.experimental.pallas import tpu as pltpu
from jax.sharding import Mesh
from jax.sharding import PartitionSpec as P

ROWS = ("rows_0", "rows_1")
COLS = ("cols_0", "cols_1", "cols_2")
MESH = pl.DeviceIdType.MESH
EPSILON = 1e-05
F32 = jnp.float32
BF16 = jnp.bfloat16

EARLY, LATE, WHOLE = 8, 16, 24
OUTPUT_F, EXPAND_F, EARLY_TILES = 16, 17, 32
SPATIAL, REDUCE_F, SPATIAL_F, LATE_TILES = 16, 52, 53, 64


def dot(a, b, ca, cb):
    return lax.dot_general(a, b, (((ca,), (cb,)), ((), ())), preferred_element_type=F32)


def sigmoid(v):
    return 0.5 + 0.5 * jnp.tanh(0.5 * v)


def silu(v):
    return v * sigmoid(v)


def slope(v):
    s = sigmoid(v)
    return s * (1.0 + v * (1.0 - s))


def total(buf, n=16):
    t = buf[0]
    for k in range(1, n):
        t = t + buf[k]
    return t


class Rows:
    def __init__(self, row, up, down):
        self.row, self.up, self.down = row, up, down

    def wait(self):
        @pl.when(self.row > 0)
        def _():
            self.up.wait_send()
            self.down.wait_recv()

        @pl.when(self.row < 7)
        def _():
            self.down.wait_send()
            self.up.wait_recv()


def kernel(
    x_hbm, c_hbm, rw_hbm, sw_hbm, ew_hbm, rf_hbm, sf_hbm, ef_hbm, of_hbm, g1_hbm, b1_hbm, g2_hbm, b2_hbm,
    y_hbm, late_out, early_out, norms,
    xraw, craw, wide, rw, sw, ew, rf, sf, ef, of, g1, b1, g2, b2,
    w1, w2, w2b, w3, rwt,
    x, c, u, ulow, h2, hb, hq, dq, dpre1, nf, pk, pr, arb, ara,
    acce, accr, accs, sxs, bn, bn0, bn1, bn2, bnc, e, e0, e1, e2, e3, g, g0, g1_, g2_, g3, both, slope1, ep, cols,
    ld_sem, st_sem, s_sem, r_sem, hs_sem, hr_sem, cs_sem, cr_sem,
):
    count = float(64 * 4096)
    x_hi, y = lax.axis_index("rows_0"), lax.axis_index("rows_1")
    z, x_lo, core = lax.axis_index("cols_0"), lax.axis_index("cols_1"), lax.axis_index("cols_2")
    row = x_hi * 4 + y
    col = z * 4 + x_lo * 2 + core
    rank_a = x_hi * 8 + x_lo * 4 + y
    rank_b = z * 2 + core

    def peer_a(d):
        a = lax.rem(rank_a + d, 16)
        return (lax.div(a, 8), lax.rem(a, 4), z, lax.rem(lax.div(a, 4), 2), core)

    def peer_b(d):
        b = lax.rem(rank_b + d, 16)
        return (x_hi, y, lax.div(b, 2), x_lo, lax.rem(b, 2))

    def peer_z(d):
        return (x_hi, y, lax.rem(z + d, 8), x_lo, core)

    def at(dr, dc):
        rr, cc = lax.rem(row + dr + 8, 8), lax.rem(col + dc + 32, 32)
        return (lax.div(rr, 4), lax.rem(rr, 4), lax.div(cc, 4), lax.rem(lax.div(cc, 2), 2), lax.rem(cc, 2))

    sides = ((0, 1), (0, -1), (1, 1), (1, -1), (-1, 1), (-1, -1))

    pairs = (
        (rw_hbm, rw), (rf_hbm, rf), (sw_hbm, sw), (ew_hbm, ew), (sf_hbm, sf), (ef_hbm, ef), (of_hbm, of),
        (g1_hbm, g1), (b1_hbm, b1), (g2_hbm, g2), (b2_hbm, b2),
    )
    load_w = [pltpu.make_async_copy(a, b, ld_sem.at[8 + n]) for n, (a, b) in enumerate(pairs)]
    load_x = [pltpu.make_async_copy(x_hbm.at[m], xraw.at[m], ld_sem.at[m]) for m in range(4)]
    load_c = [pltpu.make_async_copy(c_hbm.at[m], craw.at[m], ld_sem.at[4 + m]) for m in range(4)]
    for copy in load_w[:2] + load_x:
        copy.start()

    barrier = pltpu.get_barrier_semaphore()

    def greet(d, _):
        pl.semaphore_signal(barrier, inc=1, device_id=peer_a(d), device_id_type=MESH)
        pl.semaphore_signal(barrier, inc=1, device_id=peer_b(d), device_id_type=MESH)
        return 0

    lax.fori_loop(1, 16, greet, 0)
    for side in sides:
        pl.semaphore_signal(barrier, inc=1, device_id=at(*side), device_id_type=MESH)
    for copy in load_w[2:] + load_c:
        copy.start()

    def exchange(stage, src, buf, rank, peer, n=16):
        def start(d, _):
            pltpu.make_async_remote_copy(
                src_ref=src(d), dst_ref=buf.at[rank], send_sem=s_sem.at[stage],
                recv_sem=r_sem.at[stage], device_id=peer(d), device_id_type=MESH,
            ).start()
            return 0

        lax.fori_loop(1, n, start, 0)
        return together(buf.at[pl.ds(0, n - 1)], s_sem.at[stage], r_sem.at[stage]).wait

    def together(ref, send, recv):
        return pltpu.make_async_remote_copy(
            src_ref=ref, dst_ref=ref, send_sem=send, recv_sem=recv,
            device_id=(x_hi, y, z, x_lo, 1 - core), device_id_type=MESH,
        )

    def swap(stage, src, dst):
        copy = pltpu.make_async_remote_copy(
            src_ref=src, dst_ref=dst, send_sem=cs_sem.at[stage], recv_sem=cr_sem.at[stage],
            device_id=(x_hi, y, z, x_lo, 1 - core), device_id_type=MESH,
        )
        copy.start()
        return copy.wait

    def share_cores(stage, tiles, partner):
        return swap(stage, tiles.at[1 - core], partner)

    def share_plane(stage, wait, tiles, partner, buf):
        wait()
        for a in range(16):
            partner[a] = partner[a] + tiles[core, a]
        return exchange(stage, lambda d: partner.at[lax.rem(rank_a + d, 16)], buf, rank_a, peer_a)

    def share_depth(stage, wait, partner, buf, slots):
        wait()
        buf[rank_a] = partner[rank_a]
        slots[z] = total(buf)
        return exchange(stage, lambda d: slots.at[z], slots, z, peer_z, 8)

    def gather_plane(stage, whole):
        return exchange(stage, lambda d: whole.at[core, rank_a], whole.at[core], rank_a, peer_a)

    def gather_cores(stage, wait, whole):
        wait()
        return swap(stage, whole.at[core], whole.at[core])

    def sum_start(k, n, tile):
        arb[2 * k + n, rank_b] = tile
        return exchange(
            4 * k + 2 * n, lambda d: arb.at[2 * k + n, rank_b], arb.at[2 * k + n], rank_b, peer_b
        )

    def sum_middle(k, n, wait):
        wait()
        ara[2 * k + n, rank_a] = total(arb.at[2 * k + n])
        return exchange(
            4 * k + 2 * n + 1, lambda d: ara.at[2 * k + n, rank_a], ara.at[2 * k + n], rank_a, peer_a
        )

    def sum_end(k, n, wait):
        wait()
        return total(ara.at[2 * k + n])

    def halo(k, n):
        members = pl.ds(2 * n, 2)
        t = 2 * k + n
        copies = [
            pltpu.make_async_remote_copy(
                src_ref=hb.at[k, members, :, pl.ds(128, 128)],
                dst_ref=hb.at[k, members, :, pl.ds(1152, 128)],
                send_sem=hs_sem.at[t, 0], recv_sem=hr_sem.at[t, 0],
                device_id=at(-1, 0), device_id_type=MESH,
            ),
            pltpu.make_async_remote_copy(
                src_ref=hb.at[k, members, :, pl.ds(1024, 128)],
                dst_ref=hb.at[k, members, :, pl.ds(0, 128)],
                send_sem=hs_sem.at[t, 2], recv_sem=hr_sem.at[t, 2],
                device_id=at(1, 0), device_id_type=MESH,
            ),
        ]
        for edge, side in enumerate(sides):
            copies.append(
                pltpu.make_async_remote_copy(
                    src_ref=pk.at[k, n, (side[1] + 1) // 2], dst_ref=pr.at[k, n, edge], send_sem=hs_sem.at[t, 1],
                    recv_sem=hr_sem.at[t, 1], device_id=at(*side), device_id_type=MESH,
                )
            )
        up, down = copies[:2]
        pl.when(row > 0)(up.start)
        pl.when(row < 7)(down.start)
        for copy in copies[2:]:
            copy.start()
        return [Rows(row, up, down), together(pr.at[k, n], hs_sem.at[t, 1], hr_sem.at[t, 1])]

    lane = lax.broadcasted_iota(jnp.int32, (64, 128), 1)
    sub = lax.broadcasted_iota(jnp.int32, (8, 128), 0)
    zero = jnp.zeros((64, 128), F32)

    def put(acc, n, value):
        return jnp.where(lane == n, value, acc)

    def rows_of_columns(acc):
        return jnp.transpose(jnp.concatenate([acc, jnp.zeros((64, 128), F32)], axis=0))[:8]

    def columns_of_rows(tile, k, members):
        t = jnp.transpose(jnp.concatenate([tile, jnp.zeros((120, 128), F32)], axis=0))
        for m in members:
            cols[k, m] = t[:64, m : m + 1]
            cols[k + 1, m] = t[:64, 4 + m : 5 + m]

    def sums(m, acc, a, b):
        acc = put(acc, m, jnp.sum(a, axis=1, keepdims=True))
        return put(acc, 4 + m, jnp.sum(b, axis=1, keepdims=True))

    def pack(k, n):
        acc = zero
        for m in group(n):
            for i in range(8):
                t = hb[k, m, :, 128 + i * 128 : 256 + i * 128]
                acc = put(acc, m % 2 * 8 + i, t[:, 0:1])
                acc = put(acc, 16 + m % 2 * 8 + i, t[:, 127:128])
        t = jnp.transpose(jnp.concatenate([acc, zero], axis=0))
        pk[k, n, 0] = t[0:16]
        pk[k, n, 1] = t[16:32]

    def received(k, n):
        t = jnp.concatenate([pr[k, n, e] for e in range(6)] + [jnp.zeros((32, 128), F32)], axis=0)
        return jnp.transpose(t)[:64]

    def group(n):
        return (2 * n, 2 * n + 1)

    top = jnp.where(row > 0, 1.0, 0.0).astype(F32)
    bottom = jnp.where(row < 7, 1.0, 0.0).astype(F32)
    left = jnp.where(col > 0, 1.0, 0.0).astype(F32)
    right = jnp.where(col < 31, 1.0, 0.0).astype(F32)
    place_row = jnp.full((64, 128), row, jnp.int32)
    inside = zero
    for edge, value in enumerate((left, right, top * left, top * right, bottom * left, bottom * right)):
        inside = jnp.where((lane >= edge * 16) & (lane < edge * 16 + 16), value, inside)

    def spread(dst, m, tile, edges):
        edges = edges * inside
        for i in range(10):
            t = tile(i)
            if i == 0:
                t, first, at_row = jnp.where(place_row > 0, t, 0.0), 2, 7
            elif i == 9:
                t, first, at_row = jnp.where(place_row < 7, t, 0.0), 4, 0
            else:
                first, at_row = 0, i - 1
            where0 = first * 16 + m % 2 * 8 + at_row
            where2 = where0 + 16
            e0 = edges if where0 == 0 else pltpu.roll(edges, 128 - where0, axis=1)
            before = jnp.where(lane == 0, e0, pltpu.roll(t, 1, axis=1))
            after = jnp.where(
                lane == 127, pltpu.roll(edges, 127 - where2, axis=1), pltpu.roll(t, 127, axis=1)
            )
            span = slice(i * 128, i * 128 + 128)
            dst[m, 0:64, span] = before.astype(BF16)
            dst[m, 64:128, span] = t.astype(BF16)
            dst[m, 128:192, span] = after.astype(BF16)

    def flatten(src, dst, m):
        wide[m % 2] = src[m].astype(F32).reshape(2048, 128)
        for i in range(8):
            dst[m, :, i * 128 : i * 128 + 128] = wide[m % 2, pl.ds(i, 256, stride=8), :].astype(BF16)

    def moments(k, tile, members):
        columns_of_rows(tile, k, members)
        for m in members:
            mean = cols[k, m] / count
            var = cols[k + 1, m] / count - mean * mean
            cols[k, m] = mean
            cols[k + 1, m] = lax.rsqrt(var + EPSILON)

    for copy in load_w[:2]:
        copy.wait()
    rwt[...] = rw[...].astype(F32)
    for m in range(4):
        w1[m] = (rwt[...] * rf[m : m + 1]).astype(BF16)
    ones = jnp.ones((8, 1024), BF16)

    def free_rows(m):
        base = 2 if m < 2 else 0
        return (base + 4 * (m % 2), base + 4 * (m % 2) + 1)

    stats, halos = [None, None], [None, None]
    for n in range(2):
        acc = zero
        extra = []
        for m in group(n):
            load_x[m].wait()
            flatten(xraw, x, m)
            a = dot(w1[m], x[m], 1, 0)
            hb[0, m, :, 128:1152] = a
            acc = sums(m, acc, a, a * a)
            extra.append((m, dot(ones, x[m], 1, 1)))
        tile = rows_of_columns(acc)
        for m, line in extra:
            for h, r in enumerate(free_rows(m)):
                tile = jnp.where(sub == r, line[:, h * 128 : h * 128 + 128], tile)
        if n == 0:
            pl.semaphore_wait(barrier, 36)
        stats[n] = sum_start(0, n, tile)
        pack(0, n)
        halos[n] = halo(0, n)

    for copy in load_w[2:]:
        copy.wait()
    tail = jnp.zeros((8, 64), F32)
    columns_of_rows(
        jnp.concatenate([jnp.concatenate([sf[...], ef[...]], axis=0), tail], axis=1), 8, range(4)
    )
    columns_of_rows(
        jnp.concatenate(
            [jnp.concatenate([g1[...], b1[...], g2[...], b2[...], tail[:4]], axis=0), tail], axis=1
        ), 10, range(4),
    )
    for m in range(4):
        sfm, efm = cols[8, m], cols[9, m]
        w3[m] = (efm * ew[...].astype(F32) * of[m : m + 1]).astype(BF16)
        for p in range(3):
            taps = [(sfm * sw[3 * p + q].astype(F32)).astype(BF16) for q in range(3)]
            for q in range(3):
                w2[m, p, q * 64 : q * 64 + 64] = taps[q]
            w2b[m, 2 - p] = jnp.concatenate(taps[::-1], axis=1)
    gain1, shift1, gain2, shift2 = (cols[10, n] for n in range(4))
    for copy in load_c:
        copy.wait()
    for m in range(4):
        flatten(craw, c, m)
    stats[0] = sum_middle(0, 0, stats[0])
    stats[1] = sum_middle(0, 1, stats[1])

    for n in range(2):
        tile = sum_end(0, n, stats[n])
        moments(0, tile, group(n))
        for m in group(n):
            for h, r in enumerate(free_rows(m)):
                sxs[m, h] = jnp.broadcast_to(tile[r : r + 1], (8, 128))
        for copy in halos[n]:
            copy.wait()
        edges = received(0, n)
        acc = zero
        for m in group(n):
            mean, rstd = cols[0, m], cols[1, m]

            def hidden(v):
                return silu(gain1 * ((v - mean) * rstd) + shift1)

            spread(
                hq, m, lambda i: hidden(hb[0, m, :, i * 128 : i * 128 + 128]),
                hidden(edges),
            )
            a = dot(w2[m, 0], hq[m, :, 0:1024], 0, 0)
            a = a + dot(w2[m, 1], hq[m, :, 128:1152], 0, 0)
            a = a + dot(w2[m, 2], hq[m, :, 256:1280], 0, 0)
            hb[1, m, :, 128:1152] = a
            acc = sums(m, acc, a, a * a)
        stats[n] = sum_start(1, n, rows_of_columns(acc))
        pack(1, n)
        halos[n] = halo(1, n)

    def project(m):
        normed = (hb[0, m, :, 128:1152] - cols[0, m]) * cols[1, m]
        slope1[m] = slope(gain1 * normed + shift1)
        part = dot(normed.astype(BF16), x[m], 1, 1)
        for a in range(16):
            h, f = a // 8, a % 8
            bn[m // 2, a, m % 2 * 8 : m % 2 * 8 + 8] = part[f * 8 : f * 8 + 8, h * 128 : h * 128 + 128]

    for m in range(4):
        project(m)
    corrections = share_cores(0, bn, bn0)
    stats[0] = sum_middle(1, 0, stats[0])
    stats[1] = sum_middle(1, 1, stats[1])
    corrections = share_plane(16, corrections, bn, bn0, bn1)

    sums2 = []
    for n in range(2):
        moments(2, sum_end(1, n, stats[n]), group(n))
        for copy in halos[n]:
            copy.wait()
        acc = zero
        for m in group(n):
            mean, rstd = cols[2, m], cols[3, m]
            for o in range(0, 1024, 256):
                span = slice(o, o + 256)
                pre = gain2 * ((hb[1, m, :, o + 128 : o + 384] - mean) * rstd) + shift2
                s = sigmoid(pre)
                h2[m, :, span] = (pre * s).astype(BF16)
                dpre1[m, :, span] = s * (1.0 + pre * (1.0 - s))
                third = dot(w3[m], h2[m, :, span], 0, 0)
                up = c[m, :, span].astype(F32) * slope(x[m, :, span].astype(F32) + third)
                u[m, :, span] = up
                ulow[m, :, span] = up.astype(BF16)
            back = dot(w3[m], ulow[m], 1, 0)
            hb[2, m, :, 128:1152] = back
            dpre = back * dpre1[m]
            acc = sums(m, acc, dpre, dpre * ((hb[1, m, :, 128:1152] - mean) * rstd))
        stats[n] = sum_start(2, n, rows_of_columns(acc))
        pack(2, n)
        halos[n] = halo(2, n)

    fac = zero

    def expand(m, fac):
        part = dot(h2[m], ulow[m], 1, 1)
        ofm, efm = of[m : m + 1], cols[9, m]
        scaled = part * efm * ofm
        acce[...] = scaled if m == 0 else acce[...] + scaled
        byw = part * ew[...].astype(F32)
        nf[1, m] = jnp.sum(byw * efm, axis=0, keepdims=True)
        return put(fac, m, jnp.sum(byw * ofm, axis=1, keepdims=True))

    for m in range(4):
        fac = expand(m, fac)

    def place(buf, t, value):
        r = t // 32 * 8
        buf[t // 16 % 2, t % 16, r : r + 8] = value

    def lines(k):
        return jnp.concatenate(
            [nf[k, m, :, h * 128 : h * 128 + 128] for h in range(2) for m in range(4)], axis=0
        )

    for a in range(16):
        h, f = a // 8, a % 8
        place(e, a, acce[f * 8 : f * 8 + 8, h * 128 : h * 128 + 128])
    place(e, OUTPUT_F, lines(1))
    place(e, EXPAND_F, rows_of_columns(fac))
    for t in range(EXPAND_F + 1, EARLY_TILES):
        place(e, t, jnp.zeros((8, 128), F32))
    early = share_cores(1, e, e0)

    def prepare(n):
        for copy in halos[n]:
            copy.wait()
        second_edges, back_edges = received(1, n), received(2, n)
        for m in group(n):
            mean, rstd = cols[2, m], cols[3, m]
            scale = gain2 * rstd

            def halves(second, back):
                normed = (second - mean) * rstd
                return scale * normed, scale * (back * slope(gain2 * normed + shift2))

            for i in range(10):
                span = slice(i * 128, i * 128 + 128)
                hb[1, m, :, span], hb[2, m, :, span] = halves(hb[1, m, :, span], hb[2, m, :, span])
            ep[0, m], ep[1, m] = halves(second_edges, back_edges)

    stats[0] = sum_middle(2, 0, stats[0])
    prepare(0)
    stats[1] = sum_middle(2, 1, stats[1])
    prepare(1)
    early = share_plane(18, early, e, e0, e1)
    corrections = share_depth(17, corrections, bn0, bn1, bn2)

    for n in range(2):
        tile = sum_end(2, n, stats[n])
        sums2.append(tile)
        columns_of_rows(tile, 4, group(n))
        acc = zero
        for m in group(n):
            plain, weighted = gain2 * cols[3, m] * cols[4, m] / count, cols[5, m] / count

            def dact(normed, part):
                return part - plain - normed * weighted

            spread(
                dq, m,
                lambda i: dact(hb[1, m, :, i * 128 : i * 128 + 128], hb[2, m, :, i * 128 : i * 128 + 128]),
                dact(ep[0, m], ep[1, m]),
            )
            a = dot(w2b[m, 0], dq[m, :, 0:1024], 1, 0)
            a = a + dot(w2b[m, 1], dq[m, :, 128:1152], 1, 0)
            a = a + dot(w2b[m, 2], dq[m, :, 256:1280], 1, 0)
            normed = (hb[0, m, :, 128:1152] - cols[0, m]) * cols[1, m]
            dpre = a * slope1[m]
            dpre1[m] = dpre
            acc = sums(m, acc, dpre, dpre * normed)
        stats[n] = sum_start(3, n, rows_of_columns(acc))

    def gradients(m, fac):
        sfm = cols[8, m]
        byf = jnp.zeros((64, 1), F32)
        for p in range(3):
            part = dot(hq[m, :, p * 128 : p * 128 + 1024], dq[m, 64:128, 128:1152], 1, 1)
            for q in range(3):
                k = 3 * p + q
                tap = part[q * 64 : q * 64 + 64]
                byf = byf + jnp.sum(tap * sw[k].astype(F32), axis=1, keepdims=True)
                tap = tap * sfm
                accs[k] = tap if m == 0 else accs[k] + tap
        part = dot(dpre1[m].astype(BF16), x[m], 1, 1) * (gain1 * cols[1, m])
        scaled = part * rf[m : m + 1]
        accr[...] = scaled if m == 0 else accr[...] + scaled
        nf[0, m] = jnp.sum(part * rwt[...], axis=0, keepdims=True)
        return put(fac, m, byf)

    fac = zero
    for m in range(4):
        fac = gradients(m, fac)
    for a in range(16):
        h, f = a // 8, a % 8
        place(g, a, accr[f * 8 : f * 8 + 8, h * 128 : h * 128 + 128])
    for t in range(36):
        low, high = t * 8, 288 + t * 8
        place(g, SPATIAL + t, jnp.concatenate(
            [accs[low // 64, low % 64 : low % 64 + 8], accs[high // 64, high % 64 : high % 64 + 8]], axis=1
        ))
    place(g, REDUCE_F, lines(0))
    place(g, SPATIAL_F, rows_of_columns(fac))
    for t in range(SPATIAL_F + 1, LATE_TILES):
        place(g, t, jnp.zeros((8, 128), F32))
    late = share_cores(2, g, g0)
    early = share_depth(19, early, e0, e1, e2)
    late = share_plane(21, late, g, g0, g1_)
    stats[0] = sum_middle(3, 0, stats[0])
    stats[1] = sum_middle(3, 1, stats[1])
    corrections()
    bnc[...] = total(bn2, 8)
    early()
    e3[core, rank_a] = total(e2, 8)
    early = gather_plane(20, e3)

    def finish(m):
        mean, rstd, plain, weighted = cols[0, m], cols[1, m], cols[6, m] / count, cols[7, m] / count
        normed = (hb[0, m, :, 128:1152] - mean) * rstd
        dq[m, 0:64, 0:1024] = (gain1 * rstd * (dpre1[m] - plain - normed * weighted)).astype(BF16)
        for j in range(4):
            o = j * 256
            t = u[m, :, o : o + 256] + dot(w1[m], dq[m, 0:64, o : o + 256], 0, 0)
            wide[m % 2, pl.ds(2 * j, 256, stride=8), :] = t[:, :128]
            wide[m % 2, pl.ds(2 * j + 1, 256, stride=8), :] = t[:, 128:]
        craw[m] = wide[m % 2].reshape(256, 8, 128).astype(BF16)
        store = pltpu.make_async_copy(craw.at[m], y_hbm.at[m], st_sem.at[m])
        store.start()
        return store

    tile = sum_end(3, 0, stats[0])
    sums1 = [tile]
    columns_of_rows(tile, 6, group(0))
    late = share_depth(22, late, g0, g1_, g2_)
    stores = [finish(0), finish(1)]
    tile = sum_end(3, 1, stats[1])
    sums1.append(tile)
    columns_of_rows(tile, 6, group(1))

    half, block = lax.div(rank_a, 8), pl.ds(pl.multiple_of(lax.rem(rank_a, 8) * 8, 8), 8)
    span = pl.ds(pl.multiple_of(half * 128, 128), 128)
    fix = jnp.zeros((8, 128), F32)
    part = jnp.zeros((8, 128), F32)
    for k in range(2):
        m = 2 * core + k
        plain, weighted = cols[6, m, block] / count, cols[7, m, block] / count
        v = cols[10, 0, block] * cols[1, m, block] * (
            plain * sxs[m, half] + weighted * bnc[k * 8 : k * 8 + 8]
        )
        fix = fix + v * jnp.where(core == 0, rf[k : k + 1, span], rf[k + 2 : k + 3, span])
        part = jnp.where(
            sub == half * 4 + m, jnp.sum(v * rwt[block, span], axis=0, keepdims=True), part
        )
    both[core, 0:8] = fix
    both[core, 8:16] = part
    swap(5, both.at[core], both.at[core])()
    fix = jnp.where(core == 0, both[0, 0:8] + both[1, 0:8], 0.0)
    late()
    share = total(g2_, 8)
    g3[core, rank_a, 0:8] = share[0:8] - fix
    g3[core, rank_a, 8:LATE] = share[8:LATE]
    g3[core, rank_a, LATE:WHOLE] = both[0, 8:16] + both[1, 8:16]
    late = gather_plane(23, g3)
    early = gather_cores(3, early, e3)
    stores += [finish(2), finish(3)]
    first, second = sums1[0] + sums1[1], sums2[0] + sums2[1]
    norms[...] = jnp.concatenate(
        [
            jnp.sum(first[4:8], axis=0, keepdims=True),
            jnp.sum(first[0:4], axis=0, keepdims=True),
            jnp.sum(second[4:8], axis=0, keepdims=True),
            jnp.sum(second[0:4], axis=0, keepdims=True),
            jnp.zeros((4, 128), F32),
        ],
        axis=0,
    )
    late = gather_cores(4, late, g3)
    early()
    early_out[...] = e3[...]
    late()
    late_out[...] = g3[...]
    for copy in stores:
        copy.wait()


def unpack(
    y_hbm, whole, expand, norms,
    out_hbm, o_reduce, o_spatial, o_expand, o_rf, o_sf, o_ef, o_of, o_g1, o_b1, o_g2, o_b2,
    sem,
):
    store = [pltpu.make_async_copy(y_hbm.at[m], out_hbm.at[m], sem.at[m]) for m in range(4)]
    for copy in store:
        copy.start()

    def early(t):
        return expand[t // 16, t % 16]

    def late(t):
        return whole[t // 16 % 2, t % 16, t // 32 * 8 : t // 32 * 8 + 8]

    fix = jnp.zeros((8, 128), F32)
    for a in range(16):
        h, f = a // 8, a % 8
        o_expand[f * 8 : f * 8 + 8, h * 128 : h * 128 + 128] = early(a)
        o_reduce[f * 8 : f * 8 + 8, h * 128 : h * 128 + 128] = late(a)
        fix = fix + whole[0, a, LATE:WHOLE]
    for t in range(36):
        both = late(SPATIAL + t)
        for n in range(2):
            r = n * 288 + t * 8
            o_spatial[r // 64, r % 64 : r % 64 + 8] = both[:, n * 64 : n * 64 + 64]
    for o, e in ((o_rf, late(REDUCE_F) - fix), (o_of, early(OUTPUT_F))):
        o[:, :128] = e[:4]
        o[:, 128:] = e[4:]
    o_ef[...] = early(EXPAND_F)[:4, :64]
    o_sf[...] = late(SPATIAL_F)[:4, :64]
    for n, o in enumerate((o_g1, o_b1, o_g2, o_b2)):
        o[...] = norms[n : n + 1, :64]
    for copy in store:
        copy.wait()


def body(
    features, cotangent, reduce_weight, spatial_weight, expand_weight,
    reduce_factor, spatial_factor, expand_factor, output_factor,
    gain_first, shift_first, gain_second, shift_second,
):
    vmem = pl.BlockSpec(memory_space=pltpu.VMEM)
    hbm = pl.BlockSpec(memory_space=pl.ANY)
    sds = jax.ShapeDtypeStruct
    bufs = pl.pallas_call(
        kernel,
        out_shape=(
            sds((4, 256, 8, 128), BF16), sds((2, 16, WHOLE, 128), F32), sds((2, 16, EARLY, 128), F32),
            sds((8, 128), F32),
        ),
        in_specs=[pl.BlockSpec(memory_space=pltpu.HBM)] * 13,
        out_specs=(hbm, vmem, vmem, vmem),
        scratch_shapes=[
            pltpu.VMEM((4, 256, 8, 128), BF16),
            pltpu.VMEM((4, 256, 8, 128), BF16),
            pltpu.VMEM((2, 2048, 128), F32),
            pltpu.VMEM((64, 256), BF16),
            pltpu.VMEM((9, 64, 64), BF16),
            pltpu.VMEM((64, 256), BF16),
            pltpu.VMEM((4, 256), F32),
            pltpu.VMEM((4, 64), F32),
            pltpu.VMEM((4, 64), F32),
            pltpu.VMEM((4, 256), F32),
            pltpu.VMEM((1, 64), F32),
            pltpu.VMEM((1, 64), F32),
            pltpu.VMEM((1, 64), F32),
            pltpu.VMEM((1, 64), F32),
            pltpu.VMEM((4, 64, 256), BF16),
            pltpu.VMEM((4, 3, 192, 64), BF16),
            pltpu.VMEM((4, 3, 64, 192), BF16),
            pltpu.VMEM((4, 64, 256), BF16),
            pltpu.VMEM((64, 256), F32),
            pltpu.VMEM((4, 256, 1024), BF16),
            pltpu.VMEM((4, 256, 1024), BF16),
            pltpu.VMEM((4, 256, 1024), F32),
            pltpu.VMEM((4, 256, 1024), BF16),
            pltpu.VMEM((4, 64, 1024), BF16),
            pltpu.VMEM((3, 4, 64, 1280), F32),
            pltpu.VMEM((4, 192, 1280), BF16),
            pltpu.VMEM((4, 192, 1280), BF16),
            pltpu.VMEM((4, 64, 1024), F32),
            pltpu.VMEM((2, 4, 1, 256), F32),
            pltpu.VMEM((3, 2, 2, 16, 128), F32),
            pltpu.VMEM((3, 2, 6, 16, 128), F32),
            pltpu.VMEM((8, 16, 8, 128), F32),
            pltpu.VMEM((8, 16, 8, 128), F32),
            pltpu.VMEM((64, 256), F32),
            pltpu.VMEM((64, 256), F32),
            pltpu.VMEM((9, 64, 64), F32),
            pltpu.VMEM((4, 2, 8, 128), F32),
            pltpu.VMEM((2, 16, 16, 128), F32),
            pltpu.VMEM((16, 16, 128), F32),
            pltpu.VMEM((16, 16, 128), F32),
            pltpu.VMEM((8, 16, 128), F32),
            pltpu.VMEM((16, 128), F32),
            pltpu.VMEM((2, 16, EARLY, 128), F32),
            pltpu.VMEM((16, EARLY, 128), F32),
            pltpu.VMEM((16, EARLY, 128), F32),
            pltpu.VMEM((8, EARLY, 128), F32),
            pltpu.VMEM((2, 16, EARLY, 128), F32),
            pltpu.VMEM((2, 16, LATE, 128), F32),
            pltpu.VMEM((16, LATE, 128), F32),
            pltpu.VMEM((16, LATE, 128), F32),
            pltpu.VMEM((8, LATE, 128), F32),
            pltpu.VMEM((2, 16, WHOLE, 128), F32),
            pltpu.VMEM((2, 16, 128), F32),
            pltpu.VMEM((4, 64, 1024), F32),
            pltpu.VMEM((2, 4, 64, 128), F32),
            pltpu.VMEM((12, 4, 64, 1), F32),
            pltpu.SemaphoreType.DMA((20,)),
            pltpu.SemaphoreType.DMA((4,)),
            pltpu.SemaphoreType.DMA((24,)),
            pltpu.SemaphoreType.DMA((24,)),
            pltpu.SemaphoreType.DMA((6, 3)),
            pltpu.SemaphoreType.DMA((6, 3)),
            pltpu.SemaphoreType.DMA((6,)),
            pltpu.SemaphoreType.DMA((6,)),
        ],
        compiler_params=pltpu.CompilerParams(
            collective_id=0, has_side_effects=True, vmem_limit_bytes=44 * 1024 * 1024
        ),
        name="step",
    )(*[pltpu.with_memory_space_constraint(v, pltpu.HBM) for v in (
        features, cotangent, reduce_weight.T, spatial_weight, expand_weight,
        reduce_factor, spatial_factor, expand_factor, output_factor,
        gain_first.reshape(1, 64), shift_first.reshape(1, 64),
        gain_second.reshape(1, 64), shift_second.reshape(1, 64),
    )])
    outs = pl.pallas_call(
        unpack,
        out_shape=(
            sds((4, 256, 8, 128), BF16), sds((64, 256), F32), sds((9, 64, 64), F32), sds((64, 256), F32),
            sds((4, 256), F32), sds((4, 64), F32), sds((4, 64), F32), sds((4, 256), F32),
        ) + (sds((1, 64), F32),) * 4,
        in_specs=[hbm, vmem, vmem, vmem],
        out_specs=(hbm,) + (vmem,) * 11,
        scratch_shapes=[
            pltpu.SemaphoreType.DMA((4,)),
        ],
        compiler_params=pltpu.CompilerParams(vmem_limit_bytes=8 * 1024 * 1024),
        name="unpack",
    )(*bufs)
    return (outs[0], outs[1].T) + outs[2:8] + tuple(o.reshape(64) for o in outs[8:])


def solution(mesh):
    split = Mesh(
        mesh.devices.reshape(2, 4, 8, 2, 2), ("rows_0", "rows_1", "cols_0", "cols_1", "cols_2")
    )
    image = P(None, None, ROWS, COLS)
    return jax.shard_map(
        body,
        mesh=split,
        in_specs=(image, image) + (P(),) * 11,
        out_specs=(image,) + (P(),) * 11,
        check_vma=False,
    )
```
